32 devices in a mesh: gx: 2 (over x), gy: 4 (over z), gz: 4 (over y, core).
Axes of the slice: x: 2, y: 2, z: 4, core: 2. Of those that a mesh axis runs over, the one named last changes fastest.
Arguments:
- vectors: float32 [3, 12, 24, 24, 128], P(None, 'gx', 'gy', 'gz'), may hold values from -6 to 6
- orient_flip: int32 [4, 8, 1152], P('gx', 'gy', 'gz'), may hold values from 0 to 1
- reluctivity: float32 [4, 8, 512], P('gx', 'gy', 'gz'), may hold values from 0.05 to 0.5
- conductivity: float32 [4, 8, 512], P('gx', 'gy', 'gz'), may hold values from 1 to 10
Outputs:
- out_x: float32 [12, 28, 28, 128], P('gx', 'gy', 'gz')
- out_y: float32 [14, 24, 28, 128], P('gx', 'gy', 'gz')
- out_z: float32 [14, 28, 24, 128], P('gx', 'gy', 'gz')
The draws below stay inside these ranges and needn't reach their ends.
Inputs may be any that keep to these rules, and one draw needn't show every extreme that they name: `orient_flip`: 1 reverses the orientation of that degree of freedom in that element, 0 keeps it.
All inputs are finite; a program needn't handle non-finite values.
Results may differ from the reference program's by a relative error of at most 0.00007.
Values sent between devices are 32-bit elements; how exact they have to be, the bound alone decides.
A program may use at most 64 MiB of HBM per device.

```python
import math
import jax
import jax.numpy as jnp
import numpy as np
from jax import lax

ORDER = 3
QUAD = 4
VECS = 128
NX = 4
NY = 8
NZ = 8
ELEM_DOFS = 144
QPTS = 64
N_GX = 2
N_GY = 4
N_GZ = 4


def touch_ends(entries, key, low, high):
    place = [jax.random.randint(jax.random.fold_in(key, axis), (), 0, length) for axis, length in enumerate(entries.shape)]
    widest = entries.shape.index(max(entries.shape))
    neighbour = place[:widest] + [(place[widest] + 1) % entries.shape[widest]] + place[widest + 1:]
    return entries.at[tuple(place)].set(low).at[tuple(neighbour)].set(high)


def levels(key, shape, shards, least, largest):
    gain, own = 1.0, jax.random.fold_in(key, 6)
    for axis_at, parts in shards:
        heights = jnp.exp(jax.random.uniform(jax.random.fold_in(own, axis_at), (parts,), jnp.float32, least / len(shards), largest / len(shards)))
        gain = gain * jnp.repeat(heights, shape[axis_at] // parts).reshape([-1 if axis == axis_at else 1 for axis in range(len(shape))])
    return gain


def scatter_about(own_key, shape, scale, most, pieces=(), kind=jnp.bfloat16):
    entries = jax.random.normal(own_key, shape, jnp.float32) * scale
    if len(pieces) > 0:
        entries = levels(own_key, shape, pieces, -0.22, 0.18) * entries
    return jnp.clip(entries, min=-most, max=most).astype(kind)


def setup_inputs(seed: int = 0) -> dict:
    key_of = jax.random.split(jax.random.key(seed), 5)
    vectors = scatter_about(key_of[0], (3, NX * ORDER, NY * ORDER, NZ * ORDER, VECS), 1.0, 6.0, ((1, 2), (2, 4), (3, 4)), jnp.float32)
    orient_flip = touch_ends(jax.random.randint(key_of[1], (NX, NY, NZ * ELEM_DOFS), 0, 2), jax.random.fold_in(key_of[1], 1), 0, 1).astype(jnp.int32)
    reluctivity = jnp.clip(jnp.exp(math.log(0.5) - 2.3025851 * jax.random.uniform(key_of[2], (NX, NY, NZ * QPTS), jnp.float32) ** levels(key_of[2], (NX, NY, NZ * QPTS), ((0, 2), (1, 4), (2, 4)), -0.2, 0.2)), 0.05, 0.5)
    conductivity = jnp.clip(jnp.exp(math.log(10.0) - 2.3025851 * jax.random.uniform(key_of[3], (NX, NY, NZ * QPTS), jnp.float32) ** levels(key_of[3], (NX, NY, NZ * QPTS), ((0, 2), (1, 4), (2, 4)), -0.2, 0.2)), 1.0, 10.0)
    return {"vectors": vectors, "orient_flip": orient_flip, "reluctivity": reluctivity, "conductivity": conductivity}


def lagrange(points_at, evaluate_at):
    amount = len(points_at)
    values = np.ones((len(evaluate_at), amount))
    slopes = np.zeros((len(evaluate_at), amount))
    for which in range(amount):
        for column in range(amount):
            if column != which:
                factor = (evaluate_at - points_at[column]) / (points_at[which] - points_at[column])
                slopes[:, which] = slopes[:, which] * factor + values[:, which] / (points_at[which] - points_at[column])
                values[:, which] = values[:, which] * factor
    return (values, slopes)

def basis_tables():
    lobatto = np.array([0.0, (1 - 5 ** (-0.5)) / 2, (1 + 5 ** (-0.5)) / 2, 1.0])
    gauss_open = np.array([(1 - 0.6 ** 0.5) / 2, 0.5, (1 + 0.6 ** 0.5) / 2])
    inner_pt = (3.0 / 7 - 2.0 / 7 * (6.0 / 5) ** 0.5) ** 0.5
    outer_pt = (3.0 / 7 + 2.0 / 7 * (6.0 / 5) ** 0.5) ** 0.5
    inner_wt = (18 + 30 ** 0.5) / 36
    outer_wt = (18 - 30 ** 0.5) / 36
    quad_points = (1 + np.array([-outer_pt, -inner_pt, inner_pt, outer_pt])) / 2
    quad_weight = np.array([outer_wt, inner_wt, inner_wt, outer_wt]) / 2
    closed, slopes = lagrange(lobatto, quad_points)
    opened, unused_slopes = lagrange(gauss_open, quad_points)
    weight_cube = quad_weight[:, None, None, None, None] * quad_weight[None, :, None, None, None] * quad_weight[None, None, :, None, None]
    return (jnp.asarray(closed, dtype=jnp.float32), jnp.asarray(slopes, dtype=jnp.float32), jnp.asarray(opened, dtype=jnp.float32), jnp.asarray(weight_cube, dtype=jnp.float32))

def contract(tensor, first_mat, second_mat, third_mat):
    section_one = jnp.einsum('qa,abcef->qbcef', first_mat, tensor, precision=lax.Precision.HIGHEST)
    section_two = jnp.einsum('rb,qbcef->qrcef', second_mat, section_one, precision=lax.Precision.HIGHEST)
    return jnp.einsum('sc,qrcef->qrsef', third_mat, section_two, precision=lax.Precision.HIGHEST)

def evaluate(elem_x, elem_y, elem_z, closed, slopes, opened):
    u_x = contract(elem_x, opened, closed, closed)
    u_y = contract(elem_y, closed, opened, closed)
    u_z = contract(elem_z, closed, closed, opened)
    deriv_xy = contract(elem_x, opened, slopes, closed)
    deriv_xz = contract(elem_x, opened, closed, slopes)
    deriv_yx = contract(elem_y, slopes, opened, closed)
    deriv_yz = contract(elem_y, closed, opened, slopes)
    deriv_zx = contract(elem_z, slopes, closed, opened)
    deriv_zy = contract(elem_z, closed, slopes, opened)
    return (u_x, u_y, u_z, deriv_zy - deriv_yz, deriv_xz - deriv_zx, deriv_yx - deriv_xy)

def windows(array, axis, amount, open_dim):
    dims_now = array.shape
    if open_dim:
        split = array.reshape(dims_now[:axis] + (amount, ORDER) + dims_now[axis + 1:])
        return jnp.swapaxes(split, axis, axis + 1)
    reach = ORDER * (amount - 1) + 1
    return jnp.stack([lax.slice_in_dim(array, offset, offset + reach, ORDER, axis) for offset in range(ORDER + 1)], axis=axis)

def collect(array, open_axis, counts):
    result = array
    for axis in range(3):
        result = windows(result, 2 * axis, counts[axis], axis == open_axis)
    dims_now = result.shape
    result = jnp.transpose(result, (0, 2, 4, 1, 3, 5, 6))
    return result.reshape(dims_now[0], dims_now[2], dims_now[4], counts[0] * counts[1] * counts[2], dims_now[6])

def element_data(orient_flip, reluctivity, conductivity, elements):
    flip_float = orient_flip.reshape(elements, ELEM_DOFS).T.astype(jnp.float32)
    sign_all = 1.0 - 2.0 * flip_float
    per_comp = ORDER * (ORDER + 1) * (ORDER + 1)
    sign_x = sign_all[:per_comp].reshape(ORDER, ORDER + 1, ORDER + 1, elements, 1)
    sign_y = sign_all[per_comp:2 * per_comp].reshape(ORDER + 1, ORDER, ORDER + 1, elements, 1)
    sign_z = sign_all[2 * per_comp:].reshape(ORDER + 1, ORDER + 1, ORDER, elements, 1)
    reluct = reluctivity.reshape(elements, QPTS).T.reshape(QUAD, QUAD, QUAD, elements, 1)
    conduct = conductivity.reshape(elements, QPTS).T.reshape(QUAD, QUAD, QUAD, elements, 1)
    return (sign_x, sign_y, sign_z, reluct, conduct)

def element_apply(lvec_x, lvec_y, lvec_z, data, counts):

    def gather_all(part_x, part_y, part_z):
        return (collect(part_x, 0, counts), collect(part_y, 1, counts), collect(part_z, 2, counts))
    elems, scatter_back = jax.vjp(gather_all, lvec_x, lvec_y, lvec_z)
    sign_x, sign_y, sign_z, reluct, conduct = data
    closed, slopes, opened, weight_cube = basis_tables()

    def forward(part_x, part_y, part_z):
        return evaluate(part_x, part_y, part_z, closed, slopes, opened)
    quads, pullback = jax.vjp(forward, elems[0] * sign_x, elems[1] * sign_y, elems[2] * sign_z)
    mass_scale = weight_cube * conduct
    curl_scale = weight_cube * reluct
    cotangent = (mass_scale * quads[0], mass_scale * quads[1], mass_scale * quads[2], curl_scale * quads[3], curl_scale * quads[4], curl_scale * quads[5])
    grads = pullback(cotangent)
    return scatter_back((grads[0] * sign_x, grads[1] * sign_y, grads[2] * sign_z))

def extend(array, axes):
    for axis in axes:
        array = jnp.concatenate([array, lax.slice_in_dim(array, 0, 1, 1, axis)], axis)
    return array

def fold_back(array, axes):
    for axis in axes:
        total_len = array.shape[axis]
        head_sum = lax.slice_in_dim(array, 0, 1, 1, axis) + lax.slice_in_dim(array, total_len - 1, total_len, 1, axis)
        array = jnp.concatenate([head_sum, lax.slice_in_dim(array, 1, total_len - 1, 1, axis)], axis)
    return array

def spread(array, axis, blocks):
    dims_now = array.shape
    block_len = dims_now[axis] // blocks
    split = array.reshape(dims_now[:axis] + (blocks, block_len) + dims_now[axis + 1:])
    following = jnp.roll(lax.slice_in_dim(split, 0, 1, 1, axis + 1), -1, axis)
    joined = jnp.concatenate([split, following], axis + 1)
    return joined.reshape(dims_now[:axis] + (blocks * (block_len + 1),) + dims_now[axis + 1:])

def reference(vectors, orient_flip, reluctivity, conductivity):
    data = element_data(orient_flip, reluctivity, conductivity, NX * NY * NZ)
    group = math.gcd(VECS, 2)
    dims_now = vectors.shape
    grouped = jnp.moveaxis(vectors.reshape(dims_now[:4] + (VECS // group, group)), 4, 0)

    def apply_whole(single):
        results = element_apply(extend(single[0], (1, 2)), extend(single[1], (0, 2)), extend(single[2], (0, 1)), data, (NX, NY, NZ))
        own_x = fold_back(results[0], (1, 2))
        own_y = fold_back(results[1], (0, 2))
        own_z = fold_back(results[2], (0, 1))
        return (spread(spread(own_x, 1, N_GY), 2, N_GZ), spread(spread(own_y, 0, N_GX), 2, N_GZ), spread(spread(own_z, 0, N_GX), 1, N_GY))
    parts_x, parts_y, parts_z = lax.map(apply_whole, grouped)

    def unite(stacked):
        moved = jnp.moveaxis(stacked, 0, 3)
        shape_now = moved.shape
        return moved.reshape(shape_now[:3] + (VECS,))
    return (unite(parts_x), unite(parts_y), unite(parts_z))
```

```python
import functools
import jax
import jax.numpy as jnp
import numpy as np
from jax import lax
from jax.experimental import pallas as pl
from jax.experimental.pallas import tpu as pltpu
from jax.sharding import PartitionSpec as P

ORDER = 3
QUAD = 4
ELEM_DOFS = 144
QPTS = 64
AXES = ("gx", "gy", "gz")
MESH = pl.DeviceIdType.MESH
VMEM_ALL = 67043328


def lagrange(points_at, evaluate_at):
    amount = len(points_at)
    values = np.ones((len(evaluate_at), amount))
    slopes = np.zeros((len(evaluate_at), amount))
    for which in range(amount):
        for column in range(amount):
            if column != which:
                factor = (evaluate_at - points_at[column]) / (points_at[which] - points_at[column])
                slopes[:, which] = slopes[:, which] * factor + values[:, which] / (
                    points_at[which] - points_at[column]
                )
                values[:, which] = values[:, which] * factor
    return (values, slopes)


def basis_tables():
    lobatto = np.array([0.0, (1 - 5 ** (-0.5)) / 2, (1 + 5 ** (-0.5)) / 2, 1.0])
    gauss_open = np.array([(1 - 0.6**0.5) / 2, 0.5, (1 + 0.6**0.5) / 2])
    inner_pt = (3.0 / 7 - 2.0 / 7 * (6.0 / 5) ** 0.5) ** 0.5
    outer_pt = (3.0 / 7 + 2.0 / 7 * (6.0 / 5) ** 0.5) ** 0.5
    inner_wt = (18 + 30**0.5) / 36
    outer_wt = (18 - 30**0.5) / 36
    quad_points = (1 + np.array([-outer_pt, -inner_pt, inner_pt, outer_pt])) / 2
    quad_weight = np.array([outer_wt, inner_wt, inner_wt, outer_wt]) / 2
    closed, _ = lagrange(lobatto, quad_points)
    opened, _ = lagrange(gauss_open, quad_points)
    _, colloc = lagrange(quad_points, quad_points)
    return closed, opened, colloc, quad_weight


CLOSED, OPENED, COLLOC, WEIGHT = basis_tables()


def add_all(terms):
    total = terms[0]
    for term in terms[1:]:
        total = total + term
    return total


def apply(mat, xs, sigma=1):
    rows, cols = mat.shape
    half = cols // 2
    plus = [xs[p] + xs[cols - 1 - p] for p in range(half)]
    minus = [xs[p] - xs[cols - 1 - p] for p in range(half)]
    ys = [None] * rows
    for q in range((rows + 1) // 2):
        even_c = [(mat[q, p] + mat[q, cols - 1 - p]) / 2 for p in range(half)]
        odd_c = [(mat[q, p] - mat[q, cols - 1 - p]) / 2 for p in range(half)]
        even = [np.float32(c) * s for c, s in zip(even_c, plus)]
        if cols % 2:
            even.append(np.float32(mat[q, half]) * xs[half])
        even = add_all(even)
        if 2 * q == rows - 1:
            ys[q] = even
            continue
        odd = add_all([np.float32(c) * d for c, d in zip(odd_c, minus)])
        ys[q] = even + odd
        ys[rows - 1 - q] = even - odd if sigma > 0 else odd - even
    return ys


def swap(blocks, size):
    count = blocks[0].shape[0] // size
    return [
        jnp.concatenate([b[q * size : (q + 1) * size] for b in blocks], 0) for q in range(count)
    ]


def dims_of(comp):
    return [ORDER if axis == comp else ORDER + 1 for axis in range(3)]


def kernel(
    mesh_sizes, vec_hbm, flip_hbm, reluct_hbm, conduct_hbm, out_x, out_y, out_z,
    vec, flip, reluct, conduct, elem, sign, mass, curlw, flat, tmp, uq, cq,
    res_x, res_y, res_z, pack1, corner1, hx, hy, hz, hc, pack2_x, pack2_y, pack2_z, corner2,
    near_x, near_y, near_z, last_x, last_y, last_z, rc,
    face, face_own, face_out, coef, coef_in, top_x, top_z, low_x,
    s1, r1, s2, r2, s0, ready,
):
    f32 = jnp.float32
    cx, cy = flip.shape[0], flip.shape[1]
    cz = flip.shape[2] // ELEM_DOFS
    counts = (cx, cy, cz)
    ne = cx * cy * cz
    size = tuple(ORDER * c for c in counts)
    lanes = vec.shape[-1]
    me = [lax.axis_index(a) for a in AXES]

    def device(shift):
        return tuple(
            lax.rem(me[a] + (shift[a] + mesh_sizes[a]), mesh_sizes[a]) for a in range(3)
        )

    def signal(sem, shift):
        pl.semaphore_signal(sem, inc=1, device_id=device(shift), device_id_type=MESH)

    fetches = [
        pltpu.make_async_copy(src, dst, s0.at[t])
        for t, (src, dst) in enumerate(
            ((vec_hbm, vec), (flip_hbm, flip), (reluct_hbm, reluct), (conduct_hbm, conduct))
        )
    ]
    for fetch in fetches:
        fetch.start()
    barrier = pltpu.get_barrier_semaphore()
    greeted = (
        (0, -1, 0), (1, 0, 0), (0, 0, 1), (1, 0, 1), (1, -1, 0), (-1, -1, 0), (0, -1, 1), (0, -1, -1),
    )
    for shift in greeted:
        signal(barrier, shift)

    fetches[0].wait()
    for comp in (0, 1):
        for x in range(size[0]):
            for y in range(size[1]):
                pack1[comp, x, y : y + 1, :] = vec[comp, x, y, 0:1, :]
    for x in range(size[0]):
        corner1[0, x : x + 1, :] = vec[0, x, 0, 0:1, :]
    for y in range(size[1]):
        corner1[1, y : y + 1, :] = vec[1, 0, y, 0:1, :]
    pl.semaphore_wait(barrier, len(greeted))

    def send(src, dst, shift, sends, recvs, which):
        copy = pltpu.make_async_remote_copy(
            src_ref=src, dst_ref=dst, send_sem=sends.at[which], recv_sem=recvs.at[which],
            device_id=device(shift), device_id_type=MESH,
        )
        copy.start()
        return copy

    one = {
        2: send(vec.at[1:3, 0], hx, (-1, 0, 0), s1, r1, 2),
        5: send(corner1.at[1], hc.at[1], (-1, 0, -1), s1, r1, 5),
        3: send(pack1, hz, (0, 0, -1), s1, r1, 3),
    }
    for shift in ((0, 1, 0), (1, 1, 0), (-1, 1, 0), (0, 1, 1), (0, 1, -1)):
        signal(ready, shift)

    for fetch in fetches[1:]:
        fetch.wait()
    for i in range(cx):
        for j in range(cy):
            for k in range(cz):
                e = (i * cy + j) * cz + k
                flat[0, e : e + 1, 0:ELEM_DOFS] = 1.0 - 2.0 * flip[
                    i, j : j + 1, k * ELEM_DOFS : (k + 1) * ELEM_DOFS
                ].astype(f32)
                flat[1, e : e + 1, 0:QPTS] = reluct[i, j : j + 1, k * QPTS : (k + 1) * QPTS]
                flat[2, e : e + 1, 0:QPTS] = conduct[i, j : j + 1, k * QPTS : (k + 1) * QPTS]
    for d in range(ELEM_DOFS):
        sign[d * ne : (d + 1) * ne, :] = jnp.broadcast_to(flat[0, :, d : d + 1], (ne, lanes))
    for q in range(QPTS):
        w = np.float32(WEIGHT[q // 16] * WEIGHT[q // 4 % 4] * WEIGHT[q % 4])
        rows = slice(q * ne, (q + 1) * ne)
        curlw[rows, :] = jnp.broadcast_to(flat[1, :, q : q + 1] * w, (ne, lanes))
        mass[rows, :] = jnp.broadcast_to(flat[2, :, q : q + 1] * w, (ne, lanes))

    line_c, line_s = CLOSED[:, ORDER], COLLOC @ CLOSED[:, ORDER]
    face_dofs = [(a * 4 + 3) * 4 + c for a in range(3) for c in range(4)]
    face_dofs += [96 + (a * 4 + 3) * 3 + c for a in range(4) for c in range(3)]

    def quad_rows(ref, base, qx, qy):
        first = base + (qx * 16 + qy * 4) * ne
        return ref[first : first + 4 * ne, :]

    def pieces_of(block):
        return [block[t * ne : (t + 1) * ne] for t in range(block.shape[0] // ne)]

    summed = []
    for qx in range(QUAD):
        summed += pieces_of(add_all(
            [np.float32(line_c[qy] ** 2) * quad_rows(mass, 0, qx, qy) for qy in range(QUAD)]
            + [np.float32(line_s[qy] ** 2) * quad_rows(curlw, 0, qx, qy) for qy in range(QUAD)]
        ))
    for qx in range(QUAD):
        summed += pieces_of(add_all(
            [np.float32(line_c[qy] ** 2) * quad_rows(curlw, 0, qx, qy) for qy in range(QUAD)]
        ))
    summed += [sign[d * ne : (d + 1) * ne, :] for d in face_dofs]
    lane = lax.broadcasted_iota(jnp.int32, (ne, lanes), 1)
    packed = jnp.zeros((ne, lanes), f32)
    for t, value in enumerate(summed):
        packed = jnp.where(lane == t, value, packed)
    coef[...] = packed
    one[7] = send(coef, coef_in, (0, 1, 0), s1, r1, 7)

    def homes(comp, axis, low, high):
        found = []
        for el in range(counts[axis]):
            first = max(low, ORDER * el)
            last = min(high, ORDER * el + dims_of(comp)[axis])
            if first < last:
                found.append((el, first - ORDER * el, first - low, last - first))
        return found

    def places(comp, axis, at, low, high):
        dims = dims_of(comp)
        steps = (dims[1] * dims[2], dims[2], 1)
        span = [(p, p + 1) for p in at]
        span[axis] = (low, high)
        for fx in homes(comp, 0, *span[0]):
            for fy in homes(comp, 1, *span[1]):
                for fz in homes(comp, 2, *span[2]):
                    found = (fx, fy, fz)
                    e = (fx[0] * cy + fy[0]) * cz + fz[0]
                    d = comp * 48 + sum(found[t][1] * steps[t] for t in range(3))
                    yield found[axis][2], found[axis][3], d * ne + e, steps[axis] * ne

    def put(comp, axis, at, low, high, load):
        for offset, length, row, stride in places(comp, axis, at, low, high):
            elem[pl.ds(row, length, stride=stride), :] = load(offset, offset + length)

    def face_places(comp, x, low, high):
        for fx in homes(comp, 0, x, x + 1):
            for fz in homes(comp, 2, low, high):
                e = (fx[0] * cy + cy - 1) * cz + fz[0]
                d = comp // 2 * 12 + fx[1] * dims_of(comp)[2] + fz[1]
                yield fz[2], fz[3], d * ne + e

    def put_face(ref, comp, x, low, high, load):
        for offset, length, row in face_places(comp, x, low, high):
            ref[pl.ds(row, length, stride=ne), :] = load(offset, offset + length)

    blank = jnp.zeros((ne, lanes), f32)
    for t, d in enumerate(face_dofs):
        elem[d * ne : (d + 1) * ne, :] = blank
        face[t * ne : (t + 1) * ne, :] = blank
        face_own[t * ne : (t + 1) * ne, :] = blank
    for comp in range(3):
        for x in range(size[0]):
            for y in range(size[1]):
                put(comp, 2, (x, y, 0), 0, size[2], lambda a, b: vec[comp, x, y, a:b, :])
    for comp in (0, 2):
        for x in range(size[0]):
            put_face(face_own, comp, x, 0, size[2], lambda a, b: vec[comp, x, 0, a:b, :])
    top_x[...] = jnp.zeros_like(top_x)
    top_z[...] = jnp.zeros_like(top_z)
    results = (res_x, res_y, res_z)
    for res in results:
        res[...] = jnp.zeros_like(res)

    pl.semaphore_wait(ready, 5)
    one[4] = send(corner1.at[0], hc.at[0], (0, -1, -1), s1, r1, 4)
    one[6] = send(vec.at[2, 0, 0], hc.at[2], (-1, -1, 0), s1, r1, 6)
    one[0] = send(vec.at[0, :, 0], hy.at[0], (0, -1, 0), s1, r1, 0)
    one[1] = send(vec.at[2, :, 0], hy.at[1], (0, -1, 0), s1, r1, 1)

    def take_halo(comp):
        if comp == 1:
            for which in (2, 5, 3):
                one[which].wait_recv()
            for y in range(size[1]):
                put(1, 2, (size[0], y, 0), 0, size[2], lambda a, b: hx[0, y, a:b, :])
            for x in range(size[0]):
                put(1, 1, (x, 0, size[2]), 0, size[1], lambda a, b: hz[1, x, a:b, :])
            put(1, 1, (size[0], 0, size[2]), 0, size[1], lambda a, b: hc[1, a:b, :])
        elif comp == 0:
            for x in range(size[0]):
                put(0, 1, (x, 0, size[2]), 0, size[1], lambda a, b: hz[0, x, a:b, :])
                put_face(face_own, 0, x, size[2], size[2] + 1, lambda a, b: hz[0, x, 0:1, :])
        else:
            for y in range(size[1]):
                put(2, 2, (size[0], y, 0), 0, size[2], lambda a, b: hx[1, y, a:b, :])
            put_face(face_own, 2, size[0], 0, size[2], lambda a, b: hx[1, 0, a:b, :])

    def rows_of(axis, at, line, dims):
        others = [t for t in range(3) if t != axis]
        points = []
        for last in range(dims[others[1]]):
            index = [0, 0, 0]
            index[axis], index[others[0]], index[others[1]] = at, line, last
            points.append(((index[0] * dims[1] + index[1]) * dims[2] + index[2]) * ne)
        return points

    def load_line(ref, base, axis, at, line, dims):
        starts = [base + r for r in rows_of(axis, at, line, dims)]
        if len(starts) > 1 and starts[1] - starts[0] == ne:
            return ref[starts[0] : starts[-1] + ne, :]
        return jnp.concatenate([ref[s : s + ne, :] for s in starts], 0)

    def load_plane(ref, base, axis, at, dims):
        others = [t for t in range(3) if t != axis]
        return [load_line(ref, base, axis, at, p, dims) for p in range(dims[others[0]])]

    def store_plane(ref, base, axis, at, dims, blocks):
        for p, block in enumerate(blocks):
            starts = [base + r for r in rows_of(axis, at, p, dims)]
            if starts[1] - starts[0] == ne:
                ref[starts[0] : starts[-1] + ne, :] = block
            else:
                for t, s in enumerate(starts):
                    ref[s : s + ne, :] = block[t * ne : (t + 1) * ne]

    full = [QUAD] * 3

    def mid_dims(comp):
        return [ORDER if axis == comp else QUAD for axis in range(3)]

    for comp in (1, 0, 2):
        take_halo(comp)
        dims = dims_of(comp)
        base = comp * 48 * ne
        for a in range(ORDER):
            plane = load_plane(elem, base, comp, a, dims)
            signs = load_plane(sign, base, comp, a, dims)
            plane = [p * s for p, s in zip(plane, signs)]
            plane = apply(CLOSED, plane)
            plane = apply(CLOSED, swap(plane, ne))
            store_plane(tmp, base, comp, a, mid_dims(comp), swap(plane, ne))
        others = [t for t in range(3) if t != comp]
        for line in range(QUAD):
            xs = [load_line(tmp, base, comp, a, line, mid_dims(comp)) for a in range(ORDER)]
            for q, y in enumerate(apply(OPENED, xs)):
                starts = [comp * 64 * ne + r for r in rows_of(comp, q, line, full)]
                if starts[1] - starts[0] == ne:
                    uq[starts[0] : starts[-1] + ne, :] = y
                else:
                    for t, s in enumerate(starts):
                        uq[s : s + ne, :] = y[t * ne : (t + 1) * ne]

    part = 64 * ne

    for c in range(3):
        p, r = [t for t in range(3) if t != c]
        flipped = -1 if c == 1 else 1
        for at in range(QUAD):
            u_p = load_plane(uq, p * part, c, at, full)
            u_r = load_plane(uq, r * part, c, at, full)
            along_p = apply(COLLOC, u_r, -1)
            along_r = swap(apply(COLLOC, swap(u_p, ne), -1), ne)
            if flipped > 0:
                curl = [f - g for f, g in zip(along_p, along_r)]
            else:
                curl = [g - f for f, g in zip(along_p, along_r)]
            scale = load_plane(curlw, 0, c, at, full)
            store_plane(cq, c * part, c, at, full, [k * w for k, w in zip(curl, scale)])

    closed_t, opened_t, colloc_t = CLOSED.T, OPENED.T, COLLOC.T
    packs = (pack2_x, pack2_y, pack2_z)
    near = (near_x, near_y, near_z)
    last = (last_x, last_y, last_z)
    orders = ((0, 1, 2), (0, 1, 2), (0, 2, 1))
    sends = {0: [], 1: [], 2: []}

    def face_values(ref, signs):
        at = [ref[t * ne : (t + 1) * ne, :] * signs[t] for t in range(24)]
        xs = [jnp.concatenate([at[a * 4 + c] for a in range(3)], 0) for c in range(4)]
        u_x = apply(OPENED, swap(apply(CLOSED, xs), ne))
        xs = [jnp.concatenate([at[12 + a * 3 + c] for c in range(3)], 0) for a in range(4)]
        u_z = swap(apply(OPENED, swap(apply(CLOSED, xs), ne)), ne)
        along_z = swap(apply(COLLOC, swap(u_x, ne), -1), ne)
        along_x = apply(COLLOC, u_z, -1)
        return u_x, u_z, [f - g for f, g in zip(along_z, along_x)]

    def face_gradient(v_x, v_z, b, signs):
        by_z = swap(apply(colloc_t, swap(b, ne), -1), ne)
        by_x = apply(colloc_t, b, -1)
        v_x = [v + f for v, f in zip(v_x, by_z)]
        v_z = [v - f for v, f in zip(v_z, by_x)]
        for c, block in enumerate(apply(closed_t, swap(apply(opened_t, v_x), ne))):
            for a, y in enumerate(pieces_of(block)):
                t = a * 4 + c
                face_out[t * ne : (t + 1) * ne, :] = y * signs[t]
        for c, block in enumerate(apply(opened_t, swap(apply(closed_t, v_z), ne))):
            for a, y in enumerate(pieces_of(block)):
                t = 12 + a * 3 + c
                face_out[t * ne : (t + 1) * ne, :] = y * signs[t]

    v_x, v_z, b = [], [], []
    for qx in range(QUAD):
        t_x, t_z, t_b = [], [], []
        for qy in range(QUAD):
            m = quad_rows(mass, 0, qx, qy) * np.float32(line_c[qy])
            slope = np.float32(line_s[qy])
            t_x += [m * quad_rows(uq, 0, qx, qy), -slope * quad_rows(cq, 2 * part, qx, qy)]
            t_z += [m * quad_rows(uq, 2 * part, qx, qy), slope * quad_rows(cq, 0, qx, qy)]
            t_b += [np.float32(line_c[qy]) * quad_rows(cq, part, qx, qy)]
        v_x.append(add_all(t_x))
        v_z.append(add_all(t_z))
        b.append(add_all(t_b))
    own_signs = [sign[d * ne : (d + 1) * ne, :] for d in face_dofs]
    face_gradient(v_x, v_z, b, own_signs)
    for comp, top in ((0, top_x), (2, top_z)):
        for x in range(top.shape[0]):
            for offset, length, row in face_places(comp, x, 0, top.shape[1]):
                top[x, offset : offset + length, :] += face_out[pl.ds(row, length, stride=ne), :]

    def send_corner(comp, shift, slot, load):
        where = 4 * comp + slot
        for t in range(size[comp]):
            corner2[where, t : t + 1, :] = load(t)
        sends[comp].append(
            send(corner2.at[where], rc.at[where], shift, s2, r2, 8 * comp + slot)
        )

    for s in (0, 1):
        send_corner(0, (0, 1, 2 * s - 1), 2 + s, lambda t: top_x[t, s * size[2] : s * size[2] + 1, :])
        send_corner(2, (2 * s - 1, 1, 0), 2 * s + 1, lambda t: top_z[s * size[0], t : t + 1, :])
    sends[0].append(send(top_x, near_x.at[1], (0, 1, 0), s2, r2, 5))
    sends[2].append(send(top_z, last_z.at[1], (0, 1, 0), s2, r2, 16 + 7))

    for which in (0, 1, 4, 6):
        one[which].wait_recv()
    for x in range(size[0]):
        put_face(face, 0, x, 0, size[2], lambda a, b: hy[0, x, a:b, :])
        put_face(face, 0, x, size[2], size[2] + 1, lambda a, b: hc[0, x : x + 1, :])
        put_face(face, 2, x, 0, size[2], lambda a, b: hy[1, x, a:b, :])
    put_face(face, 2, size[0], 0, size[2], lambda a, b: hc[2, a:b, :])
    u_x, u_z, turn = face_values(face, own_signs)
    for qx in range(QUAD):
        for qy in range(QUAD):
            first = (qx * 16 + qy * 4) * ne
            value, slope = np.float32(line_c[qy]), np.float32(line_s[qy])
            w = curlw[first : first + 4 * ne, :]
            sloped = w * slope
            uq[first : first + 4 * ne, :] += value * u_x[qx]
            uq[2 * part + first : 2 * part + first + 4 * ne, :] += value * u_z[qx]
            cq[first : first + 4 * ne, :] += sloped * u_z[qx]
            cq[part + first : part + first + 4 * ne, :] += (w * value) * turn[qx]
            cq[2 * part + first : 2 * part + first + 4 * ne, :] -= sloped * u_x[qx]

    for comp in (1, 0, 2):
        if comp == 0:
            one[7].wait_recv()
            theirs = [
                jnp.broadcast_to(coef_in[:, t : t + 1], (ne, lanes)) for t in range(56)
            ]
            u_x, u_z, turn = face_values(face_own, theirs[32:])
            m2 = [jnp.concatenate(theirs[4 * qx : 4 * qx + 4], 0) for qx in range(QUAD)]
            k2 = [jnp.concatenate(theirs[16 + 4 * qx : 20 + 4 * qx], 0) for qx in range(QUAD)]
            face_gradient(
                [m * u for m, u in zip(m2, u_x)], [m * u for m, u in zip(m2, u_z)],
                [k * u for k, u in zip(k2, turn)], theirs[32:],
            )
        dims = dims_of(comp)
        base = comp * 48 * ne
        p, r = [t for t in range(3) if t != comp]
        for at in range(QUAD):
            u = load_plane(uq, comp * part, comp, at, full)
            m = load_plane(mass, 0, comp, at, full)
            total = [a * b for a, b in zip(u, m)]
            by_p = apply(colloc_t, load_plane(cq, r * part, comp, at, full), -1)
            by_r = apply(colloc_t, swap(load_plane(cq, p * part, comp, at, full), ne), -1)
            by_r = swap(by_r, ne)
            if comp == 1:
                total = [t + a - b for t, a, b in zip(total, by_p, by_r)]
            else:
                total = [t - a + b for t, a, b in zip(total, by_p, by_r)]
            total = apply(closed_t, total)
            total = apply(closed_t, swap(total, ne))
            kept = [QUAD if axis == comp else ORDER + 1 for axis in range(3)]
            store_plane(tmp, 0, comp, at, kept, swap(total, ne))
        for line in range(ORDER + 1):
            xs = [load_line(tmp, 0, comp, q, line, kept) for q in range(QUAD)]
            for a, y in enumerate(apply(opened_t, xs)):
                y = y * load_line(sign, base, comp, a, line, dims)
                for t, s in enumerate(rows_of(comp, a, line, dims)):
                    elem[base + s : base + s + ne, :] = y[t * ne : (t + 1) * ne]
        res = results[comp]
        order = orders[comp]
        for first in range(res.shape[0]):
            for middle in range(res.shape[1]):
                at = [0, 0, 0]
                at[order[0]], at[order[1]] = first, middle
                pieces = places(comp, order[2], at, 0, res.shape[2])
                for offset, length, row, stride in pieces:
                    res[first, middle, offset : offset + length, :] += elem[
                        pl.ds(row, length, stride=stride), :
                    ]
        rim = order[1] if comp == 0 else order[0]
        open_size, rim_size, last_size = size[comp], size[rim], size[order[2]]

        def corner(s_rim, s_last):
            shift = [0, 0, 0]
            shift[rim], shift[order[2]] = 2 * s_rim - 1, 2 * s_last - 1
            edge, row = s_rim * rim_size, s_last * last_size

            def load(t):
                f, m = (t, edge) if comp == 0 else (edge, t)
                return res[f, m, row : row + 1, :]

            send_corner(comp, shift, 2 * s_rim + s_last, load)

        def send_near(src, side):
            shift = [0, 0, 0]
            shift[rim] = 2 * side - 1
            sends[comp].append(send(src, near[comp].at[side], shift, s2, r2, 8 * comp + 4 + side))

        def send_last(side):
            shift = [0, 0, 0]
            shift[order[2]] = 2 * side - 1
            row = side * last_size
            for f in range(res.shape[0]):
                for m in range(res.shape[1]):
                    packs[comp][side, f, m : m + 1, :] = res[f, m, row : row + 1, :]
            sends[comp].append(
                send(packs[comp].at[side], last[comp].at[side], shift, s2, r2, 8 * comp + 6 + side)
            )

        if comp == 1:
            for s_rim in (0, 1):
                for s_last in (0, 1):
                    corner(s_rim, s_last)
            for side in (0, 1):
                send_near(res.at[side * rim_size], side)
            for side in (0, 1):
                send_last(side)
        elif comp == 0:
            for s_last in (0, 1):
                corner(0, s_last)
            for f in range(res.shape[0]):
                low_x[f] = res[f, 0]
            send_near(low_x, 0)
            for x in range(res.shape[0]):
                for offset, length, row in face_places(0, x, 0, res.shape[2]):
                    res[x, 0, offset : offset + length, :] += face_out[
                        pl.ds(row, length, stride=ne), :
                    ]
            for side in (0, 1):
                send_last(side)
        else:
            for s_rim in (0, 1):
                corner(s_rim, 0)
            send_last(0)
            for x in range(res.shape[0]):
                for offset, length, row in face_places(2, x, 0, res.shape[1]):
                    for t in range(length):
                        res[x, offset + t, 0:1, :] += face_out[row + t * ne : row + t * ne + 1, :]
            for side in (0, 1):
                send_near(res.at[side * rim_size], side)

    outs = (out_x, out_y, out_z)
    for comp in range(3):
        outs[comp][...] = results[comp][...]
    for comp in (1, 0, 2):
        out, order = outs[comp], orders[comp]
        rim = order[1] if comp == 0 else order[0]
        for copy in sends[comp]:
            copy.wait_recv()
        for side in (0, 1):
            edge = (1 - side) * size[rim]
            row = (1 - side) * size[order[2]]
            if comp == 0:
                for f in range(out.shape[0]):
                    out[f, edge] += near[comp][side, f]
            else:
                out[edge] += near[comp][side]
            for f in range(out.shape[0]):
                for m in range(out.shape[1]):
                    out[f, m, row : row + 1, :] += last[comp][side, f, m : m + 1, :]
            for s_last in (0, 1):
                where = 4 * comp + 2 * side + s_last
                row = (1 - s_last) * size[order[2]]
                for t in range(size[comp]):
                    f, m = (t, edge) if comp == 0 else (edge, t)
                    out[f, m, row : row + 1, :] += rc[where, t : t + 1, :]
    for copy in list(one.values()) + sends[0] + sends[1] + sends[2]:
        copy.wait_send()


def write_out(from_x, from_y, from_z, to_x, to_y, to_z, sems):
    pairs = ((from_x, to_x), (from_y, to_y), (from_z, to_z))
    copies = [pltpu.make_async_copy(src, dst, sems.at[t]) for t, (src, dst) in enumerate(pairs)]
    for copy in copies:
        copy.start()
    for copy in copies:
        copy.wait()


def on_device(mesh_sizes, vectors, orient_flip, reluctivity, conductivity):
    counts = (
        orient_flip.shape[0], orient_flip.shape[1], orient_flip.shape[2] // ELEM_DOFS,
    )
    ne = counts[0] * counts[1] * counts[2]
    sx, sy, sz = (ORDER * c for c in counts)
    lanes = vectors.shape[-1]
    f32 = jnp.float32
    shapes = (
        (sx, sy + 1, sz + 1, lanes), (sx + 1, sy, sz + 1, lanes), (sx + 1, sz, sy + 1, lanes),
    )
    longest = max(sx, sy, sz)
    faces = tuple((2,) + s[:2] + (lanes,) for s in shapes)
    scratch = [
        (ELEM_DOFS * ne, lanes), (ELEM_DOFS * ne, lanes), (QPTS * ne, lanes), (QPTS * ne, lanes),
        (3, ne, ELEM_DOFS), (ELEM_DOFS * ne, lanes), (3 * QPTS * ne, lanes), (3 * QPTS * ne, lanes),
        *shapes,
        (2, sx, sy, lanes), (2, longest, lanes),
        (2, sy, sz, lanes), (2, sx, sz, lanes), (2, sx, sy, lanes), (3, longest, lanes),
        *faces, (12, longest, lanes),
        (2, sx, sz + 1, lanes), (2, sy, sz + 1, lanes), (2, sz, sy + 1, lanes),
        *faces, (12, longest, lanes),
        (24 * ne, lanes), (24 * ne, lanes), (24 * ne, lanes), (ne, lanes), (ne, lanes),
        (sx, sz + 1, lanes), (sx + 1, sz, lanes), (sx, sz + 1, lanes),
    ]
    vmem = pl.BlockSpec(memory_space=pltpu.VMEM)
    padded = [s[0] * s[1] * (s[2] + -s[2] % 8) * lanes * 4 for s in shapes]
    room = sum(padded) + max(padded)
    anywhere = pl.BlockSpec(memory_space=pltpu.HBM)
    arguments = (vectors, orient_flip, reluctivity, conductivity)
    outs = [jax.ShapeDtypeStruct(s, f32) for s in shapes]
    held = pl.pallas_call(
        functools.partial(kernel, mesh_sizes),
        out_shape=[pltpu.VMEM(s, f32) for s in shapes],
        in_specs=[anywhere] * 4,
        out_specs=[vmem] * 3,
        scratch_shapes=[pltpu.VMEM(a.shape, a.dtype) for a in arguments]
        + [pltpu.VMEM(s, f32) for s in scratch]
        + [pltpu.SemaphoreType.DMA((8,))] * 2
        + [pltpu.SemaphoreType.DMA((24,))] * 2
        + [pltpu.SemaphoreType.DMA((4,)), pltpu.SemaphoreType.REGULAR],
        compiler_params=pltpu.CompilerParams(
            collective_id=0, has_side_effects=True, vmem_limit_bytes=VMEM_ALL - room
        ),
        name="curl_mass",
    )(*arguments)
    held = pl.pallas_call(
        write_out,
        out_shape=outs,
        in_specs=[pl.BlockSpec(memory_space=pl.ANY)] * 3,
        out_specs=[anywhere] * 3,
        scratch_shapes=[pltpu.SemaphoreType.DMA((3,))],
        compiler_params=pltpu.CompilerParams(vmem_limit_bytes=2**20),
        name="write_out",
    )(*held)
    return held[0], held[1], jnp.swapaxes(held[2], 1, 2)


def solution(mesh):
    return jax.shard_map(
        functools.partial(on_device, tuple(mesh.shape[a] for a in AXES)),
        mesh=mesh,
        in_specs=(
            P(None, "gx", "gy", "gz", None),
            P("gx", "gy", "gz"),
            P("gx", "gy", "gz"),
            P("gx", "gy", "gz"),
        ),
        out_specs=(P("gx", "gy", "gz", None), P("gx", "gy", "gz", None), P("gx", "gy", "gz", None)),
        check_vma=False,
    )
```

```python
import functools
import jax
import jax.numpy as jnp
import numpy as np
from jax import lax
from jax.experimental import pallas as pl
from jax.experimental.pallas import tpu as pltpu
from jax.sharding import PartitionSpec as P

ORDER = 3
QUAD = 4
ELEM_DOFS = 144
QPTS = 64
AXES = ("gx", "gy", "gz")
MESH = pl.DeviceIdType.MESH
VMEM_ALL = 67043328


def lagrange(points_at, evaluate_at):
    amount = len(points_at)
    values = np.ones((len(evaluate_at), amount))
    slopes = np.zeros((len(evaluate_at), amount))
    for which in range(amount):
        for column in range(amount):
            if column != which:
                factor = (evaluate_at - points_at[column]) / (points_at[which] - points_at[column])
                slopes[:, which] = slopes[:, which] * factor + values[:, which] / (
                    points_at[which] - points_at[column]
                )
                values[:, which] = values[:, which] * factor
    return (values, slopes)


def basis_tables():
    lobatto = np.array([0.0, (1 - 5 ** (-0.5)) / 2, (1 + 5 ** (-0.5)) / 2, 1.0])
    gauss_open = np.array([(1 - 0.6**0.5) / 2, 0.5, (1 + 0.6**0.5) / 2])
    inner_pt = (3.0 / 7 - 2.0 / 7 * (6.0 / 5) ** 0.5) ** 0.5
    outer_pt = (3.0 / 7 + 2.0 / 7 * (6.0 / 5) ** 0.5) ** 0.5
    inner_wt = (18 + 30**0.5) / 36
    outer_wt = (18 - 30**0.5) / 36
    quad_points = (1 + np.array([-outer_pt, -inner_pt, inner_pt, outer_pt])) / 2
    quad_weight = np.array([outer_wt, inner_wt, inner_wt, outer_wt]) / 2
    closed, _ = lagrange(lobatto, quad_points)
    opened, _ = lagrange(gauss_open, quad_points)
    _, colloc = lagrange(quad_points, quad_points)
    return closed, opened, colloc, quad_weight


CLOSED, OPENED, COLLOC, WEIGHT = basis_tables()


def add_all(terms):
    total = terms[0]
    for term in terms[1:]:
        total = total + term
    return total


def apply(mat, xs, sigma=1):
    rows, cols = mat.shape
    half = cols // 2
    plus = [xs[p] + xs[cols - 1 - p] for p in range(half)]
    minus = [xs[p] - xs[cols - 1 - p] for p in range(half)]
    ys = [None] * rows
    for q in range((rows + 1) // 2):
        even_c = [(mat[q, p] + mat[q, cols - 1 - p]) / 2 for p in range(half)]
        odd_c = [(mat[q, p] - mat[q, cols - 1 - p]) / 2 for p in range(half)]
        even = [np.float32(c) * s for c, s in zip(even_c, plus)]
        if cols % 2:
            even.append(np.float32(mat[q, half]) * xs[half])
        even = add_all(even)
        if 2 * q == rows - 1:
            ys[q] = even
            continue
        odd = add_all([np.float32(c) * d for c, d in zip(odd_c, minus)])
        ys[q] = even + odd
        ys[rows - 1 - q] = even - odd if sigma > 0 else odd - even
    return ys


def swap(blocks, size):
    count = blocks[0].shape[0] // size
    return [
        jnp.concatenate([b[q * size : (q + 1) * size] for b in blocks], 0) for q in range(count)
    ]


def dims_of(comp):
    return [ORDER if axis == comp else ORDER + 1 for axis in range(3)]


def kernel(
    mesh_sizes, vec_hbm, flip_hbm, reluct_hbm, conduct_hbm, out_x, out_y, out_z,
    vec, flip, reluct, conduct, elem, sign, mass, curlw, flat, tmp, uq, cq,
    res_x, res_y, res_z, pack1, corner1, hx, hy, hz, hc, pack2_x, pack2_y, corner2,
    near_x, near_y, near_z, last_x, last_y, last_z, rc,
    face, face_own, face_out, coef, coef_in, top_x, top_z, low_x, low_z,
    sent, came, s0, ready,
):
    f32 = jnp.float32
    cx, cy = flip.shape[0], flip.shape[1]
    cz = flip.shape[2] // ELEM_DOFS
    counts = (cx, cy, cz)
    ne = cx * cy * cz
    size = tuple(ORDER * c for c in counts)
    lanes = vec.shape[-1]
    me = [lax.axis_index(a) for a in AXES]

    def device(shift):
        return tuple(
            lax.rem(me[a] + (shift[a] + mesh_sizes[a]), mesh_sizes[a]) for a in range(3)
        )

    def signal(sem, shift):
        pl.semaphore_signal(sem, inc=1, device_id=device(shift), device_id_type=MESH)

    fetches = [
        pltpu.make_async_copy(src, dst, s0.at[t])
        for t, (src, dst) in enumerate(
            ((vec_hbm, vec), (flip_hbm, flip), (reluct_hbm, reluct), (conduct_hbm, conduct))
        )
    ]
    for fetch in fetches:
        fetch.start()
    barrier = pltpu.get_barrier_semaphore()
    greeted = (
        (0, -1, 0), (1, 0, 0), (0, 0, 1), (1, 0, 1), (1, -1, 0), (-1, -1, 0), (0, -1, 1), (0, -1, -1),
    )
    for shift in greeted:
        signal(barrier, shift)

    fetches[0].wait()
    for comp in (0, 1):
        for x in range(size[0]):
            for y in range(size[1]):
                pack1[comp, x, y : y + 1, :] = vec[comp, x, y, 0:1, :]
    for x in range(size[0]):
        corner1[0, x : x + 1, :] = vec[0, x, 0, 0:1, :]
    for y in range(size[1]):
        corner1[1, y : y + 1, :] = vec[1, 0, y, 0:1, :]
    pl.semaphore_wait(barrier, len(greeted))

    def remote(src, dst, shift, out, into):
        return pltpu.make_async_remote_copy(
            src_ref=src, dst_ref=dst, send_sem=sent.at[out], recv_sem=came.at[into],
            device_id=device(shift), device_id_type=MESH,
        )

    def send(src, dst, shift, out, into):
        remote(src, dst, shift, out, into).start()

    def arrived(ref, into):
        remote(ref, ref, (0, 1, 0), 0, into).wait_recv()

    def left(ref, out):
        remote(ref, ref, (0, 1, 0), out, 0).wait_send()

    send(vec.at[2, 0], hx.at[1], (-1, 0, 0), 0, 0)
    send(pack1.at[0], hz.at[0], (0, 0, -1), 1, 1)
    send(corner1.at[1], hc.at[0], (-1, 0, -1), 2, 2)
    send(vec.at[1, 0], hx.at[0], (-1, 0, 0), 0, 3)
    send(pack1.at[1], hz.at[1], (0, 0, -1), 1, 4)
    for shift in ((0, 1, 0), (1, 1, 0), (-1, 1, 0), (0, 1, 1), (0, 1, -1)):
        signal(ready, shift)

    for fetch in fetches[1:]:
        fetch.wait()
    for i in range(cx):
        for j in range(cy):
            for k in range(cz):
                e = (i * cy + j) * cz + k
                flat[0, e : e + 1, 0:ELEM_DOFS] = 1.0 - 2.0 * flip[
                    i, j : j + 1, k * ELEM_DOFS : (k + 1) * ELEM_DOFS
                ].astype(f32)
                flat[1, e : e + 1, 0:QPTS] = reluct[i, j : j + 1, k * QPTS : (k + 1) * QPTS]
                flat[2, e : e + 1, 0:QPTS] = conduct[i, j : j + 1, k * QPTS : (k + 1) * QPTS]
    for d in range(ELEM_DOFS):
        sign[d * ne : (d + 1) * ne, :] = jnp.broadcast_to(flat[0, :, d : d + 1], (ne, lanes))
    for q in range(QPTS):
        w = np.float32(WEIGHT[q // 16] * WEIGHT[q // 4 % 4] * WEIGHT[q % 4])
        rows = slice(q * ne, (q + 1) * ne)
        curlw[rows, :] = jnp.broadcast_to(flat[1, :, q : q + 1] * w, (ne, lanes))
        mass[rows, :] = jnp.broadcast_to(flat[2, :, q : q + 1] * w, (ne, lanes))

    line_c, line_s = CLOSED[:, ORDER], COLLOC @ CLOSED[:, ORDER]

    def plane_dofs(b):
        found = [(a * 4 + b) * 4 + c for a in range(3) for c in range(4)]
        return found + [96 + (a * 4 + b) * 3 + c for a in range(4) for c in range(3)]

    face_dofs = plane_dofs(ORDER)

    def quad_rows(ref, base, qx, qy):
        first = base + (qx * 16 + qy * 4) * ne
        return ref[first : first + 4 * ne, :]

    def pieces_of(block):
        return [block[t * ne : (t + 1) * ne] for t in range(block.shape[0] // ne)]

    summed = []
    for qx in range(QUAD):
        summed += pieces_of(add_all(
            [np.float32(line_c[qy] ** 2) * quad_rows(mass, 0, qx, qy) for qy in range(QUAD)]
            + [np.float32(line_s[qy] ** 2) * quad_rows(curlw, 0, qx, qy) for qy in range(QUAD)]
        ))
    for qx in range(QUAD):
        summed += pieces_of(add_all(
            [np.float32(line_c[qy] ** 2) * quad_rows(curlw, 0, qx, qy) for qy in range(QUAD)]
        ))
    summed += [sign[d * ne : (d + 1) * ne, :] for d in face_dofs]
    lane = lax.broadcasted_iota(jnp.int32, (ne, lanes), 1)
    packed = jnp.zeros((ne, lanes), f32)
    for t, value in enumerate(summed):
        packed = jnp.where(lane == t, value, packed)
    coef[...] = packed
    send(coef, coef_in, (0, 1, 0), 4, 7)

    def homes(comp, axis, low, high):
        found = []
        for el in range(counts[axis]):
            first = max(low, ORDER * el)
            last = min(high, ORDER * el + dims_of(comp)[axis])
            if first < last:
                found.append((el, first - ORDER * el, first - low, last - first))
        return found

    def places(comp, axis, at, low, high):
        dims = dims_of(comp)
        steps = (dims[1] * dims[2], dims[2], 1)
        span = [(p, p + 1) for p in at]
        span[axis] = (low, high)
        for fx in homes(comp, 0, *span[0]):
            for fy in homes(comp, 1, *span[1]):
                for fz in homes(comp, 2, *span[2]):
                    found = (fx, fy, fz)
                    e = (fx[0] * cy + fy[0]) * cz + fz[0]
                    d = comp * 48 + sum(found[t][1] * steps[t] for t in range(3))
                    yield found[axis][2], found[axis][3], d * ne + e, steps[axis] * ne

    def put(comp, axis, at, low, high, load):
        for offset, length, row, stride in places(comp, axis, at, low, high):
            elem[pl.ds(row, length, stride=stride), :] = load(offset, offset + length)

    def face_places(comp, x, low, high, layer=cy - 1):
        for fx in homes(comp, 0, x, x + 1):
            for fz in homes(comp, 2, low, high):
                e = (fx[0] * cy + layer) * cz + fz[0]
                d = comp // 2 * 12 + fx[1] * dims_of(comp)[2] + fz[1]
                yield fz[2], fz[3], d * ne + e

    def put_face(ref, comp, x, low, high, load):
        for offset, length, row in face_places(comp, x, low, high):
            ref[pl.ds(row, length, stride=ne), :] = load(offset, offset + length)

    blank = jnp.zeros((ne, lanes), f32)
    for t, d in enumerate(face_dofs):
        elem[d * ne : (d + 1) * ne, :] = blank
        face[t * ne : (t + 1) * ne, :] = blank
        face_own[t * ne : (t + 1) * ne, :] = blank
    for comp in range(3):
        for x in range(size[0]):
            for y in range(size[1]):
                put(comp, 2, (x, y, 0), 0, size[2], lambda a, b: vec[comp, x, y, a:b, :])
    for comp in (0, 2):
        for x in range(size[0]):
            put_face(face_own, comp, x, 0, size[2], lambda a, b: vec[comp, x, 0, a:b, :])
    results = (res_x, res_y, res_z)
    for res in (top_x, top_z, low_x, low_z) + results:
        res[...] = jnp.zeros_like(res)

    pl.semaphore_wait(ready, 5)
    send(corner1.at[0], hc.at[1], (0, -1, -1), 2, 6)
    send(vec.at[2, 0, 0], hc.at[2], (-1, -1, 0), 2, 6)
    send(vec.at[0, :, 0], hy.at[0], (0, -1, 0), 3, 5)
    send(vec.at[2, :, 0], hy.at[1], (0, -1, 0), 3, 5)

    def take_halo(comp):
        if comp == 1:
            arrived(hc.at[0], 2)
            arrived(hx.at[0], 3)
            arrived(hz.at[1], 4)
            for y in range(size[1]):
                put(1, 2, (size[0], y, 0), 0, size[2], lambda a, b: hx[0, y, a:b, :])
            for x in range(size[0]):
                put(1, 1, (x, 0, size[2]), 0, size[1], lambda a, b: hz[1, x, a:b, :])
            put(1, 1, (size[0], 0, size[2]), 0, size[1], lambda a, b: hc[0, a:b, :])
        elif comp == 0:
            arrived(hz.at[0], 1)
            for x in range(size[0]):
                put(0, 1, (x, 0, size[2]), 0, size[1], lambda a, b: hz[0, x, a:b, :])
                put_face(face_own, 0, x, size[2], size[2] + 1, lambda a, b: hz[0, x, 0:1, :])
        else:
            arrived(hx.at[1], 0)
            for y in range(size[1]):
                put(2, 2, (size[0], y, 0), 0, size[2], lambda a, b: hx[1, y, a:b, :])
            put_face(face_own, 2, size[0], 0, size[2], lambda a, b: hx[1, 0, a:b, :])

    def rows_of(axis, at, line, dims):
        others = [t for t in range(3) if t != axis]
        points = []
        for last in range(dims[others[1]]):
            index = [0, 0, 0]
            index[axis], index[others[0]], index[others[1]] = at, line, last
            points.append(((index[0] * dims[1] + index[1]) * dims[2] + index[2]) * ne)
        return points

    def load_line(ref, base, axis, at, line, dims):
        starts = [base + r for r in rows_of(axis, at, line, dims)]
        if len(starts) > 1 and starts[1] - starts[0] == ne:
            return ref[starts[0] : starts[-1] + ne, :]
        return jnp.concatenate([ref[s : s + ne, :] for s in starts], 0)

    def load_plane(ref, base, axis, at, dims):
        others = [t for t in range(3) if t != axis]
        return [load_line(ref, base, axis, at, p, dims) for p in range(dims[others[0]])]

    def store_plane(ref, base, axis, at, dims, blocks):
        for p, block in enumerate(blocks):
            starts = [base + r for r in rows_of(axis, at, p, dims)]
            if starts[1] - starts[0] == ne:
                ref[starts[0] : starts[-1] + ne, :] = block
            else:
                for t, s in enumerate(starts):
                    ref[s : s + ne, :] = block[t * ne : (t + 1) * ne]

    full = [QUAD] * 3

    def mid_dims(comp):
        return [ORDER if axis == comp else QUAD for axis in range(3)]

    def evaluate(comp):
        take_halo(comp)
        dims = dims_of(comp)
        base = comp * 48 * ne
        for a in range(ORDER):
            plane = load_plane(elem, base, comp, a, dims)
            signs = load_plane(sign, base, comp, a, dims)
            plane = [p * s for p, s in zip(plane, signs)]
            plane = apply(CLOSED, plane)
            plane = apply(CLOSED, swap(plane, ne))
            store_plane(tmp, base, comp, a, mid_dims(comp), swap(plane, ne))
        others = [t for t in range(3) if t != comp]
        for line in range(QUAD):
            xs = [load_line(tmp, base, comp, a, line, mid_dims(comp)) for a in range(ORDER)]
            for q, y in enumerate(apply(OPENED, xs)):
                starts = [comp * 64 * ne + r for r in rows_of(comp, q, line, full)]
                if starts[1] - starts[0] == ne:
                    uq[starts[0] : starts[-1] + ne, :] = y
                else:
                    for t, s in enumerate(starts):
                        uq[s : s + ne, :] = y[t * ne : (t + 1) * ne]

    part = 64 * ne

    def turn_of(c):
        p, r = [t for t in range(3) if t != c]
        flipped = -1 if c == 1 else 1
        for at in range(QUAD):
            u_p = load_plane(uq, p * part, c, at, full)
            u_r = load_plane(uq, r * part, c, at, full)
            along_p = apply(COLLOC, u_r, -1)
            along_r = swap(apply(COLLOC, swap(u_p, ne), -1), ne)
            if flipped > 0:
                curl = [f - g for f, g in zip(along_p, along_r)]
            else:
                curl = [g - f for f, g in zip(along_p, along_r)]
            scale = load_plane(curlw, 0, c, at, full)
            store_plane(cq, c * part, c, at, full, [k * w for k, w in zip(curl, scale)])

    evaluate(2)
    evaluate(0)
    turn_of(1)
    evaluate(1)
    turn_of(0)
    turn_of(2)

    closed_t, opened_t, colloc_t = CLOSED.T, OPENED.T, COLLOC.T
    packs = (pack2_x, pack2_y)
    near = (near_x, near_y, near_z)
    last = (last_x, last_y, last_z)
    orders = ((0, 1, 2), (0, 1, 2), (0, 2, 1))

    def face_values(ref, signs):
        at = [ref[t * ne : (t + 1) * ne, :] * signs[t] for t in range(24)]
        xs = [jnp.concatenate([at[a * 4 + c] for a in range(3)], 0) for c in range(4)]
        u_x = apply(OPENED, swap(apply(CLOSED, xs), ne))
        xs = [jnp.concatenate([at[12 + a * 3 + c] for c in range(3)], 0) for a in range(4)]
        u_z = swap(apply(OPENED, swap(apply(CLOSED, xs), ne)), ne)
        along_z = swap(apply(COLLOC, swap(u_x, ne), -1), ne)
        along_x = apply(COLLOC, u_z, -1)
        return u_x, u_z, [f - g for f, g in zip(along_z, along_x)]

    def face_gradient(v_x, v_z, b, signs):
        by_z = swap(apply(colloc_t, swap(b, ne), -1), ne)
        by_x = apply(colloc_t, b, -1)
        v_x = [v + f for v, f in zip(v_x, by_z)]
        v_z = [v - f for v, f in zip(v_z, by_x)]
        for c, block in enumerate(apply(closed_t, swap(apply(opened_t, v_x), ne))):
            for a, y in enumerate(pieces_of(block)):
                t = a * 4 + c
                face_out[t * ne : (t + 1) * ne, :] = y * signs[t]
        for c, block in enumerate(apply(opened_t, swap(apply(closed_t, v_z), ne))):
            for a, y in enumerate(pieces_of(block)):
                t = 12 + a * 3 + c
                face_out[t * ne : (t + 1) * ne, :] = y * signs[t]

    def plane_fields(values, slopes):
        v_x, v_z, b = [], [], []
        for qx in range(QUAD):
            t_x, t_z, t_b = [], [], []
            for qy in range(QUAD):
                m = quad_rows(mass, 0, qx, qy) * np.float32(values[qy])
                slope = np.float32(slopes[qy])
                t_x += [m * quad_rows(uq, 0, qx, qy), -slope * quad_rows(cq, 2 * part, qx, qy)]
                t_z += [m * quad_rows(uq, 2 * part, qx, qy), slope * quad_rows(cq, 0, qx, qy)]
                t_b += [np.float32(values[qy]) * quad_rows(cq, part, qx, qy)]
            v_x.append(add_all(t_x))
            v_z.append(add_all(t_z))
            b.append(add_all(t_b))
        return v_x, v_z, b

    def signs_of(dofs):
        return [sign[d * ne : (d + 1) * ne, :] for d in dofs]

    def send_corner(comp, shift, slot, load):
        where = 4 * comp + slot
        for t in range(size[comp]):
            corner2[where, t : t + 1, :] = load(t)
        send(corner2.at[where], rc.at[where], shift, 5 + comp, 8 + comp)

    def send_plane(side, plane_x, plane_z):
        b, layer = side * ORDER, side * (cy - 1)
        fields = plane_fields(CLOSED[:, b], COLLOC @ CLOSED[:, b])
        face_gradient(*fields, signs_of(plane_dofs(b)))
        for comp, plane in ((0, plane_x), (2, plane_z)):
            for x in range(plane.shape[0]):
                for offset, length, row in face_places(comp, x, 0, plane.shape[1], layer):
                    plane[x, offset : offset + length, :] += face_out[
                        pl.ds(row, length, stride=ne), :
                    ]
        way = 2 * side - 1
        for s in (0, 1):
            z, x = s * size[2], s * size[0]
            send_corner(0, (0, way, 2 * s - 1), 2 * side + s, lambda t: plane_x[t, z : z + 1, :])
            send_corner(2, (2 * s - 1, way, 0), 2 * s + side, lambda t: plane_z[x, t : t + 1, :])
        send(plane_x, near_x.at[side], (0, way, 0), 8, 11)
        send(plane_z, last_z.at[side], (0, way, 0), 13, 16)

    send_plane(1, top_x, top_z)
    if cy > 1:
        send_plane(0, low_x, low_z)

    arrived(hy, 5)
    arrived(hc.at[1:3], 6)
    for x in range(size[0]):
        put_face(face, 0, x, 0, size[2], lambda a, b: hy[0, x, a:b, :])
        put_face(face, 0, x, size[2], size[2] + 1, lambda a, b: hc[1, x : x + 1, :])
        put_face(face, 2, x, 0, size[2], lambda a, b: hy[1, x, a:b, :])
    put_face(face, 2, size[0], 0, size[2], lambda a, b: hc[2, a:b, :])
    own_signs = signs_of(face_dofs)
    u_x, u_z, turn = face_values(face, own_signs)
    for qx in range(QUAD):
        for qy in range(QUAD):
            first = (qx * 16 + qy * 4) * ne
            value, slope = np.float32(line_c[qy]), np.float32(line_s[qy])
            w = curlw[first : first + 4 * ne, :]
            sloped = w * slope
            uq[first : first + 4 * ne, :] += value * u_x[qx]
            uq[2 * part + first : 2 * part + first + 4 * ne, :] += value * u_z[qx]
            cq[first : first + 4 * ne, :] += sloped * u_z[qx]
            cq[part + first : part + first + 4 * ne, :] += (w * value) * turn[qx]
            cq[2 * part + first : 2 * part + first + 4 * ne, :] -= sloped * u_x[qx]

    if cy == 1:
        send_plane(0, low_x, low_z)

    for comp in (1, 2, 0):
        if comp == 2:
            arrived(coef_in, 7)
            theirs = [
                jnp.broadcast_to(coef_in[:, t : t + 1], (ne, lanes)) for t in range(56)
            ]
            u_x, u_z, turn = face_values(face_own, theirs[32:])
            m2 = [jnp.concatenate(theirs[4 * qx : 4 * qx + 4], 0) for qx in range(QUAD)]
            k2 = [jnp.concatenate(theirs[16 + 4 * qx : 20 + 4 * qx], 0) for qx in range(QUAD)]
            face_gradient(
                [m * u for m, u in zip(m2, u_x)], [m * u for m, u in zip(m2, u_z)],
                [k * u for k, u in zip(k2, turn)], theirs[32:],
            )
        dims = dims_of(comp)
        base = comp * 48 * ne
        p, r = [t for t in range(3) if t != comp]
        for at in range(QUAD):
            u = load_plane(uq, comp * part, comp, at, full)
            m = load_plane(mass, 0, comp, at, full)
            total = [a * b for a, b in zip(u, m)]
            by_p = apply(colloc_t, load_plane(cq, r * part, comp, at, full), -1)
            by_r = apply(colloc_t, swap(load_plane(cq, p * part, comp, at, full), ne), -1)
            by_r = swap(by_r, ne)
            if comp == 1:
                total = [t + a - b for t, a, b in zip(total, by_p, by_r)]
            else:
                total = [t - a + b for t, a, b in zip(total, by_p, by_r)]
            total = apply(closed_t, total)
            total = apply(closed_t, swap(total, ne))
            kept = [QUAD if axis == comp else ORDER + 1 for axis in range(3)]
            store_plane(tmp, 0, comp, at, kept, swap(total, ne))
        for line in range(ORDER + 1):
            xs = [load_line(tmp, 0, comp, q, line, kept) for q in range(QUAD)]
            for a, y in enumerate(apply(opened_t, xs)):
                y = y * load_line(sign, base, comp, a, line, dims)
                for t, s in enumerate(rows_of(comp, a, line, dims)):
                    elem[base + s : base + s + ne, :] = y[t * ne : (t + 1) * ne]
        res = results[comp]
        order = orders[comp]
        for first in range(res.shape[0]):
            for middle in range(res.shape[1]):
                at = [0, 0, 0]
                at[order[0]], at[order[1]] = first, middle
                pieces = places(comp, order[2], at, 0, res.shape[2])
                for offset, length, row, stride in pieces:
                    res[first, middle, offset : offset + length, :] += elem[
                        pl.ds(row, length, stride=stride), :
                    ]
        if comp == 0:
            for x in range(size[0]):
                for offset, length, row in face_places(0, x, 0, res.shape[2]):
                    res[x, 0, offset : offset + length, :] += face_out[
                        pl.ds(row, length, stride=ne), :
                    ]
        elif comp == 1:
            for s_x in (0, 1):
                for s_z in (0, 1):
                    x, z = s_x * size[0], s_z * size[2]
                    send_corner(
                        1, (2 * s_x - 1, 0, 2 * s_z - 1), 2 * s_x + s_z,
                        lambda t: res[x, t, z : z + 1, :],
                    )
        else:
            for x in range(res.shape[0]):
                for offset, length, row in face_places(2, x, 0, res.shape[1]):
                    for t in range(length):
                        res[x, offset + t, 0:1, :] += face_out[row + t * ne : row + t * ne + 1, :]
        if comp > 0:
            for side in (0, 1):
                send(
                    res.at[side * size[0]], near[comp].at[side], (2 * side - 1, 0, 0),
                    8 + comp, 11 + comp,
                )
        if comp < 2:
            for side in (0, 1):
                row = side * size[2]
                for f in range(res.shape[0]):
                    for m in range(res.shape[1]):
                        packs[comp][side, f, m : m + 1, :] = res[f, m, row : row + 1, :]
                send(
                    packs[comp].at[side], last[comp].at[side], (0, 0, 2 * side - 1),
                    11 + comp, 14 + comp,
                )

    outs = (out_x, out_y, out_z)
    for comp in range(3):
        outs[comp][...] = results[comp][...]
    for comp in (1, 0, 2):
        out, order = outs[comp], orders[comp]
        rim = order[1] if comp == 0 else order[0]
        arrived(rc.at[4 * comp : 4 * comp + 4], 8 + comp)
        arrived(near[comp], 11 + comp)
        arrived(last[comp], 14 + comp)
        for side in (0, 1):
            edge = (1 - side) * size[rim]
            row = (1 - side) * size[order[2]]
            if comp == 0:
                for f in range(out.shape[0]):
                    out[f, edge] += near[comp][side, f]
            else:
                out[edge] += near[comp][side]
            for f in range(out.shape[0]):
                for m in range(out.shape[1]):
                    out[f, m, row : row + 1, :] += last[comp][side, f, m : m + 1, :]
            for s_last in (0, 1):
                where = 4 * comp + 2 * side + s_last
                row = (1 - s_last) * size[order[2]]
                for t in range(size[comp]):
                    f, m = (t, edge) if comp == 0 else (edge, t)
                    out[f, m, row : row + 1, :] += rc[where, t : t + 1, :]
    for out, ref in enumerate((hx, hz, hc, hy, coef)):
        left(ref, out)
    for comp in range(3):
        left(rc.at[4 * comp : 4 * comp + 4], 5 + comp)
        left(near[comp], 8 + comp)
        left(last[comp], 11 + comp)


def write_out(from_x, from_y, from_z, to_x, to_y, to_z, sems):
    pairs = ((from_x, to_x), (from_y, to_y), (from_z, to_z))
    copies = [pltpu.make_async_copy(src, dst, sems.at[t]) for t, (src, dst) in enumerate(pairs)]
    for copy in copies:
        copy.start()
    for copy in copies:
        copy.wait()


def on_device(mesh_sizes, vectors, orient_flip, reluctivity, conductivity):
    counts = (
        orient_flip.shape[0], orient_flip.shape[1], orient_flip.shape[2] // ELEM_DOFS,
    )
    ne = counts[0] * counts[1] * counts[2]
    sx, sy, sz = (ORDER * c for c in counts)
    lanes = vectors.shape[-1]
    f32 = jnp.float32
    shapes = (
        (sx, sy + 1, sz + 1, lanes), (sx + 1, sy, sz + 1, lanes), (sx + 1, sz, sy + 1, lanes),
    )
    longest = max(sx, sy, sz)
    faces = tuple((2,) + s[:2] + (lanes,) for s in shapes)
    scratch = [
        (ELEM_DOFS * ne, lanes), (ELEM_DOFS * ne, lanes), (QPTS * ne, lanes), (QPTS * ne, lanes),
        (3, ne, ELEM_DOFS), (ELEM_DOFS * ne, lanes), (3 * QPTS * ne, lanes), (3 * QPTS * ne, lanes),
        *shapes,
        (2, sx, sy, lanes), (2, longest, lanes),
        (2, sy, sz, lanes), (2, sx, sz, lanes), (2, sx, sy, lanes), (3, longest, lanes),
        *faces[:2], (12, longest, lanes),
        (2, sx, sz + 1, lanes), (2, sy, sz + 1, lanes), (2, sz, sy + 1, lanes),
        *faces, (12, longest, lanes),
        (24 * ne, lanes), (24 * ne, lanes), (24 * ne, lanes), (ne, lanes), (ne, lanes),
        (sx, sz + 1, lanes), (sx + 1, sz, lanes), (sx, sz + 1, lanes), (sx + 1, sz, lanes),
    ]
    vmem = pl.BlockSpec(memory_space=pltpu.VMEM)
    padded = [s[0] * s[1] * (s[2] + -s[2] % 8) * lanes * 4 for s in shapes]
    room = sum(padded) + max(padded)
    anywhere = pl.BlockSpec(memory_space=pltpu.HBM)
    arguments = (vectors, orient_flip, reluctivity, conductivity)
    outs = [jax.ShapeDtypeStruct(s, f32) for s in shapes]
    held = pl.pallas_call(
        functools.partial(kernel, mesh_sizes),
        out_shape=[pltpu.VMEM(s, f32) for s in shapes],
        in_specs=[anywhere] * 4,
        out_specs=[vmem] * 3,
        scratch_shapes=[pltpu.VMEM(a.shape, a.dtype) for a in arguments]
        + [pltpu.VMEM(s, f32) for s in scratch]
        + [pltpu.SemaphoreType.DMA((14,)), pltpu.SemaphoreType.DMA((17,))]
        + [pltpu.SemaphoreType.DMA((4,)), pltpu.SemaphoreType.REGULAR],
        compiler_params=pltpu.CompilerParams(
            collective_id=0, has_side_effects=True, vmem_limit_bytes=VMEM_ALL - room
        ),
        name="curl_mass",
    )(*arguments)
    held = pl.pallas_call(
        write_out,
        out_shape=outs,
        in_specs=[pl.BlockSpec(memory_space=pl.ANY)] * 3,
        out_specs=[anywhere] * 3,
        scratch_shapes=[pltpu.SemaphoreType.DMA((3,))],
        compiler_params=pltpu.CompilerParams(vmem_limit_bytes=2**20),
        name="write_out",
    )(*held)
    return held[0], held[1], jnp.swapaxes(held[2], 1, 2)


def solution(mesh):
    return jax.shard_map(
        functools.partial(on_device, tuple(mesh.shape[a] for a in AXES)),
        mesh=mesh,
        in_specs=(
            P(None, "gx", "gy", "gz", None),
            P("gx", "gy", "gz"),
            P("gx", "gy", "gz"),
            P("gx", "gy", "gz"),
        ),
        out_specs=(P("gx", "gy", "gz", None), P("gx", "gy", "gz", None), P("gx", "gy", "gz", None)),
        check_vma=False,
    )
```

```python
import functools
import jax
import jax.numpy as jnp
import numpy as np
from jax import lax
from jax.experimental import pallas as pl
from jax.experimental.pallas import tpu as pltpu
from jax.sharding import PartitionSpec as P

ORDER = 3
QUAD = 4
ELEM_DOFS = 144
QPTS = 64
AXES = ("gx", "gy", "gz")
MESH = pl.DeviceIdType.MESH
VMEM_ALL = 67043328


def lagrange(points_at, evaluate_at):
    amount = len(points_at)
    values = np.ones((len(evaluate_at), amount))
    slopes = np.zeros((len(evaluate_at), amount))
    for which in range(amount):
        for column in range(amount):
            if column != which:
                factor = (evaluate_at - points_at[column]) / (points_at[which] - points_at[column])
                slopes[:, which] = slopes[:, which] * factor + values[:, which] / (
                    points_at[which] - points_at[column]
                )
                values[:, which] = values[:, which] * factor
    return (values, slopes)


def basis_tables():
    lobatto = np.array([0.0, (1 - 5 ** (-0.5)) / 2, (1 + 5 ** (-0.5)) / 2, 1.0])
    gauss_open = np.array([(1 - 0.6**0.5) / 2, 0.5, (1 + 0.6**0.5) / 2])
    inner_pt = (3.0 / 7 - 2.0 / 7 * (6.0 / 5) ** 0.5) ** 0.5
    outer_pt = (3.0 / 7 + 2.0 / 7 * (6.0 / 5) ** 0.5) ** 0.5
    inner_wt = (18 + 30**0.5) / 36
    outer_wt = (18 - 30**0.5) / 36
    quad_points = (1 + np.array([-outer_pt, -inner_pt, inner_pt, outer_pt])) / 2
    quad_weight = np.array([outer_wt, inner_wt, inner_wt, outer_wt]) / 2
    closed, _ = lagrange(lobatto, quad_points)
    opened, _ = lagrange(gauss_open, quad_points)
    _, colloc = lagrange(quad_points, quad_points)
    return closed, opened, colloc, quad_weight


CLOSED, OPENED, COLLOC, WEIGHT = basis_tables()


def add_all(terms):
    total = terms[0]
    for term in terms[1:]:
        total = total + term
    return total


def apply(mat, xs, sigma=1):
    rows, cols = mat.shape
    half = cols // 2
    plus = [xs[p] + xs[cols - 1 - p] for p in range(half)]
    minus = [xs[p] - xs[cols - 1 - p] for p in range(half)]
    ys = [None] * rows
    for q in range((rows + 1) // 2):
        even_c = [(mat[q, p] + mat[q, cols - 1 - p]) / 2 for p in range(half)]
        odd_c = [(mat[q, p] - mat[q, cols - 1 - p]) / 2 for p in range(half)]
        even = [np.float32(c) * s for c, s in zip(even_c, plus)]
        if cols % 2:
            even.append(np.float32(mat[q, half]) * xs[half])
        even = add_all(even)
        if 2 * q == rows - 1:
            ys[q] = even
            continue
        odd = add_all([np.float32(c) * d for c, d in zip(odd_c, minus)])
        ys[q] = even + odd
        ys[rows - 1 - q] = even - odd if sigma > 0 else odd - even
    return ys


def swap(blocks, size):
    count = blocks[0].shape[0] // size
    return [
        jnp.concatenate([b[q * size : (q + 1) * size] for b in blocks], 0) for q in range(count)
    ]


def dims_of(comp):
    return [ORDER if axis == comp else ORDER + 1 for axis in range(3)]


def kernel(
    mesh_sizes, vec_hbm, flip_hbm, reluct_hbm, conduct_hbm, out_x, out_y, out_z,
    vec, flip, reluct, conduct, elem, sign, mass, curlw, flat, tmp, uq, cq,
    res_x, res_y, res_z, pack1, corner1, hx, hy, hz, hc, pack2_x, pack2_y, corner2,
    near_x, near_y, near_z, last_x, last_y, last_z, rc,
    face, face_own, face_out, coef, coef_in, top_x, top_z, low_x, low_z,
    sent, came, s0, ready,
):
    f32 = jnp.float32
    cx, cy = flip.shape[0], flip.shape[1]
    cz = flip.shape[2] // ELEM_DOFS
    counts = (cx, cy, cz)
    ne = cx * cy * cz
    size = tuple(ORDER * c for c in counts)
    lanes = vec.shape[-1]
    me = [lax.axis_index(a) for a in AXES]

    def device(shift):
        return tuple(
            lax.rem(me[a] + (shift[a] + mesh_sizes[a]), mesh_sizes[a]) for a in range(3)
        )

    def signal(sem, shift):
        pl.semaphore_signal(sem, inc=1, device_id=device(shift), device_id_type=MESH)

    fetches = [
        pltpu.make_async_copy(src, dst, s0.at[t])
        for t, (src, dst) in enumerate(
            ((vec_hbm, vec), (flip_hbm, flip), (reluct_hbm, reluct), (conduct_hbm, conduct))
        )
    ]
    for fetch in fetches:
        fetch.start()
    barrier = pltpu.get_barrier_semaphore()
    greeted = (
        (0, -1, 0), (1, 0, 0), (0, 0, 1), (1, 0, 1), (1, -1, 0), (-1, -1, 0), (0, -1, 1), (0, -1, -1),
    )
    for shift in greeted:
        signal(barrier, shift)

    fetches[0].wait()
    for comp in (0, 1):
        for x in range(size[0]):
            for y in range(size[1]):
                pack1[comp, x, y : y + 1, :] = vec[comp, x, y, 0:1, :]
    for x in range(size[0]):
        corner1[0, x : x + 1, :] = vec[0, x, 0, 0:1, :]
    for y in range(size[1]):
        corner1[1, y : y + 1, :] = vec[1, 0, y, 0:1, :]
    pl.semaphore_wait(barrier, len(greeted))

    def remote(src, dst, shift, out, into):
        return pltpu.make_async_remote_copy(
            src_ref=src, dst_ref=dst, send_sem=sent.at[out], recv_sem=came.at[into],
            device_id=device(shift), device_id_type=MESH,
        )

    def send(src, dst, shift, out, into):
        remote(src, dst, shift, out, into).start()

    def arrived(ref, into):
        remote(ref, ref, (0, 1, 0), 0, into).wait_recv()

    def left(ref, out):
        remote(ref, ref, (0, 1, 0), out, 0).wait_send()

    send(vec.at[2, 0], hx.at[1], (-1, 0, 0), 0, 0)
    send(pack1.at[0], hz.at[0], (0, 0, -1), 1, 1)
    send(corner1.at[1], hc.at[0], (-1, 0, -1), 2, 2)
    send(vec.at[1, 0], hx.at[0], (-1, 0, 0), 0, 3)
    send(pack1.at[1], hz.at[1], (0, 0, -1), 1, 4)
    for shift in ((0, 1, 0), (1, 1, 0), (-1, 1, 0), (0, 1, 1), (0, 1, -1)):
        signal(ready, shift)

    for fetch in fetches[1:]:
        fetch.wait()
    for i in range(cx):
        for j in range(cy):
            for k in range(cz):
                e = (i * cy + j) * cz + k
                flat[0, e : e + 1, 0:ELEM_DOFS] = 1.0 - 2.0 * flip[
                    i, j : j + 1, k * ELEM_DOFS : (k + 1) * ELEM_DOFS
                ].astype(f32)
                flat[1, e : e + 1, 0:QPTS] = reluct[i, j : j + 1, k * QPTS : (k + 1) * QPTS]
                flat[2, e : e + 1, 0:QPTS] = conduct[i, j : j + 1, k * QPTS : (k + 1) * QPTS]
    for d in range(ELEM_DOFS):
        sign[d * ne : (d + 1) * ne, :] = jnp.broadcast_to(flat[0, :, d : d + 1], (ne, lanes))
    for q in range(QPTS):
        w = np.float32(WEIGHT[q // 16] * WEIGHT[q // 4 % 4] * WEIGHT[q % 4])
        rows = slice(q * ne, (q + 1) * ne)
        curlw[rows, :] = jnp.broadcast_to(flat[1, :, q : q + 1] * w, (ne, lanes))
        mass[rows, :] = jnp.broadcast_to(flat[2, :, q : q + 1] * w, (ne, lanes))

    line_c, line_s = CLOSED[:, ORDER], COLLOC @ CLOSED[:, ORDER]

    def plane_dofs(b):
        found = [(a * 4 + b) * 4 + c for a in range(3) for c in range(4)]
        return found + [96 + (a * 4 + b) * 3 + c for a in range(4) for c in range(3)]

    face_dofs = plane_dofs(ORDER)

    def quad_rows(ref, base, qx, qy):
        first = base + (qx * 16 + qy * 4) * ne
        return ref[first : first + 4 * ne, :]

    def pieces_of(block):
        return [block[t * ne : (t + 1) * ne] for t in range(block.shape[0] // ne)]

    summed = []
    for qx in range(QUAD):
        summed += pieces_of(add_all(
            [np.float32(line_c[qy] ** 2) * quad_rows(mass, 0, qx, qy) for qy in range(QUAD)]
            + [np.float32(line_s[qy] ** 2) * quad_rows(curlw, 0, qx, qy) for qy in range(QUAD)]
        ))
    for qx in range(QUAD):
        summed += pieces_of(add_all(
            [np.float32(line_c[qy] ** 2) * quad_rows(curlw, 0, qx, qy) for qy in range(QUAD)]
        ))
    summed += [sign[d * ne : (d + 1) * ne, :] for d in face_dofs]
    lane = lax.broadcasted_iota(jnp.int32, (ne, lanes), 1)
    packed = jnp.zeros((ne, lanes), f32)
    for t, value in enumerate(summed):
        packed = jnp.where(lane == t, value, packed)
    coef[...] = packed
    send(coef, coef_in, (0, 1, 0), 4, 7)

    def homes(comp, axis, low, high):
        found = []
        for el in range(counts[axis]):
            first = max(low, ORDER * el)
            last = min(high, ORDER * el + dims_of(comp)[axis])
            if first < last:
                found.append((el, first - ORDER * el, first - low, last - first))
        return found

    def places(comp, axis, at, low, high):
        dims = dims_of(comp)
        steps = (dims[1] * dims[2], dims[2], 1)
        span = [(p, p + 1) for p in at]
        span[axis] = (low, high)
        for fx in homes(comp, 0, *span[0]):
            for fy in homes(comp, 1, *span[1]):
                for fz in homes(comp, 2, *span[2]):
                    found = (fx, fy, fz)
                    e = (fx[0] * cy + fy[0]) * cz + fz[0]
                    d = comp * 48 + sum(found[t][1] * steps[t] for t in range(3))
                    yield found[axis][2], found[axis][3], d * ne + e, steps[axis] * ne

    def put(comp, axis, at, low, high, load):
        for offset, length, row, stride in places(comp, axis, at, low, high):
            elem[pl.ds(row, length, stride=stride), :] = load(offset, offset + length)

    def face_places(comp, x, low, high, layer=cy - 1):
        for fx in homes(comp, 0, x, x + 1):
            for fz in homes(comp, 2, low, high):
                e = (fx[0] * cy + layer) * cz + fz[0]
                d = comp // 2 * 12 + fx[1] * dims_of(comp)[2] + fz[1]
                yield fz[2], fz[3], d * ne + e

    def put_face(ref, comp, x, low, high, load):
        for offset, length, row in face_places(comp, x, low, high):
            ref[pl.ds(row, length, stride=ne), :] = load(offset, offset + length)

    blank = jnp.zeros((ne, lanes), f32)
    for t, d in enumerate(face_dofs):
        elem[d * ne : (d + 1) * ne, :] = blank
        face[t * ne : (t + 1) * ne, :] = blank
        face_own[t * ne : (t + 1) * ne, :] = blank
    for comp in range(3):
        for x in range(size[0]):
            for y in range(size[1]):
                put(comp, 2, (x, y, 0), 0, size[2], lambda a, b: vec[comp, x, y, a:b, :])
    for comp in (0, 2):
        for x in range(size[0]):
            put_face(face_own, comp, x, 0, size[2], lambda a, b: vec[comp, x, 0, a:b, :])
    results = (res_x, res_y, res_z)
    for res in (top_x, top_z, low_x, low_z) + results:
        res[...] = jnp.zeros_like(res)

    pl.semaphore_wait(ready, 5)
    send(corner1.at[0], hc.at[1], (0, -1, -1), 2, 6)
    send(vec.at[2, 0, 0], hc.at[2], (-1, -1, 0), 2, 6)
    send(vec.at[0, :, 0], hy.at[0], (0, -1, 0), 3, 5)
    send(vec.at[2, :, 0], hy.at[1], (0, -1, 0), 3, 5)

    def take_halo(comp):
        if comp == 1:
            arrived(hc.at[0], 2)
            arrived(hx.at[0], 3)
            arrived(hz.at[1], 4)
            for y in range(size[1]):
                put(1, 2, (size[0], y, 0), 0, size[2], lambda a, b: hx[0, y, a:b, :])
            for x in range(size[0]):
                put(1, 1, (x, 0, size[2]), 0, size[1], lambda a, b: hz[1, x, a:b, :])
            put(1, 1, (size[0], 0, size[2]), 0, size[1], lambda a, b: hc[0, a:b, :])
        elif comp == 0:
            arrived(hz.at[0], 1)
            for x in range(size[0]):
                put(0, 1, (x, 0, size[2]), 0, size[1], lambda a, b: hz[0, x, a:b, :])
                put_face(face_own, 0, x, size[2], size[2] + 1, lambda a, b: hz[0, x, 0:1, :])
        else:
            arrived(hx.at[1], 0)
            for y in range(size[1]):
                put(2, 2, (size[0], y, 0), 0, size[2], lambda a, b: hx[1, y, a:b, :])
            put_face(face_own, 2, size[0], 0, size[2], lambda a, b: hx[1, 0, a:b, :])

    def rows_of(axis, at, line, dims):
        others = [t for t in range(3) if t != axis]
        points = []
        for last in range(dims[others[1]]):
            index = [0, 0, 0]
            index[axis], index[others[0]], index[others[1]] = at, line, last
            points.append(((index[0] * dims[1] + index[1]) * dims[2] + index[2]) * ne)
        return points

    def load_line(ref, base, axis, at, line, dims):
        starts = [base + r for r in rows_of(axis, at, line, dims)]
        if len(starts) > 1 and starts[1] - starts[0] == ne:
            return ref[starts[0] : starts[-1] + ne, :]
        return jnp.concatenate([ref[s : s + ne, :] for s in starts], 0)

    def load_plane(ref, base, axis, at, dims):
        others = [t for t in range(3) if t != axis]
        return [load_line(ref, base, axis, at, p, dims) for p in range(dims[others[0]])]

    def store_plane(ref, base, axis, at, dims, blocks):
        for p, block in enumerate(blocks):
            starts = [base + r for r in rows_of(axis, at, p, dims)]
            if starts[1] - starts[0] == ne:
                ref[starts[0] : starts[-1] + ne, :] = block
            else:
                for t, s in enumerate(starts):
                    ref[s : s + ne, :] = block[t * ne : (t + 1) * ne]

    full = [QUAD] * 3

    def mid_dims(comp):
        return [ORDER if axis == comp else QUAD for axis in range(3)]

    def evaluate(comp):
        take_halo(comp)
        dims = dims_of(comp)
        base = comp * 48 * ne
        for a in range(ORDER):
            plane = load_plane(elem, base, comp, a, dims)
            signs = load_plane(sign, base, comp, a, dims)
            plane = [p * s for p, s in zip(plane, signs)]
            plane = apply(CLOSED, plane)
            plane = apply(CLOSED, swap(plane, ne))
            store_plane(tmp, base, comp, a, mid_dims(comp), swap(plane, ne))
        others = [t for t in range(3) if t != comp]
        for line in range(QUAD):
            xs = [load_line(tmp, base, comp, a, line, mid_dims(comp)) for a in range(ORDER)]
            for q, y in enumerate(apply(OPENED, xs)):
                starts = [comp * 64 * ne + r for r in rows_of(comp, q, line, full)]
                if starts[1] - starts[0] == ne:
                    uq[starts[0] : starts[-1] + ne, :] = y
                else:
                    for t, s in enumerate(starts):
                        uq[s : s + ne, :] = y[t * ne : (t + 1) * ne]

    part = 64 * ne

    def half_turn(c, axis, at):
        other = 3 - c - axis
        u = load_plane(uq, other * part, c, at, full)
        if axis < other:
            return apply(COLLOC, u, -1)
        return swap(apply(COLLOC, swap(u, ne), -1), ne)

    def turn_of(c, axis, kept):
        plus = (axis - c) % 3 == 1
        for at in range(QUAD):
            one = half_turn(c, axis, at)
            if kept:
                two = load_plane(cq, c * part, c, at, full)
            else:
                two = half_turn(c, 3 - c - axis, at)
            both = [a - b if plus else b - a for a, b in zip(one, two)]
            scale = load_plane(curlw, 0, c, at, full)
            store_plane(cq, c * part, c, at, full, [k * w for k, w in zip(both, scale)])

    evaluate(2)
    evaluate(0)
    turn_of(1, 2, False)
    for c in (0, 2):
        for at in range(QUAD):
            store_plane(cq, c * part, c, at, full, half_turn(c, 1, at))
    evaluate(1)
    turn_of(0, 2, True)
    turn_of(2, 0, True)

    closed_t, opened_t, colloc_t = CLOSED.T, OPENED.T, COLLOC.T
    packs = (pack2_x, pack2_y)
    near = (near_x, near_y, near_z)
    last = (last_x, last_y, last_z)
    orders = ((0, 1, 2), (0, 1, 2), (0, 2, 1))

    def face_values(ref, signs):
        at = [ref[t * ne : (t + 1) * ne, :] * signs[t] for t in range(24)]
        xs = [jnp.concatenate([at[a * 4 + c] for a in range(3)], 0) for c in range(4)]
        u_x = apply(OPENED, swap(apply(CLOSED, xs), ne))
        xs = [jnp.concatenate([at[12 + a * 3 + c] for c in range(3)], 0) for a in range(4)]
        u_z = swap(apply(OPENED, swap(apply(CLOSED, xs), ne)), ne)
        along_z = swap(apply(COLLOC, swap(u_x, ne), -1), ne)
        along_x = apply(COLLOC, u_z, -1)
        return u_x, u_z, [f - g for f, g in zip(along_z, along_x)]

    def face_gradient(v_x, v_z, b, signs):
        by_z = swap(apply(colloc_t, swap(b, ne), -1), ne)
        by_x = apply(colloc_t, b, -1)
        v_x = [v + f for v, f in zip(v_x, by_z)]
        v_z = [v - f for v, f in zip(v_z, by_x)]
        for c, block in enumerate(apply(closed_t, swap(apply(opened_t, v_x), ne))):
            for a, y in enumerate(pieces_of(block)):
                t = a * 4 + c
                face_out[t * ne : (t + 1) * ne, :] = y * signs[t]
        for c, block in enumerate(apply(opened_t, swap(apply(closed_t, v_z), ne))):
            for a, y in enumerate(pieces_of(block)):
                t = 12 + a * 3 + c
                face_out[t * ne : (t + 1) * ne, :] = y * signs[t]

    def plane_fields(values, slopes):
        v_x, v_z, b = [], [], []
        for qx in range(QUAD):
            t_x, t_z, t_b = [], [], []
            for qy in range(QUAD):
                m = quad_rows(mass, 0, qx, qy) * np.float32(values[qy])
                slope = np.float32(slopes[qy])
                t_x += [m * quad_rows(uq, 0, qx, qy), -slope * quad_rows(cq, 2 * part, qx, qy)]
                t_z += [m * quad_rows(uq, 2 * part, qx, qy), slope * quad_rows(cq, 0, qx, qy)]
                t_b += [np.float32(values[qy]) * quad_rows(cq, part, qx, qy)]
            v_x.append(add_all(t_x))
            v_z.append(add_all(t_z))
            b.append(add_all(t_b))
        return v_x, v_z, b

    def signs_of(dofs):
        return [sign[d * ne : (d + 1) * ne, :] for d in dofs]

    def pack_corner(comp, slot, load):
        for t in range(size[comp]):
            corner2[4 * comp + slot, t : t + 1, :] = load(t)

    def send_corner(comp, shift, slot):
        where = 4 * comp + slot
        send(corner2.at[where], rc.at[where], shift, 5 + comp, 8 + comp)

    def make_plane(side, plane_x, plane_z):
        b, layer = side * ORDER, side * (cy - 1)
        fields = plane_fields(CLOSED[:, b], COLLOC @ CLOSED[:, b])
        face_gradient(*fields, signs_of(plane_dofs(b)))
        for comp, plane in ((0, plane_x), (2, plane_z)):
            for x in range(plane.shape[0]):
                for offset, length, row in face_places(comp, x, 0, plane.shape[1], layer):
                    plane[x, offset : offset + length, :] += face_out[
                        pl.ds(row, length, stride=ne), :
                    ]
        for s in (0, 1):
            z, x = s * size[2], s * size[0]
            pack_corner(0, 2 * side + s, lambda t: plane_x[t, z : z + 1, :])
            pack_corner(2, 2 * s + side, lambda t: plane_z[x, t : t + 1, :])

    def send_plane(side, plane_x, plane_z):
        way = 2 * side - 1
        for s in (0, 1):
            send_corner(0, (0, way, 2 * s - 1), 2 * side + s)
            send_corner(2, (2 * s - 1, way, 0), 2 * s + side)
        send(plane_x, near_x.at[side], (0, way, 0), 8, 11)
        send(plane_z, last_z.at[side], (0, way, 0), 13, 16)

    far = me[1] == mesh_sizes[1] - 1
    make_plane(1, top_x, top_z)

    @pl.when(far)
    def _():
        send_plane(1, top_x, top_z)

    if cy > 1:
        make_plane(0, low_x, low_z)

    arrived(hy, 5)
    arrived(hc.at[1:3], 6)
    if cy > 1:
        send_plane(0, low_x, low_z)
    for x in range(size[0]):
        put_face(face, 0, x, 0, size[2], lambda a, b: hy[0, x, a:b, :])
        put_face(face, 0, x, size[2], size[2] + 1, lambda a, b: hc[1, x : x + 1, :])
        put_face(face, 2, x, 0, size[2], lambda a, b: hy[1, x, a:b, :])
    put_face(face, 2, size[0], 0, size[2], lambda a, b: hc[2, a:b, :])
    own_signs = signs_of(face_dofs)
    u_x, u_z, turn = face_values(face, own_signs)
    for qx in range(QUAD):
        for qy in range(QUAD):
            first = (qx * 16 + qy * 4) * ne
            value, slope = np.float32(line_c[qy]), np.float32(line_s[qy])
            w = curlw[first : first + 4 * ne, :]
            sloped = w * slope
            uq[first : first + 4 * ne, :] += value * u_x[qx]
            uq[2 * part + first : 2 * part + first + 4 * ne, :] += value * u_z[qx]
            cq[first : first + 4 * ne, :] += sloped * u_z[qx]
            cq[part + first : part + first + 4 * ne, :] += (w * value) * turn[qx]
            cq[2 * part + first : 2 * part + first + 4 * ne, :] -= sloped * u_x[qx]

    if cy == 1:
        make_plane(0, low_x, low_z)
        send_plane(0, low_x, low_z)

    for comp in (1, 2, 0):
        if comp == 2:
            arrived(coef_in, 7)
            theirs = [
                jnp.broadcast_to(coef_in[:, t : t + 1], (ne, lanes)) for t in range(56)
            ]
            u_x, u_z, turn = face_values(face_own, theirs[32:])
            m2 = [jnp.concatenate(theirs[4 * qx : 4 * qx + 4], 0) for qx in range(QUAD)]
            k2 = [jnp.concatenate(theirs[16 + 4 * qx : 20 + 4 * qx], 0) for qx in range(QUAD)]
            face_gradient(
                [m * u for m, u in zip(m2, u_x)], [m * u for m, u in zip(m2, u_z)],
                [k * u for k, u in zip(k2, turn)], theirs[32:],
            )
        dims = dims_of(comp)
        base = comp * 48 * ne
        p, r = [t for t in range(3) if t != comp]
        for at in range(QUAD):
            u = load_plane(uq, comp * part, comp, at, full)
            m = load_plane(mass, 0, comp, at, full)
            total = [a * b for a, b in zip(u, m)]
            by_p = apply(colloc_t, load_plane(cq, r * part, comp, at, full), -1)
            by_r = apply(colloc_t, swap(load_plane(cq, p * part, comp, at, full), ne), -1)
            by_r = swap(by_r, ne)
            if comp == 1:
                total = [t + a - b for t, a, b in zip(total, by_p, by_r)]
            else:
                total = [t - a + b for t, a, b in zip(total, by_p, by_r)]
            total = apply(closed_t, total)
            total = apply(closed_t, swap(total, ne))
            kept = [QUAD if axis == comp else ORDER + 1 for axis in range(3)]
            store_plane(tmp, 0, comp, at, kept, swap(total, ne))
        for line in range(ORDER + 1):
            xs = [load_line(tmp, 0, comp, q, line, kept) for q in range(QUAD)]
            for a, y in enumerate(apply(opened_t, xs)):
                y = y * load_line(sign, base, comp, a, line, dims)
                for t, s in enumerate(rows_of(comp, a, line, dims)):
                    elem[base + s : base + s + ne, :] = y[t * ne : (t + 1) * ne]
        res = results[comp]
        order = orders[comp]
        for first in range(res.shape[0]):
            for middle in range(res.shape[1]):
                at = [0, 0, 0]
                at[order[0]], at[order[1]] = first, middle
                pieces = places(comp, order[2], at, 0, res.shape[2])
                for offset, length, row, stride in pieces:
                    res[first, middle, offset : offset + length, :] += elem[
                        pl.ds(row, length, stride=stride), :
                    ]
        if comp == 0:
            for x in range(size[0]):
                for offset, length, row in face_places(0, x, 0, res.shape[2]):
                    res[x, 0, offset : offset + length, :] += face_out[
                        pl.ds(row, length, stride=ne), :
                    ]
        elif comp == 1:
            for s_x in (0, 1):
                for s_z in (0, 1):
                    x, z = s_x * size[0], s_z * size[2]
                    pack_corner(1, 2 * s_x + s_z, lambda t: res[x, t, z : z + 1, :])
                    send_corner(1, (2 * s_x - 1, 0, 2 * s_z - 1), 2 * s_x + s_z)
        else:
            for x in range(res.shape[0]):
                for offset, length, row in face_places(2, x, 0, res.shape[1]):
                    for t in range(length):
                        res[x, offset + t, 0:1, :] += face_out[row + t * ne : row + t * ne + 1, :]
        if comp > 0:
            for side in (0, 1):
                send(
                    res.at[side * size[0]], near[comp].at[side], (2 * side - 1, 0, 0),
                    8 + comp, 11 + comp,
                )
        if comp < 2:
            for side in (0, 1):
                row = side * size[2]
                for f in range(res.shape[0]):
                    for m in range(res.shape[1]):
                        packs[comp][side, f, m : m + 1, :] = res[f, m, row : row + 1, :]
                send(
                    packs[comp].at[side], last[comp].at[side], (0, 0, 2 * side - 1),
                    11 + comp, 14 + comp,
                )
        if comp == 1:

            @pl.when(jnp.logical_not(far))
            def _():
                send_plane(1, top_x, top_z)

    outs = (out_x, out_y, out_z)
    for comp in range(3):
        outs[comp][...] = results[comp][...]
    for comp in (1, 0, 2):
        out, order = outs[comp], orders[comp]
        rim = order[1] if comp == 0 else order[0]
        arrived(rc.at[4 * comp : 4 * comp + 4], 8 + comp)
        arrived(near[comp], 11 + comp)
        arrived(last[comp], 14 + comp)
        for side in (0, 1):
            edge = (1 - side) * size[rim]
            row = (1 - side) * size[order[2]]
            if comp == 0:
                for f in range(out.shape[0]):
                    out[f, edge] += near[comp][side, f]
            else:
                out[edge] += near[comp][side]
            for f in range(out.shape[0]):
                for m in range(out.shape[1]):
                    out[f, m, row : row + 1, :] += last[comp][side, f, m : m + 1, :]
            for s_last in (0, 1):
                where = 4 * comp + 2 * side + s_last
                row = (1 - s_last) * size[order[2]]
                for t in range(size[comp]):
                    f, m = (t, edge) if comp == 0 else (edge, t)
                    out[f, m, row : row + 1, :] += rc[where, t : t + 1, :]
    for out, ref in enumerate((hx, hz, hc, hy, coef)):
        left(ref, out)
    for comp in range(3):
        left(rc.at[4 * comp : 4 * comp + 4], 5 + comp)
        left(near[comp], 8 + comp)
        left(last[comp], 11 + comp)


def write_out(from_x, from_y, from_z, to_x, to_y, to_z, sems):
    pairs = ((from_x, to_x), (from_y, to_y), (from_z, to_z))
    copies = [pltpu.make_async_copy(src, dst, sems.at[t]) for t, (src, dst) in enumerate(pairs)]
    for copy in copies:
        copy.start()
    for copy in copies:
        copy.wait()


def on_device(mesh_sizes, vectors, orient_flip, reluctivity, conductivity):
    counts = (
        orient_flip.shape[0], orient_flip.shape[1], orient_flip.shape[2] // ELEM_DOFS,
    )
    ne = counts[0] * counts[1] * counts[2]
    sx, sy, sz = (ORDER * c for c in counts)
    lanes = vectors.shape[-1]
    f32 = jnp.float32
    shapes = (
        (sx, sy + 1, sz + 1, lanes), (sx + 1, sy, sz + 1, lanes), (sx + 1, sz, sy + 1, lanes),
    )
    longest = max(sx, sy, sz)
    faces = tuple((2,) + s[:2] + (lanes,) for s in shapes)
    scratch = [
        (ELEM_DOFS * ne, lanes), (ELEM_DOFS * ne, lanes), (QPTS * ne, lanes), (QPTS * ne, lanes),
        (3, ne, ELEM_DOFS), (ELEM_DOFS * ne, lanes), (3 * QPTS * ne, lanes), (3 * QPTS * ne, lanes),
        *shapes,
        (2, sx, sy, lanes), (2, longest, lanes),
        (2, sy, sz, lanes), (2, sx, sz, lanes), (2, sx, sy, lanes), (3, longest, lanes),
        *faces[:2], (12, longest, lanes),
        (2, sx, sz + 1, lanes), (2, sy, sz + 1, lanes), (2, sz, sy + 1, lanes),
        *faces, (12, longest, lanes),
        (24 * ne, lanes), (24 * ne, lanes), (24 * ne, lanes), (ne, lanes), (ne, lanes),
        (sx, sz + 1, lanes), (sx + 1, sz, lanes), (sx, sz + 1, lanes), (sx + 1, sz, lanes),
    ]
    vmem = pl.BlockSpec(memory_space=pltpu.VMEM)
    padded = [s[0] * s[1] * (s[2] + -s[2] % 8) * lanes * 4 for s in shapes]
    room = sum(padded) + max(padded)
    anywhere = pl.BlockSpec(memory_space=pltpu.HBM)
    arguments = (vectors, orient_flip, reluctivity, conductivity)
    outs = [jax.ShapeDtypeStruct(s, f32) for s in shapes]
    held = pl.pallas_call(
        functools.partial(kernel, mesh_sizes),
        out_shape=[pltpu.VMEM(s, f32) for s in shapes],
        in_specs=[anywhere] * 4,
        out_specs=[vmem] * 3,
        scratch_shapes=[pltpu.VMEM(a.shape, a.dtype) for a in arguments]
        + [pltpu.VMEM(s, f32) for s in scratch]
        + [pltpu.SemaphoreType.DMA((14,)), pltpu.SemaphoreType.DMA((17,))]
        + [pltpu.SemaphoreType.DMA((4,)), pltpu.SemaphoreType.REGULAR],
        compiler_params=pltpu.CompilerParams(
            collective_id=0, has_side_effects=True, vmem_limit_bytes=VMEM_ALL - room
        ),
        name="curl_mass",
    )(*arguments)
    held = pl.pallas_call(
        write_out,
        out_shape=outs,
        in_specs=[pl.BlockSpec(memory_space=pl.ANY)] * 3,
        out_specs=[anywhere] * 3,
        scratch_shapes=[pltpu.SemaphoreType.DMA((3,))],
        compiler_params=pltpu.CompilerParams(vmem_limit_bytes=2**20),
        name="write_out",
    )(*held)
    return held[0], held[1], jnp.swapaxes(held[2], 1, 2)


def solution(mesh):
    return jax.shard_map(
        functools.partial(on_device, tuple(mesh.shape[a] for a in AXES)),
        mesh=mesh,
        in_specs=(
            P(None, "gx", "gy", "gz", None),
            P("gx", "gy", "gz"),
            P("gx", "gy", "gz"),
            P("gx", "gy", "gz"),
        ),
        out_specs=(P("gx", "gy", "gz", None), P("gx", "gy", "gz", None), P("gx", "gy", "gz", None)),
        check_vma=False,
    )
```

```python
import functools
import jax
import jax.numpy as jnp
import numpy as np
from jax import lax
from jax.experimental import pallas as pl
from jax.experimental.pallas import tpu as pltpu
from jax.sharding import PartitionSpec as P

ORDER = 3
QUAD = 4
ELEM_DOFS = 144
QPTS = 64
AXES = ("gx", "gy", "gz")
MESH = pl.DeviceIdType.MESH
VMEM_ALL = 67043328


def lagrange(points_at, evaluate_at):
    amount = len(points_at)
    values = np.ones((len(evaluate_at), amount))
    slopes = np.zeros((len(evaluate_at), amount))
    for which in range(amount):
        for column in range(amount):
            if column != which:
                factor = (evaluate_at - points_at[column]) / (points_at[which] - points_at[column])
                slopes[:, which] = slopes[:, which] * factor + values[:, which] / (
                    points_at[which] - points_at[column]
                )
                values[:, which] = values[:, which] * factor
    return (values, slopes)


def basis_tables():
    lobatto = np.array([0.0, (1 - 5 ** (-0.5)) / 2, (1 + 5 ** (-0.5)) / 2, 1.0])
    gauss_open = np.array([(1 - 0.6**0.5) / 2, 0.5, (1 + 0.6**0.5) / 2])
    inner_pt = (3.0 / 7 - 2.0 / 7 * (6.0 / 5) ** 0.5) ** 0.5
    outer_pt = (3.0 / 7 + 2.0 / 7 * (6.0 / 5) ** 0.5) ** 0.5
    inner_wt = (18 + 30**0.5) / 36
    outer_wt = (18 - 30**0.5) / 36
    quad_points = (1 + np.array([-outer_pt, -inner_pt, inner_pt, outer_pt])) / 2
    quad_weight = np.array([outer_wt, inner_wt, inner_wt, outer_wt]) / 2
    closed, _ = lagrange(lobatto, quad_points)
    opened, _ = lagrange(gauss_open, quad_points)
    _, colloc = lagrange(quad_points, quad_points)
    return closed, opened, colloc, quad_weight


CLOSED, OPENED, COLLOC, WEIGHT = basis_tables()


def add_all(terms):
    total = terms[0]
    for term in terms[1:]:
        total = total + term
    return total


def apply(mat, xs, sigma=1):
    rows, cols = mat.shape
    half = cols // 2
    plus = [xs[p] + xs[cols - 1 - p] for p in range(half)]
    minus = [xs[p] - xs[cols - 1 - p] for p in range(half)]
    ys = [None] * rows
    for q in range((rows + 1) // 2):
        even_c = [(mat[q, p] + mat[q, cols - 1 - p]) / 2 for p in range(half)]
        odd_c = [(mat[q, p] - mat[q, cols - 1 - p]) / 2 for p in range(half)]
        even = [np.float32(c) * s for c, s in zip(even_c, plus)]
        if cols % 2:
            even.append(np.float32(mat[q, half]) * xs[half])
        even = add_all(even)
        if 2 * q == rows - 1:
            ys[q] = even
            continue
        odd = add_all([np.float32(c) * d for c, d in zip(odd_c, minus)])
        ys[q] = even + odd
        ys[rows - 1 - q] = even - odd if sigma > 0 else odd - even
    return ys


def swap(blocks, size):
    count = blocks[0].shape[0] // size
    return [
        jnp.concatenate([b[q * size : (q + 1) * size] for b in blocks], 0) for q in range(count)
    ]


def dims_of(comp):
    return [ORDER if axis == comp else ORDER + 1 for axis in range(3)]


def kernel(
    mesh_sizes, vec_hbm, flip_hbm, reluct_hbm, conduct_hbm, out_x, out_y, out_z,
    vec, flip, reluct, conduct, elem, sign, mass, curlw, flat, tmp, uq, cq,
    res_x, res_y, res_z, pack1, corner1, hx, hy, hz, hc, pack2_x, pack2_y, corner2,
    near_x, near_y, near_z, last_x, last_y, last_z, rc,
    face, face_own, face_out, coef, coef_in, top_x, top_z, low_x, low_z,
    edge_out, edge_in, sent, came, s0, ready,
):
    f32 = jnp.float32
    cx, cy = flip.shape[0], flip.shape[1]
    cz = flip.shape[2] // ELEM_DOFS
    counts = (cx, cy, cz)
    ne = cx * cy * cz
    size = tuple(ORDER * c for c in counts)
    lanes = vec.shape[-1]
    me = [lax.axis_index(a) for a in AXES]

    def device(shift):
        return tuple(
            lax.rem(me[a] + (shift[a] + mesh_sizes[a]), mesh_sizes[a]) for a in range(3)
        )

    def signal(sem, shift):
        pl.semaphore_signal(sem, inc=1, device_id=device(shift), device_id_type=MESH)

    fetches = [
        pltpu.make_async_copy(src, dst, s0.at[t])
        for t, (src, dst) in enumerate(
            ((vec_hbm, vec), (flip_hbm, flip), (reluct_hbm, reluct), (conduct_hbm, conduct))
        )
    ]
    for fetch in fetches:
        fetch.start()
    barrier = pltpu.get_barrier_semaphore()
    first, final = me[1] == 0, me[1] == mesh_sizes[1] - 1
    above = ((0, 1, 0), (1, 1, 0), (-1, 1, 0), (0, 1, 1), (0, 1, -1))
    greeted = ((1, 0, 0), (0, 0, 1), (1, 0, 1)) + tuple((s[0], -1, s[2]) for s in above)
    for shift in greeted:
        signal(barrier, shift)

    @pl.when(jnp.logical_not(final))
    def _():
        for shift in above:
            signal(barrier, shift)

    fetches[0].wait()
    for comp in (0, 1):
        for x in range(size[0]):
            for y in range(size[1]):
                pack1[comp, x, y : y + 1, :] = vec[comp, x, y, 0:1, :]
    for x in range(size[0]):
        corner1[0, x : x + 1, :] = vec[0, x, 0, 0:1, :]
    for y in range(size[1]):
        corner1[1, y : y + 1, :] = vec[1, 0, y, 0:1, :]
    pl.semaphore_wait(barrier, len(greeted) + jnp.where(first, 0, len(above)))

    def remote(src, dst, shift, out, into):
        return pltpu.make_async_remote_copy(
            src_ref=src, dst_ref=dst, send_sem=sent.at[out], recv_sem=came.at[into],
            device_id=device(shift), device_id_type=MESH,
        )

    def send(src, dst, shift, out, into):
        remote(src, dst, shift, out, into).start()

    def arrived(rows, into):
        remote(elem.at[0:rows], elem.at[0:rows], (0, 1, 0), 0, into).wait_recv()

    send(vec.at[2, 0], hx.at[1], (-1, 0, 0), 0, 0)
    send(pack1.at[0], hz.at[0], (0, 0, -1), 0, 1)
    send(corner1.at[1], hc.at[0], (-1, 0, -1), 0, 2)
    send(vec.at[1, 0], hx.at[0], (-1, 0, 0), 0, 2)
    send(pack1.at[1], hz.at[1], (0, 0, -1), 0, 2)

    @pl.when(final)
    def _():
        for shift in above:
            signal(ready, shift)

    def send_down():
        send(corner1.at[0], hc.at[1], (0, -1, -1), 0, 3)
        send(vec.at[2, 0, 0], hc.at[2], (-1, -1, 0), 0, 3)
        send(vec.at[0, :, 0], hy.at[0], (0, -1, 0), 0, 3)
        send(vec.at[2, :, 0], hy.at[1], (0, -1, 0), 0, 3)

    pl.when(jnp.logical_not(first))(send_down)

    for fetch in fetches[1:]:
        fetch.wait()
    for i in range(cx):
        for j in range(cy):
            for k in range(cz):
                e = (i * cy + j) * cz + k
                flat[0, e : e + 1, 0:ELEM_DOFS] = 1.0 - 2.0 * flip[
                    i, j : j + 1, k * ELEM_DOFS : (k + 1) * ELEM_DOFS
                ].astype(f32)
                flat[1, e : e + 1, 0:QPTS] = reluct[i, j : j + 1, k * QPTS : (k + 1) * QPTS]
                flat[2, e : e + 1, 0:QPTS] = conduct[i, j : j + 1, k * QPTS : (k + 1) * QPTS]
    for d in range(ELEM_DOFS):
        sign[d * ne : (d + 1) * ne, :] = jnp.broadcast_to(flat[0, :, d : d + 1], (ne, lanes))
    for q in range(QPTS):
        w = np.float32(WEIGHT[q // 16] * WEIGHT[q // 4 % 4] * WEIGHT[q % 4])
        rows = slice(q * ne, (q + 1) * ne)
        curlw[rows, :] = jnp.broadcast_to(flat[1, :, q : q + 1] * w, (ne, lanes))
        mass[rows, :] = jnp.broadcast_to(flat[2, :, q : q + 1] * w, (ne, lanes))

    line_c, line_s = CLOSED[:, ORDER], COLLOC @ CLOSED[:, ORDER]

    def plane_dofs(b):
        found = [(a * 4 + b) * 4 + c for a in range(3) for c in range(4)]
        return found + [96 + (a * 4 + b) * 3 + c for a in range(4) for c in range(3)]

    face_dofs = plane_dofs(ORDER)

    def quad_rows(ref, base, qx, qy):
        first = base + (qx * 16 + qy * 4) * ne
        return ref[first : first + 4 * ne, :]

    def pieces_of(block):
        return [block[t * ne : (t + 1) * ne] for t in range(block.shape[0] // ne)]

    summed = []
    for qx in range(QUAD):
        summed += pieces_of(add_all(
            [np.float32(line_c[qy] ** 2) * quad_rows(mass, 0, qx, qy) for qy in range(QUAD)]
            + [np.float32(line_s[qy] ** 2) * quad_rows(curlw, 0, qx, qy) for qy in range(QUAD)]
        ))
    for qx in range(QUAD):
        summed += pieces_of(add_all(
            [np.float32(line_c[qy] ** 2) * quad_rows(curlw, 0, qx, qy) for qy in range(QUAD)]
        ))
    summed += [sign[d * ne : (d + 1) * ne, :] for d in face_dofs]
    lane = lax.broadcasted_iota(jnp.int32, (ne, lanes), 1)
    packed = jnp.zeros((ne, lanes), f32)
    for t, value in enumerate(summed):
        packed = jnp.where(lane == t, value, packed)
    coef[...] = packed
    send(coef, coef_in, (0, 1, 0), 0, 4)

    def homes(comp, axis, low, high):
        found = []
        for el in range(counts[axis]):
            first = max(low, ORDER * el)
            last = min(high, ORDER * el + dims_of(comp)[axis])
            if first < last:
                found.append((el, first - ORDER * el, first - low, last - first))
        return found

    def places(comp, axis, at, low, high):
        dims = dims_of(comp)
        steps = (dims[1] * dims[2], dims[2], 1)
        span = [(p, p + 1) for p in at]
        span[axis] = (low, high)
        for fx in homes(comp, 0, *span[0]):
            for fy in homes(comp, 1, *span[1]):
                for fz in homes(comp, 2, *span[2]):
                    found = (fx, fy, fz)
                    e = (fx[0] * cy + fy[0]) * cz + fz[0]
                    d = comp * 48 + sum(found[t][1] * steps[t] for t in range(3))
                    yield found[axis][2], found[axis][3], d * ne + e, steps[axis] * ne

    def put(comp, axis, at, low, high, load):
        for offset, length, row, stride in places(comp, axis, at, low, high):
            elem[pl.ds(row, length, stride=stride), :] = load(offset, offset + length)

    def face_places(comp, x, low, high, layer=cy - 1):
        for fx in homes(comp, 0, x, x + 1):
            for fz in homes(comp, 2, low, high):
                e = (fx[0] * cy + layer) * cz + fz[0]
                d = comp // 2 * 12 + fx[1] * dims_of(comp)[2] + fz[1]
                yield fz[2], fz[3], d * ne + e

    def put_face(ref, comp, x, low, high, load):
        for offset, length, row in face_places(comp, x, low, high):
            ref[pl.ds(row, length, stride=ne), :] = load(offset, offset + length)

    blank = jnp.zeros((ne, lanes), f32)
    for t, d in enumerate(face_dofs):
        elem[d * ne : (d + 1) * ne, :] = blank
        face[t * ne : (t + 1) * ne, :] = blank
        face_own[t * ne : (t + 1) * ne, :] = blank
    for comp in range(3):
        for x in range(size[0]):
            for y in range(size[1]):
                put(comp, 2, (x, y, 0), 0, size[2], lambda a, b: vec[comp, x, y, a:b, :])
    for comp in (0, 2):
        for x in range(size[0]):
            put_face(face_own, comp, x, 0, size[2], lambda a, b: vec[comp, x, 0, a:b, :])
    results = (res_x, res_y, res_z)
    for res in (top_x, top_z, low_x, low_z) + results:
        res[...] = jnp.zeros_like(res)

    @pl.when(first)
    def _():
        pl.semaphore_wait(ready, len(above))
        send_down()

    def take_halo(comp):
        if comp == 1:
            arrived(hc.shape[1] + size[1] * size[2] + size[0] * size[1], 2)
            for y in range(size[1]):
                put(1, 2, (size[0], y, 0), 0, size[2], lambda a, b: hx[0, y, a:b, :])
            for x in range(size[0]):
                put(1, 1, (x, 0, size[2]), 0, size[1], lambda a, b: hz[1, x, a:b, :])
            put(1, 1, (size[0], 0, size[2]), 0, size[1], lambda a, b: hc[0, a:b, :])
        elif comp == 0:
            arrived(size[0] * size[1], 1)
            for x in range(size[0]):
                put(0, 1, (x, 0, size[2]), 0, size[1], lambda a, b: hz[0, x, a:b, :])
                put_face(face_own, 0, x, size[2], size[2] + 1, lambda a, b: hz[0, x, 0:1, :])
        else:
            arrived(size[1] * size[2], 0)
            for y in range(size[1]):
                put(2, 2, (size[0], y, 0), 0, size[2], lambda a, b: hx[1, y, a:b, :])
            put_face(face_own, 2, size[0], 0, size[2], lambda a, b: hx[1, 0, a:b, :])

    def rows_of(axis, at, line, dims):
        others = [t for t in range(3) if t != axis]
        points = []
        for last in range(dims[others[1]]):
            index = [0, 0, 0]
            index[axis], index[others[0]], index[others[1]] = at, line, last
            points.append(((index[0] * dims[1] + index[1]) * dims[2] + index[2]) * ne)
        return points

    def load_line(ref, base, axis, at, line, dims):
        starts = [base + r for r in rows_of(axis, at, line, dims)]
        if len(starts) > 1 and starts[1] - starts[0] == ne:
            return ref[starts[0] : starts[-1] + ne, :]
        return jnp.concatenate([ref[s : s + ne, :] for s in starts], 0)

    def load_plane(ref, base, axis, at, dims):
        others = [t for t in range(3) if t != axis]
        return [load_line(ref, base, axis, at, p, dims) for p in range(dims[others[0]])]

    def store_plane(ref, base, axis, at, dims, blocks):
        for p, block in enumerate(blocks):
            starts = [base + r for r in rows_of(axis, at, p, dims)]
            if starts[1] - starts[0] == ne:
                ref[starts[0] : starts[-1] + ne, :] = block
            else:
                for t, s in enumerate(starts):
                    ref[s : s + ne, :] = block[t * ne : (t + 1) * ne]

    full = [QUAD] * 3

    def mid_dims(comp):
        return [ORDER if axis == comp else QUAD for axis in range(3)]

    def evaluate(comp):
        take_halo(comp)
        dims = dims_of(comp)
        base = comp * 48 * ne
        for a in range(ORDER):
            plane = load_plane(elem, base, comp, a, dims)
            signs = load_plane(sign, base, comp, a, dims)
            plane = [p * s for p, s in zip(plane, signs)]
            plane = apply(CLOSED, plane)
            plane = apply(CLOSED, swap(plane, ne))
            store_plane(tmp, base, comp, a, mid_dims(comp), swap(plane, ne))
        others = [t for t in range(3) if t != comp]
        for line in range(QUAD):
            xs = [load_line(tmp, base, comp, a, line, mid_dims(comp)) for a in range(ORDER)]
            for q, y in enumerate(apply(OPENED, xs)):
                starts = [comp * 64 * ne + r for r in rows_of(comp, q, line, full)]
                if starts[1] - starts[0] == ne:
                    uq[starts[0] : starts[-1] + ne, :] = y
                else:
                    for t, s in enumerate(starts):
                        uq[s : s + ne, :] = y[t * ne : (t + 1) * ne]

    part = 64 * ne

    def half_turn(c, axis, at):
        other = 3 - c - axis
        u = load_plane(uq, other * part, c, at, full)
        if axis < other:
            return apply(COLLOC, u, -1)
        return swap(apply(COLLOC, swap(u, ne), -1), ne)

    def turn_of(c, axis, kept):
        plus = (axis - c) % 3 == 1
        for at in range(QUAD):
            one = half_turn(c, axis, at)
            if kept:
                two = load_plane(cq, c * part, c, at, full)
            else:
                two = half_turn(c, 3 - c - axis, at)
            both = [a - b if plus else b - a for a, b in zip(one, two)]
            scale = load_plane(curlw, 0, c, at, full)
            store_plane(cq, c * part, c, at, full, [k * w for k, w in zip(both, scale)])

    evaluate(2)
    evaluate(0)
    turn_of(1, 2, False)
    for c in (0, 2):
        for at in range(QUAD):
            store_plane(cq, c * part, c, at, full, half_turn(c, 1, at))
    evaluate(1)
    turn_of(0, 2, True)
    turn_of(2, 0, True)

    closed_t, opened_t, colloc_t = CLOSED.T, OPENED.T, COLLOC.T
    packs = (pack2_x, pack2_y)
    near = (near_x, near_y, near_z)
    last = (last_x, last_y, last_z)
    orders = ((0, 1, 2), (0, 1, 2), (0, 2, 1))

    def face_values(ref, signs):
        at = [ref[t * ne : (t + 1) * ne, :] * signs[t] for t in range(24)]
        xs = [jnp.concatenate([at[a * 4 + c] for a in range(3)], 0) for c in range(4)]
        u_x = apply(OPENED, swap(apply(CLOSED, xs), ne))
        xs = [jnp.concatenate([at[12 + a * 3 + c] for c in range(3)], 0) for a in range(4)]
        u_z = swap(apply(OPENED, swap(apply(CLOSED, xs), ne)), ne)
        along_z = swap(apply(COLLOC, swap(u_x, ne), -1), ne)
        along_x = apply(COLLOC, u_z, -1)
        return u_x, u_z, [f - g for f, g in zip(along_z, along_x)]

    def face_gradient(v_x, v_z, b, signs):
        by_z = swap(apply(colloc_t, swap(b, ne), -1), ne)
        by_x = apply(colloc_t, b, -1)
        v_x = [v + f for v, f in zip(v_x, by_z)]
        v_z = [v - f for v, f in zip(v_z, by_x)]
        for c, block in enumerate(apply(closed_t, swap(apply(opened_t, v_x), ne))):
            for a, y in enumerate(pieces_of(block)):
                t = a * 4 + c
                face_out[t * ne : (t + 1) * ne, :] = y * signs[t]
        for c, block in enumerate(apply(opened_t, swap(apply(closed_t, v_z), ne))):
            for a, y in enumerate(pieces_of(block)):
                t = 12 + a * 3 + c
                face_out[t * ne : (t + 1) * ne, :] = y * signs[t]

    def plane_fields(values, slopes):
        v_x, v_z, b = [], [], []
        for qx in range(QUAD):
            t_x, t_z, t_b = [], [], []
            for qy in range(QUAD):
                m = quad_rows(mass, 0, qx, qy) * np.float32(values[qy])
                slope = np.float32(slopes[qy])
                t_x += [m * quad_rows(uq, 0, qx, qy), -slope * quad_rows(cq, 2 * part, qx, qy)]
                t_z += [m * quad_rows(uq, 2 * part, qx, qy), slope * quad_rows(cq, 0, qx, qy)]
                t_b += [np.float32(values[qy]) * quad_rows(cq, part, qx, qy)]
            v_x.append(add_all(t_x))
            v_z.append(add_all(t_z))
            b.append(add_all(t_b))
        return v_x, v_z, b

    def signs_of(dofs):
        return [sign[d * ne : (d + 1) * ne, :] for d in dofs]

    def pack_corner(comp, slot, load):
        for t in range(size[comp]):
            corner2[4 * comp + slot, t : t + 1, :] = load(t)

    def send_corner(comp, shift, slot):
        where = 4 * comp + slot
        send(corner2.at[where], rc.at[where], shift, 0, 8)

    def make_plane(side, plane_x, plane_z):
        b, layer = side * ORDER, side * (cy - 1)
        fields = plane_fields(CLOSED[:, b], COLLOC @ CLOSED[:, b])
        face_gradient(*fields, signs_of(plane_dofs(b)))
        for comp, plane in ((0, plane_x), (2, plane_z)):
            for x in range(plane.shape[0]):
                for offset, length, row in face_places(comp, x, 0, plane.shape[1], layer):
                    plane[x, offset : offset + length, :] += face_out[
                        pl.ds(row, length, stride=ne), :
                    ]
        for s in (0, 1):
            z, x = s * size[2], s * size[0]
            pack_corner(0, 2 * side + s, lambda t: plane_x[t, z : z + 1, :])
            pack_corner(2, 2 * s + side, lambda t: plane_z[x, t : t + 1, :])

    def send_plane(side, plane_x, plane_z):
        way = 2 * side - 1
        for s in (0, 1):
            send_corner(0, (0, way, 2 * s - 1), 2 * side + s)
            send_corner(2, (2 * s - 1, way, 0), 2 * s + side)
        send(plane_x, near_x.at[side], (0, way, 0), 0, 5)
        send(plane_z, last_z.at[side], (0, way, 0), 0, 7)

    make_plane(1, top_x, top_z)

    send_plane(1, top_x, top_z)

    if cy > 1:
        make_plane(0, low_x, low_z)
        send_plane(0, low_x, low_z)

    arrived(2 * size[0] * size[2] + 2 * hc.shape[1], 3)
    for x in range(size[0]):
        put_face(face, 0, x, 0, size[2], lambda a, b: hy[0, x, a:b, :])
        put_face(face, 0, x, size[2], size[2] + 1, lambda a, b: hc[1, x : x + 1, :])
        put_face(face, 2, x, 0, size[2], lambda a, b: hy[1, x, a:b, :])
    put_face(face, 2, size[0], 0, size[2], lambda a, b: hc[2, a:b, :])
    own_signs = signs_of(face_dofs)
    u_x, u_z, turn = face_values(face, own_signs)

    def add_rows(ref, which, qx, qy, more):
        first = which * part + (qx * 16 + qy * 4) * ne
        ref[first : first + 4 * ne, :] += more

    for qx in range(QUAD):
        for qy in range(QUAD):
            sloped = quad_rows(curlw, 0, qx, qy) * np.float32(line_s[qy])
            add_rows(cq, 0, qx, qy, sloped * u_z[qx])
            add_rows(cq, 2, qx, qy, -sloped * u_x[qx])

    if cy == 1:
        make_plane(0, low_x, low_z)
        send_plane(0, low_x, low_z)

    for comp in (1, 2, 0):
        if comp == 2:
            for qx in range(QUAD):
                for qy in range(QUAD):
                    value = np.float32(line_c[qy])
                    add_rows(uq, 0, qx, qy, value * u_x[qx])
                    add_rows(uq, 2, qx, qy, value * u_z[qx])
                    add_rows(cq, 1, qx, qy, (quad_rows(curlw, 0, qx, qy) * value) * turn[qx])
        dims = dims_of(comp)
        base = comp * 48 * ne
        p, r = [t for t in range(3) if t != comp]
        for at in range(QUAD):
            u = load_plane(uq, comp * part, comp, at, full)
            m = load_plane(mass, 0, comp, at, full)
            total = [a * b for a, b in zip(u, m)]
            by_p = apply(colloc_t, load_plane(cq, r * part, comp, at, full), -1)
            by_r = apply(colloc_t, swap(load_plane(cq, p * part, comp, at, full), ne), -1)
            by_r = swap(by_r, ne)
            if comp == 1:
                total = [t + a - b for t, a, b in zip(total, by_p, by_r)]
            else:
                total = [t - a + b for t, a, b in zip(total, by_p, by_r)]
            total = apply(closed_t, total)
            total = apply(closed_t, swap(total, ne))
            kept = [QUAD if axis == comp else ORDER + 1 for axis in range(3)]
            store_plane(tmp, 0, comp, at, kept, swap(total, ne))
        for line in range(ORDER + 1):
            xs = [load_line(tmp, 0, comp, q, line, kept) for q in range(QUAD)]
            for a, y in enumerate(apply(opened_t, xs)):
                y = y * load_line(sign, base, comp, a, line, dims)
                for t, s in enumerate(rows_of(comp, a, line, dims)):
                    elem[base + s : base + s + ne, :] = y[t * ne : (t + 1) * ne]
        res = results[comp]
        order = orders[comp]
        for first in range(res.shape[0]):
            for middle in range(res.shape[1]):
                at = [0, 0, 0]
                at[order[0]], at[order[1]] = first, middle
                pieces = places(comp, order[2], at, 0, res.shape[2])
                for offset, length, row, stride in pieces:
                    res[first, middle, offset : offset + length, :] += elem[
                        pl.ds(row, length, stride=stride), :
                    ]
        if comp == 1:
            for s_x in (0, 1):
                for s_z in (0, 1):
                    x, z = s_x * size[0], s_z * size[2]
                    pack_corner(1, 2 * s_x + s_z, lambda t: res[x, t, z : z + 1, :])
                    send_corner(1, (2 * s_x - 1, 0, 2 * s_z - 1), 2 * s_x + s_z)
        if comp > 0:
            for side in (0, 1):
                send(
                    res.at[side * size[0]], near[comp].at[side], (2 * side - 1, 0, 0),
                    0, 5 + comp,
                )
        if comp < 2:
            for side in (0, 1):
                row = side * size[2]
                for f in range(res.shape[0]):
                    for m in range(res.shape[1]):
                        packs[comp][side, f, m : m + 1, :] = res[f, m, row : row + 1, :]
                send(
                    packs[comp].at[side], last[comp].at[side], (0, 0, 2 * side - 1),
                    0, 5 + comp,
                )
    arrived(ne, 4)
    theirs = [jnp.broadcast_to(coef_in[:, t : t + 1], (ne, lanes)) for t in range(56)]
    u_x, u_z, turn = face_values(face_own, theirs[32:])
    m2 = [jnp.concatenate(theirs[4 * qx : 4 * qx + 4], 0) for qx in range(QUAD)]
    k2 = [jnp.concatenate(theirs[16 + 4 * qx : 20 + 4 * qx], 0) for qx in range(QUAD)]
    face_gradient(
        [m * u for m, u in zip(m2, u_x)], [m * u for m, u in zip(m2, u_z)],
        [k * u for k, u in zip(k2, turn)], theirs[32:],
    )
    for s in (0, 1):
        for x in range(size[0]):
            for _, _, row in face_places(0, x, s * size[2], s * size[2] + 1):
                edge_out[s, x : x + 1, :] = face_out[row : row + 1, :]
        for offset, length, row in face_places(2, s * size[0], 0, size[2]):
            edge_out[2 + s, offset : offset + length, :] = face_out[
                pl.ds(row, length, stride=ne), :
            ]
        send(edge_out.at[s], edge_in.at[s], (0, 0, 2 * s - 1), 0, 8)
        send(edge_out.at[2 + s], edge_in.at[2 + s], (2 * s - 1, 0, 0), 0, 8)

    outs = (out_x, out_y, out_z)
    for comp in range(3):
        outs[comp][...] = results[comp][...]
    for x in range(size[0]):
        for offset, length, row in face_places(0, x, 0, size[2] + 1):
            out_x[x, 0, offset : offset + length, :] += face_out[pl.ds(row, length, stride=ne), :]
    for x in range(size[0] + 1):
        for offset, length, row in face_places(2, x, 0, size[2]):
            for t in range(length):
                out_z[x, offset + t, 0:1, :] += face_out[row + t * ne : row + t * ne + 1, :]
    def rim_of(comp):
        return orders[comp][1] if comp == 0 else orders[comp][0]

    for comp in (1, 0, 2):
        out, order, rim = outs[comp], orders[comp], rim_of(comp)
        arrived(2 * size[comp] * (size[rim] + size[order[2]] + 2), 5 + comp)
        for side in (0, 1):
            edge = (1 - side) * size[rim]
            row = (1 - side) * size[order[2]]
            if comp == 0:
                for f in range(out.shape[0]):
                    out[f, edge] += near[comp][side, f]
            else:
                out[edge] += near[comp][side]
            for f in range(out.shape[0]):
                for m in range(out.shape[1]):
                    out[f, m, row : row + 1, :] += last[comp][side, f, m : m + 1, :]
    arrived((12 + 4) * rc.shape[1], 8)
    for comp in range(3):
        out, order, rim = outs[comp], orders[comp], rim_of(comp)
        for slot in range(4):
            edge = (1 - slot // 2) * size[rim]
            row = (1 - slot % 2) * size[order[2]]
            for t in range(size[comp]):
                f, m = (t, edge) if comp == 0 else (edge, t)
                out[f, m, row : row + 1, :] += rc[4 * comp + slot, t : t + 1, :]
    for s in (0, 1):
        z, x = (1 - s) * size[2], (1 - s) * size[0]
        for t in range(size[0]):
            out_x[t, 0, z : z + 1, :] += edge_in[s, t : t + 1, :]
        for t in range(size[2]):
            out_z[x, t, 0:1, :] += edge_in[2 + s, t : t + 1, :]
    rows = ne + (3 + 12 + 4) * rc.shape[1]
    for comp in range(3):
        p, r = [size[t] for t in range(3) if t != comp]
        rows += size[comp] * (p + r) + 2 * size[comp] * (p + r + 2)
    remote(elem.at[0:rows], elem.at[0:rows], (0, 1, 0), 0, 0).wait_send()


def write_out(from_x, from_y, from_z, to_x, to_y, to_z, sems):
    pairs = ((from_x, to_x), (from_y, to_y), (from_z, to_z))
    copies = [pltpu.make_async_copy(src, dst, sems.at[t]) for t, (src, dst) in enumerate(pairs)]
    for copy in copies:
        copy.start()
    for copy in copies:
        copy.wait()


def on_device(mesh_sizes, vectors, orient_flip, reluctivity, conductivity):
    counts = (
        orient_flip.shape[0], orient_flip.shape[1], orient_flip.shape[2] // ELEM_DOFS,
    )
    ne = counts[0] * counts[1] * counts[2]
    sx, sy, sz = (ORDER * c for c in counts)
    lanes = vectors.shape[-1]
    f32 = jnp.float32
    shapes = (
        (sx, sy + 1, sz + 1, lanes), (sx + 1, sy, sz + 1, lanes), (sx + 1, sz, sy + 1, lanes),
    )
    longest = max(sx, sy, sz)
    faces = tuple((2,) + s[:2] + (lanes,) for s in shapes)
    scratch = [
        (ELEM_DOFS * ne, lanes), (ELEM_DOFS * ne, lanes), (QPTS * ne, lanes), (QPTS * ne, lanes),
        (3, ne, ELEM_DOFS), (ELEM_DOFS * ne, lanes), (3 * QPTS * ne, lanes), (3 * QPTS * ne, lanes),
        *shapes,
        (2, sx, sy, lanes), (2, longest, lanes),
        (2, sy, sz, lanes), (2, sx, sz, lanes), (2, sx, sy, lanes), (3, longest, lanes),
        *faces[:2], (12, longest, lanes),
        (2, sx, sz + 1, lanes), (2, sy, sz + 1, lanes), (2, sz, sy + 1, lanes),
        *faces, (12, longest, lanes),
        (24 * ne, lanes), (24 * ne, lanes), (24 * ne, lanes), (ne, lanes), (ne, lanes),
        (sx, sz + 1, lanes), (sx + 1, sz, lanes), (sx, sz + 1, lanes), (sx + 1, sz, lanes),
        (4, longest, lanes), (4, longest, lanes),
    ]
    vmem = pl.BlockSpec(memory_space=pltpu.VMEM)
    padded = [s[0] * s[1] * (s[2] + -s[2] % 8) * lanes * 4 for s in shapes]
    room = sum(padded) + max(padded)
    anywhere = pl.BlockSpec(memory_space=pltpu.HBM)
    arguments = (vectors, orient_flip, reluctivity, conductivity)
    outs = [jax.ShapeDtypeStruct(s, f32) for s in shapes]
    held = pl.pallas_call(
        functools.partial(kernel, mesh_sizes),
        out_shape=[pltpu.VMEM(s, f32) for s in shapes],
        in_specs=[anywhere] * 4,
        out_specs=[vmem] * 3,
        scratch_shapes=[pltpu.VMEM(a.shape, a.dtype) for a in arguments]
        + [pltpu.VMEM(s, f32) for s in scratch]
        + [pltpu.SemaphoreType.DMA((1,)), pltpu.SemaphoreType.DMA((9,))]
        + [pltpu.SemaphoreType.DMA((4,)), pltpu.SemaphoreType.REGULAR],
        compiler_params=pltpu.CompilerParams(
            collective_id=0, has_side_effects=True, vmem_limit_bytes=VMEM_ALL - room
        ),
        name="curl_mass",
    )(*arguments)
    held = pl.pallas_call(
        write_out,
        out_shape=outs,
        in_specs=[pl.BlockSpec(memory_space=pl.ANY)] * 3,
        out_specs=[anywhere] * 3,
        scratch_shapes=[pltpu.SemaphoreType.DMA((3,))],
        compiler_params=pltpu.CompilerParams(vmem_limit_bytes=2**20),
        name="write_out",
    )(*held)
    return held[0], held[1], jnp.swapaxes(held[2], 1, 2)


def solution(mesh):
    return jax.shard_map(
        functools.partial(on_device, tuple(mesh.shape[a] for a in AXES)),
        mesh=mesh,
        in_specs=(
            P(None, "gx", "gy", "gz", None),
            P("gx", "gy", "gz"),
            P("gx", "gy", "gz"),
            P("gx", "gy", "gz"),
        ),
        out_specs=(P("gx", "gy", "gz", None), P("gx", "gy", "gz", None), P("gx", "gy", "gz", None)),
        check_vma=False,
    )
```

```python
import functools
import jax
import jax.numpy as jnp
import numpy as np
from jax import lax
from jax.experimental import pallas as pl
from jax.experimental.pallas import tpu as pltpu
from jax.sharding import PartitionSpec as P

ORDER = 3
QUAD = 4
ELEM_DOFS = 144
QPTS = 64
AXES = ("gx", "gy", "gz")
MESH = pl.DeviceIdType.MESH
VMEM_ALL = 67043328


def lagrange(points_at, evaluate_at):
    amount = len(points_at)
    values = np.ones((len(evaluate_at), amount))
    slopes = np.zeros((len(evaluate_at), amount))
    for which in range(amount):
        for column in range(amount):
            if column != which:
                factor = (evaluate_at - points_at[column]) / (points_at[which] - points_at[column])
                slopes[:, which] = slopes[:, which] * factor + values[:, which] / (
                    points_at[which] - points_at[column]
                )
                values[:, which] = values[:, which] * factor
    return (values, slopes)


def basis_tables():
    lobatto = np.array([0.0, (1 - 5 ** (-0.5)) / 2, (1 + 5 ** (-0.5)) / 2, 1.0])
    gauss_open = np.array([(1 - 0.6**0.5) / 2, 0.5, (1 + 0.6**0.5) / 2])
    inner_pt = (3.0 / 7 - 2.0 / 7 * (6.0 / 5) ** 0.5) ** 0.5
    outer_pt = (3.0 / 7 + 2.0 / 7 * (6.0 / 5) ** 0.5) ** 0.5
    inner_wt = (18 + 30**0.5) / 36
    outer_wt = (18 - 30**0.5) / 36
    quad_points = (1 + np.array([-outer_pt, -inner_pt, inner_pt, outer_pt])) / 2
    quad_weight = np.array([outer_wt, inner_wt, inner_wt, outer_wt]) / 2
    closed, _ = lagrange(lobatto, quad_points)
    opened, _ = lagrange(gauss_open, quad_points)
    _, colloc = lagrange(quad_points, quad_points)
    return closed, opened, colloc, quad_weight


CLOSED, OPENED, COLLOC, WEIGHT = basis_tables()


def add_all(terms):
    total = terms[0]
    for term in terms[1:]:
        total = total + term
    return total


def apply(mat, xs, sigma=1):
    rows, cols = mat.shape
    half = cols // 2
    plus = [xs[p] + xs[cols - 1 - p] for p in range(half)]
    minus = [xs[p] - xs[cols - 1 - p] for p in range(half)]
    ys = [None] * rows
    for q in range((rows + 1) // 2):
        even_c = [(mat[q, p] + mat[q, cols - 1 - p]) / 2 for p in range(half)]
        odd_c = [(mat[q, p] - mat[q, cols - 1 - p]) / 2 for p in range(half)]
        even = [np.float32(c) * s for c, s in zip(even_c, plus)]
        if cols % 2:
            even.append(np.float32(mat[q, half]) * xs[half])
        even = add_all(even)
        if 2 * q == rows - 1:
            ys[q] = even
            continue
        odd = add_all([np.float32(c) * d for c, d in zip(odd_c, minus)])
        ys[q] = even + odd
        ys[rows - 1 - q] = even - odd if sigma > 0 else odd - even
    return ys


def swap(blocks, size):
    count = blocks[0].shape[0] // size
    return [
        jnp.concatenate([b[q * size : (q + 1) * size] for b in blocks], 0) for q in range(count)
    ]


def dims_of(comp):
    return [ORDER if axis == comp else ORDER + 1 for axis in range(3)]


def kernel(
    mesh_sizes, vec_hbm, flip_hbm, reluct_hbm, conduct_hbm, out_x, out_y, out_z,
    vec, flip, reluct, conduct, elem, sign, mass, curlw, flat, tmp, uq, cq,
    res_x, res_y, res_z, pack1, corner1, hx, hy, hz, hc, pack2_x, pack2_y, corner2,
    near_x, near_y, near_z, last_x, last_y, last_z, rc,
    face, face_own, face_out, coef, coef_in, top_x, top_z, low_x, low_z,
    edge_out, edge_in, low_out, sent, came, s0, ready,
):
    f32 = jnp.float32
    cx, cy = flip.shape[0], flip.shape[1]
    cz = flip.shape[2] // ELEM_DOFS
    counts = (cx, cy, cz)
    ne = cx * cy * cz
    size = tuple(ORDER * c for c in counts)
    lanes = vec.shape[-1]
    me = [lax.axis_index(a) for a in AXES]

    def device(shift):
        return tuple(
            lax.rem(me[a] + (shift[a] + mesh_sizes[a]), mesh_sizes[a]) for a in range(3)
        )

    def signal(sem, shift):
        pl.semaphore_signal(sem, inc=1, device_id=device(shift), device_id_type=MESH)

    fetches = [
        pltpu.make_async_copy(src, dst, s0.at[t])
        for t, (src, dst) in enumerate(
            ((vec_hbm, vec), (flip_hbm, flip), (reluct_hbm, reluct), (conduct_hbm, conduct))
        )
    ]
    for fetch in fetches:
        fetch.start()
    barrier = pltpu.get_barrier_semaphore()
    lowest, highest = me[1] == 0, me[1] == mesh_sizes[1] - 1
    above = ((0, 1, 0), (1, 1, 0), (-1, 1, 0), (0, 1, 1), (0, 1, -1))
    greeted = ((1, 0, 0), (0, 0, 1), (1, 0, 1)) + tuple((s[0], -1, s[2]) for s in above)
    for shift in greeted:
        signal(barrier, shift)

    @pl.when(jnp.logical_not(highest))
    def _():
        for shift in above:
            signal(barrier, shift)

    fetches[0].wait()
    for comp in (0, 1):
        for x in range(size[0]):
            for y in range(size[1]):
                pack1[comp, x, y : y + 1, :] = vec[comp, x, y, 0:1, :]
    for x in range(size[0]):
        corner1[0, x : x + 1, :] = vec[0, x, 0, 0:1, :]
    for y in range(size[1]):
        corner1[1, y : y + 1, :] = vec[1, 0, y, 0:1, :]
    pl.semaphore_wait(barrier, len(greeted) + jnp.where(lowest, 0, len(above)))

    def remote(src, dst, shift, out, into):
        return pltpu.make_async_remote_copy(
            src_ref=src, dst_ref=dst, send_sem=sent.at[out], recv_sem=came.at[into],
            device_id=device(shift), device_id_type=MESH,
        )

    def send(src, dst, shift, out, into):
        remote(src, dst, shift, out, into).start()

    def arrived(rows, into):
        remote(elem.at[0:rows], elem.at[0:rows], (0, 1, 0), 0, into).wait_recv()

    send(vec.at[2, 0], hx.at[1], (-1, 0, 0), 0, 0)
    send(pack1.at[0], hz.at[0], (0, 0, -1), 0, 1)
    send(corner1.at[1], hc.at[0], (-1, 0, -1), 0, 2)
    send(vec.at[1, 0], hx.at[0], (-1, 0, 0), 0, 2)
    send(pack1.at[1], hz.at[1], (0, 0, -1), 0, 2)

    @pl.when(highest)
    def _():
        for shift in above:
            signal(ready, shift)

    def send_down():
        send(corner1.at[0], hc.at[1], (0, -1, -1), 0, 3)
        send(vec.at[2, 0, 0], hc.at[2], (-1, -1, 0), 0, 3)
        send(vec.at[0, :, 0], hy.at[0], (0, -1, 0), 0, 3)
        send(vec.at[2, :, 0], hy.at[1], (0, -1, 0), 0, 3)

    pl.when(jnp.logical_not(lowest))(send_down)

    for fetch in fetches[1:]:
        fetch.wait()
    for i in range(cx):
        for j in range(cy):
            for k in range(cz):
                e = (i * cy + j) * cz + k
                flat[0, e : e + 1, 0:ELEM_DOFS] = 1.0 - 2.0 * flip[
                    i, j : j + 1, k * ELEM_DOFS : (k + 1) * ELEM_DOFS
                ].astype(f32)
                flat[1, e : e + 1, 0:QPTS] = reluct[i, j : j + 1, k * QPTS : (k + 1) * QPTS]
                flat[2, e : e + 1, 0:QPTS] = conduct[i, j : j + 1, k * QPTS : (k + 1) * QPTS]
    for d in range(ELEM_DOFS):
        sign[d * ne : (d + 1) * ne, :] = jnp.broadcast_to(flat[0, :, d : d + 1], (ne, lanes))
    for q in range(QPTS):
        w = np.float32(WEIGHT[q // 16] * WEIGHT[q // 4 % 4] * WEIGHT[q % 4])
        rows = slice(q * ne, (q + 1) * ne)
        curlw[rows, :] = jnp.broadcast_to(flat[1, :, q : q + 1] * w, (ne, lanes))
        mass[rows, :] = jnp.broadcast_to(flat[2, :, q : q + 1] * w, (ne, lanes))

    line_c, line_s = CLOSED[:, ORDER], COLLOC @ CLOSED[:, ORDER]

    def plane_dofs(b):
        found = [(a * 4 + b) * 4 + c for a in range(3) for c in range(4)]
        return found + [96 + (a * 4 + b) * 3 + c for a in range(4) for c in range(3)]

    face_dofs = plane_dofs(ORDER)

    def quad_rows(ref, base, qx, qy):
        first = base + (qx * 16 + qy * 4) * ne
        return ref[first : first + 4 * ne, :]

    def pieces_of(block):
        return [block[t * ne : (t + 1) * ne] for t in range(block.shape[0] // ne)]

    summed = []
    for qx in range(QUAD):
        summed += pieces_of(add_all(
            [np.float32(line_c[qy] ** 2) * quad_rows(mass, 0, qx, qy) for qy in range(QUAD)]
            + [np.float32(line_s[qy] ** 2) * quad_rows(curlw, 0, qx, qy) for qy in range(QUAD)]
        ))
    for qx in range(QUAD):
        summed += pieces_of(add_all(
            [np.float32(line_c[qy] ** 2) * quad_rows(curlw, 0, qx, qy) for qy in range(QUAD)]
        ))
    summed += [sign[d * ne : (d + 1) * ne, :] for d in face_dofs]
    lane = lax.broadcasted_iota(jnp.int32, (ne, lanes), 1)
    packed = jnp.zeros((ne, lanes), f32)
    for t, value in enumerate(summed):
        packed = jnp.where(lane == t, value, packed)
    coef[...] = packed
    send(coef, coef_in, (0, 1, 0), 0, 4)

    def homes(comp, axis, low, high):
        found = []
        for el in range(counts[axis]):
            first = max(low, ORDER * el)
            last = min(high, ORDER * el + dims_of(comp)[axis])
            if first < last:
                found.append((el, first - ORDER * el, first - low, last - first))
        return found

    def places(comp, axis, at, low, high):
        dims = dims_of(comp)
        steps = (dims[1] * dims[2], dims[2], 1)
        span = [(p, p + 1) for p in at]
        span[axis] = (low, high)
        for fx in homes(comp, 0, *span[0]):
            for fy in homes(comp, 1, *span[1]):
                for fz in homes(comp, 2, *span[2]):
                    found = (fx, fy, fz)
                    e = (fx[0] * cy + fy[0]) * cz + fz[0]
                    d = comp * 48 + sum(found[t][1] * steps[t] for t in range(3))
                    yield found[axis][2], found[axis][3], d * ne + e, steps[axis] * ne

    def put(comp, axis, at, low, high, load):
        for offset, length, row, stride in places(comp, axis, at, low, high):
            elem[pl.ds(row, length, stride=stride), :] = load(offset, offset + length)

    def face_places(comp, x, low, high, layer=cy - 1):
        for fx in homes(comp, 0, x, x + 1):
            for fz in homes(comp, 2, low, high):
                e = (fx[0] * cy + layer) * cz + fz[0]
                d = comp // 2 * 12 + fx[1] * dims_of(comp)[2] + fz[1]
                yield fz[2], fz[3], d * ne + e

    def put_face(ref, comp, x, low, high, load):
        for offset, length, row in face_places(comp, x, low, high):
            ref[pl.ds(row, length, stride=ne), :] = load(offset, offset + length)

    blank = jnp.zeros((ne, lanes), f32)
    for t, d in enumerate(face_dofs):
        elem[d * ne : (d + 1) * ne, :] = blank
        face[t * ne : (t + 1) * ne, :] = blank
        face_own[t * ne : (t + 1) * ne, :] = blank
    for comp in range(3):
        for x in range(size[0]):
            for y in range(size[1]):
                put(comp, 2, (x, y, 0), 0, size[2], lambda a, b: vec[comp, x, y, a:b, :])
    for comp in (0, 2):
        for x in range(size[0]):
            put_face(face_own, comp, x, 0, size[2], lambda a, b: vec[comp, x, 0, a:b, :])
    results = (res_x, res_y, res_z)
    for res in (top_x, top_z, low_x, low_z) + results:
        res[...] = jnp.zeros_like(res)


    def take_halo(comp):
        if comp == 1:
            arrived(hc.shape[1] + size[1] * size[2] + size[0] * size[1], 2)
            for y in range(size[1]):
                put(1, 2, (size[0], y, 0), 0, size[2], lambda a, b: hx[0, y, a:b, :])
            for x in range(size[0]):
                put(1, 1, (x, 0, size[2]), 0, size[1], lambda a, b: hz[1, x, a:b, :])
            put(1, 1, (size[0], 0, size[2]), 0, size[1], lambda a, b: hc[0, a:b, :])
        elif comp == 0:
            arrived(size[0] * size[1], 1)
            for x in range(size[0]):
                put(0, 1, (x, 0, size[2]), 0, size[1], lambda a, b: hz[0, x, a:b, :])
                put_face(face_own, 0, x, size[2], size[2] + 1, lambda a, b: hz[0, x, 0:1, :])
        else:
            arrived(size[1] * size[2], 0)
            for y in range(size[1]):
                put(2, 2, (size[0], y, 0), 0, size[2], lambda a, b: hx[1, y, a:b, :])
            put_face(face_own, 2, size[0], 0, size[2], lambda a, b: hx[1, 0, a:b, :])

    def rows_of(axis, at, line, dims):
        others = [t for t in range(3) if t != axis]
        points = []
        for last in range(dims[others[1]]):
            index = [0, 0, 0]
            index[axis], index[others[0]], index[others[1]] = at, line, last
            points.append(((index[0] * dims[1] + index[1]) * dims[2] + index[2]) * ne)
        return points

    def load_line(ref, base, axis, at, line, dims):
        starts = [base + r for r in rows_of(axis, at, line, dims)]
        if len(starts) > 1 and starts[1] - starts[0] == ne:
            return ref[starts[0] : starts[-1] + ne, :]
        return jnp.concatenate([ref[s : s + ne, :] for s in starts], 0)

    def load_plane(ref, base, axis, at, dims):
        others = [t for t in range(3) if t != axis]
        return [load_line(ref, base, axis, at, p, dims) for p in range(dims[others[0]])]

    def store_plane(ref, base, axis, at, dims, blocks):
        for p, block in enumerate(blocks):
            starts = [base + r for r in rows_of(axis, at, p, dims)]
            if starts[1] - starts[0] == ne:
                ref[starts[0] : starts[-1] + ne, :] = block
            else:
                for t, s in enumerate(starts):
                    ref[s : s + ne, :] = block[t * ne : (t + 1) * ne]

    full = [QUAD] * 3

    def mid_dims(comp):
        return [ORDER if axis == comp else QUAD for axis in range(3)]

    def evaluate(comp):
        take_halo(comp)
        dims = dims_of(comp)
        base = comp * 48 * ne
        for a in range(ORDER):
            plane = load_plane(elem, base, comp, a, dims)
            signs = load_plane(sign, base, comp, a, dims)
            plane = [p * s for p, s in zip(plane, signs)]
            plane = apply(CLOSED, plane)
            plane = apply(CLOSED, swap(plane, ne))
            store_plane(tmp, base, comp, a, mid_dims(comp), swap(plane, ne))
        others = [t for t in range(3) if t != comp]
        for line in range(QUAD):
            xs = [load_line(tmp, base, comp, a, line, mid_dims(comp)) for a in range(ORDER)]
            for q, y in enumerate(apply(OPENED, xs)):
                starts = [comp * 64 * ne + r for r in rows_of(comp, q, line, full)]
                if starts[1] - starts[0] == ne:
                    uq[starts[0] : starts[-1] + ne, :] = y
                else:
                    for t, s in enumerate(starts):
                        uq[s : s + ne, :] = y[t * ne : (t + 1) * ne]

    part = 64 * ne

    def half_turn(c, axis, at):
        other = 3 - c - axis
        u = load_plane(uq, other * part, c, at, full)
        if axis < other:
            return apply(COLLOC, u, -1)
        return swap(apply(COLLOC, swap(u, ne), -1), ne)

    def turn_of(c, axis, kept):
        plus = (axis - c) % 3 == 1
        for at in range(QUAD):
            one = half_turn(c, axis, at)
            if kept:
                two = load_plane(cq, c * part, c, at, full)
            else:
                two = half_turn(c, 3 - c - axis, at)
            both = [a - b if plus else b - a for a, b in zip(one, two)]
            scale = load_plane(curlw, 0, c, at, full)
            store_plane(cq, c * part, c, at, full, [k * w for k, w in zip(both, scale)])

    evaluate(2)
    evaluate(0)
    turn_of(1, 2, False)
    for c in (0, 2):
        for at in range(QUAD):
            store_plane(cq, c * part, c, at, full, half_turn(c, 1, at))
    @pl.when(lowest)
    def _():
        pl.semaphore_wait(ready, len(above))
        send_down()

    evaluate(1)
    turn_of(0, 2, True)
    turn_of(2, 0, True)

    closed_t, opened_t, colloc_t = CLOSED.T, OPENED.T, COLLOC.T
    packs = (pack2_x, pack2_y)
    near = (near_x, near_y, near_z)
    last = (last_x, last_y, last_z)
    orders = ((0, 1, 2), (0, 1, 2), (0, 2, 1))

    def face_values(ref, signs):
        at = [ref[t * ne : (t + 1) * ne, :] * signs[t] for t in range(24)]
        xs = [jnp.concatenate([at[a * 4 + c] for a in range(3)], 0) for c in range(4)]
        u_x = apply(OPENED, swap(apply(CLOSED, xs), ne))
        xs = [jnp.concatenate([at[12 + a * 3 + c] for c in range(3)], 0) for a in range(4)]
        u_z = swap(apply(OPENED, swap(apply(CLOSED, xs), ne)), ne)
        along_z = swap(apply(COLLOC, swap(u_x, ne), -1), ne)
        along_x = apply(COLLOC, u_z, -1)
        return u_x, u_z, [f - g for f, g in zip(along_z, along_x)]

    def face_gradient(v_x, v_z, b, signs, into=None):
        into = face_out if into is None else into
        by_z = swap(apply(colloc_t, swap(b, ne), -1), ne)
        by_x = apply(colloc_t, b, -1)
        v_x = [v + f for v, f in zip(v_x, by_z)]
        v_z = [v - f for v, f in zip(v_z, by_x)]
        for c, block in enumerate(apply(closed_t, swap(apply(opened_t, v_x), ne))):
            for a, y in enumerate(pieces_of(block)):
                t = a * 4 + c
                into[t * ne : (t + 1) * ne, :] = y * signs[t]
        for c, block in enumerate(apply(opened_t, swap(apply(closed_t, v_z), ne))):
            for a, y in enumerate(pieces_of(block)):
                t = 12 + a * 3 + c
                into[t * ne : (t + 1) * ne, :] = y * signs[t]

    def plane_fields(values, slopes):
        v_x, v_z, b = [], [], []
        for qx in range(QUAD):
            t_x, t_z, t_b = [], [], []
            for qy in range(QUAD):
                m = quad_rows(mass, 0, qx, qy) * np.float32(values[qy])
                slope = np.float32(slopes[qy])
                t_x += [m * quad_rows(uq, 0, qx, qy), -slope * quad_rows(cq, 2 * part, qx, qy)]
                t_z += [m * quad_rows(uq, 2 * part, qx, qy), slope * quad_rows(cq, 0, qx, qy)]
                t_b += [np.float32(values[qy]) * quad_rows(cq, part, qx, qy)]
            v_x.append(add_all(t_x))
            v_z.append(add_all(t_z))
            b.append(add_all(t_b))
        return v_x, v_z, b

    def signs_of(dofs):
        return [sign[d * ne : (d + 1) * ne, :] for d in dofs]

    def pack_corner(comp, slot, load):
        for t in range(size[comp]):
            corner2[4 * comp + slot, t : t + 1, :] = load(t)

    def send_corner(comp, shift, slot):
        where = 4 * comp + slot
        send(corner2.at[where], rc.at[where], shift, 0, 8)

    def make_plane(side, plane_x, plane_z):
        b, layer = side * ORDER, side * (cy - 1)
        fields = plane_fields(CLOSED[:, b], COLLOC @ CLOSED[:, b])
        face_gradient(*fields, signs_of(plane_dofs(b)))
        for comp, plane in ((0, plane_x), (2, plane_z)):
            for x in range(plane.shape[0]):
                for offset, length, row in face_places(comp, x, 0, plane.shape[1], layer):
                    plane[x, offset : offset + length, :] += face_out[
                        pl.ds(row, length, stride=ne), :
                    ]
        for s in (0, 1):
            z, x = s * size[2], s * size[0]
            pack_corner(0, 2 * side + s, lambda t: plane_x[t, z : z + 1, :])
            pack_corner(2, 2 * s + side, lambda t: plane_z[x, t : t + 1, :])

    def send_plane(side, plane_x, plane_z):
        way = 2 * side - 1
        for s in (0, 1):
            send_corner(0, (0, way, 2 * s - 1), 2 * side + s)
            send_corner(2, (2 * s - 1, way, 0), 2 * s + side)
        send(plane_x, near_x.at[side], (0, way, 0), 0, 5)
        send(plane_z, last_z.at[side], (0, way, 0), 0, 7)

    make_plane(1, top_x, top_z)

    send_plane(1, top_x, top_z)

    if cy > 1:
        make_plane(0, low_x, low_z)
        send_plane(0, low_x, low_z)

    def low_lines():
        arrived(ne, 4)
        theirs = [jnp.broadcast_to(coef_in[:, t : t + 1], (ne, lanes)) for t in range(56)]
        u_x, u_z, turn = face_values(face_own, theirs[32:])
        m2 = [jnp.concatenate(theirs[4 * qx : 4 * qx + 4], 0) for qx in range(QUAD)]
        k2 = [jnp.concatenate(theirs[16 + 4 * qx : 20 + 4 * qx], 0) for qx in range(QUAD)]
        face_gradient(
            [m * u for m, u in zip(m2, u_x)], [m * u for m, u in zip(m2, u_z)],
            [k * u for k, u in zip(k2, turn)], theirs[32:], low_out,
        )
        for s in (0, 1):
            for x in range(size[0]):
                for _, _, row in face_places(0, x, s * size[2], s * size[2] + 1):
                    edge_out[s, x : x + 1, :] = low_out[row : row + 1, :]
            for offset, length, row in face_places(2, s * size[0], 0, size[2]):
                edge_out[2 + s, offset : offset + length, :] = low_out[
                    pl.ds(row, length, stride=ne), :
                ]
            send(edge_out.at[s], edge_in.at[s], (0, 0, 2 * s - 1), 0, 8)
            send(edge_out.at[2 + s], edge_in.at[2 + s], (2 * s - 1, 0, 0), 0, 8)

    pl.when(jnp.logical_not(lowest))(low_lines)
    arrived(2 * size[0] * size[2] + 2 * hc.shape[1], 3)
    for x in range(size[0]):
        put_face(face, 0, x, 0, size[2], lambda a, b: hy[0, x, a:b, :])
        put_face(face, 0, x, size[2], size[2] + 1, lambda a, b: hc[1, x : x + 1, :])
        put_face(face, 2, x, 0, size[2], lambda a, b: hy[1, x, a:b, :])
    put_face(face, 2, size[0], 0, size[2], lambda a, b: hc[2, a:b, :])
    own_signs = signs_of(face_dofs)
    u_x, u_z, turn = face_values(face, own_signs)

    def add_rows(ref, which, qx, qy, more):
        first = which * part + (qx * 16 + qy * 4) * ne
        ref[first : first + 4 * ne, :] += more

    for qx in range(QUAD):
        for qy in range(QUAD):
            sloped = quad_rows(curlw, 0, qx, qy) * np.float32(line_s[qy])
            add_rows(cq, 0, qx, qy, sloped * u_z[qx])
            add_rows(cq, 2, qx, qy, -sloped * u_x[qx])

    if cy == 1:
        make_plane(0, low_x, low_z)
        send_plane(0, low_x, low_z)

    for comp in (1, 2, 0):
        if comp == 2:
            for qx in range(QUAD):
                for qy in range(QUAD):
                    value = np.float32(line_c[qy])
                    add_rows(uq, 0, qx, qy, value * u_x[qx])
                    add_rows(uq, 2, qx, qy, value * u_z[qx])
                    add_rows(cq, 1, qx, qy, (quad_rows(curlw, 0, qx, qy) * value) * turn[qx])
        dims = dims_of(comp)
        base = comp * 48 * ne
        p, r = [t for t in range(3) if t != comp]
        for at in range(QUAD):
            u = load_plane(uq, comp * part, comp, at, full)
            m = load_plane(mass, 0, comp, at, full)
            total = [a * b for a, b in zip(u, m)]
            by_p = apply(colloc_t, load_plane(cq, r * part, comp, at, full), -1)
            by_r = apply(colloc_t, swap(load_plane(cq, p * part, comp, at, full), ne), -1)
            by_r = swap(by_r, ne)
            if comp == 1:
                total = [t + a - b for t, a, b in zip(total, by_p, by_r)]
            else:
                total = [t - a + b for t, a, b in zip(total, by_p, by_r)]
            total = apply(closed_t, total)
            total = apply(closed_t, swap(total, ne))
            kept = [QUAD if axis == comp else ORDER + 1 for axis in range(3)]
            store_plane(tmp, 0, comp, at, kept, swap(total, ne))
        for line in range(ORDER + 1):
            xs = [load_line(tmp, 0, comp, q, line, kept) for q in range(QUAD)]
            for a, y in enumerate(apply(opened_t, xs)):
                y = y * load_line(sign, base, comp, a, line, dims)
                for t, s in enumerate(rows_of(comp, a, line, dims)):
                    elem[base + s : base + s + ne, :] = y[t * ne : (t + 1) * ne]
        res = results[comp]
        order = orders[comp]
        for first in range(res.shape[0]):
            for middle in range(res.shape[1]):
                at = [0, 0, 0]
                at[order[0]], at[order[1]] = first, middle
                pieces = places(comp, order[2], at, 0, res.shape[2])
                for offset, length, row, stride in pieces:
                    res[first, middle, offset : offset + length, :] += elem[
                        pl.ds(row, length, stride=stride), :
                    ]
        if comp == 1:
            for s_x in (0, 1):
                for s_z in (0, 1):
                    x, z = s_x * size[0], s_z * size[2]
                    pack_corner(1, 2 * s_x + s_z, lambda t: res[x, t, z : z + 1, :])
                    send_corner(1, (2 * s_x - 1, 0, 2 * s_z - 1), 2 * s_x + s_z)
        if comp > 0:
            for side in (0, 1):
                send(
                    res.at[side * size[0]], near[comp].at[side], (2 * side - 1, 0, 0),
                    0, 5 + comp,
                )
        if comp < 2:
            for side in (0, 1):
                row = side * size[2]
                for f in range(res.shape[0]):
                    for m in range(res.shape[1]):
                        packs[comp][side, f, m : m + 1, :] = res[f, m, row : row + 1, :]
                send(
                    packs[comp].at[side], last[comp].at[side], (0, 0, 2 * side - 1),
                    0, 5 + comp,
                )
    pl.when(lowest)(low_lines)

    outs = (out_x, out_y, out_z)
    for comp in range(3):
        outs[comp][...] = results[comp][...]
    for x in range(size[0]):
        for offset, length, row in face_places(0, x, 0, size[2] + 1):
            out_x[x, 0, offset : offset + length, :] += low_out[pl.ds(row, length, stride=ne), :]
    for x in range(size[0] + 1):
        for offset, length, row in face_places(2, x, 0, size[2]):
            for t in range(length):
                out_z[x, offset + t, 0:1, :] += low_out[row + t * ne : row + t * ne + 1, :]
    def rim_of(comp):
        return orders[comp][1] if comp == 0 else orders[comp][0]

    for comp in (1, 0, 2):
        out, order, rim = outs[comp], orders[comp], rim_of(comp)
        arrived(2 * size[comp] * (size[rim] + size[order[2]] + 2), 5 + comp)
        for side in (0, 1):
            edge = (1 - side) * size[rim]
            row = (1 - side) * size[order[2]]
            if comp == 0:
                for f in range(out.shape[0]):
                    out[f, edge] += near[comp][side, f]
            else:
                out[edge] += near[comp][side]
            for f in range(out.shape[0]):
                for m in range(out.shape[1]):
                    out[f, m, row : row + 1, :] += last[comp][side, f, m : m + 1, :]
    arrived((12 + 4) * rc.shape[1], 8)
    for comp in range(3):
        out, order, rim = outs[comp], orders[comp], rim_of(comp)
        for slot in range(4):
            edge = (1 - slot // 2) * size[rim]
            row = (1 - slot % 2) * size[order[2]]
            for t in range(size[comp]):
                f, m = (t, edge) if comp == 0 else (edge, t)
                out[f, m, row : row + 1, :] += rc[4 * comp + slot, t : t + 1, :]
    for s in (0, 1):
        z, x = (1 - s) * size[2], (1 - s) * size[0]
        for t in range(size[0]):
            out_x[t, 0, z : z + 1, :] += edge_in[s, t : t + 1, :]
        for t in range(size[2]):
            out_z[x, t, 0:1, :] += edge_in[2 + s, t : t + 1, :]
    rows = ne + (3 + 12 + 4) * rc.shape[1]
    for comp in range(3):
        p, r = [size[t] for t in range(3) if t != comp]
        rows += size[comp] * (p + r) + 2 * size[comp] * (p + r + 2)
    remote(elem.at[0:rows], elem.at[0:rows], (0, 1, 0), 0, 0).wait_send()


def write_out(from_x, from_y, from_z, to_x, to_y, to_z, sems):
    pairs = ((from_x, to_x), (from_y, to_y), (from_z, to_z))
    copies = [pltpu.make_async_copy(src, dst, sems.at[t]) for t, (src, dst) in enumerate(pairs)]
    for copy in copies:
        copy.start()
    for copy in copies:
        copy.wait()


def on_device(mesh_sizes, vectors, orient_flip, reluctivity, conductivity):
    counts = (
        orient_flip.shape[0], orient_flip.shape[1], orient_flip.shape[2] // ELEM_DOFS,
    )
    ne = counts[0] * counts[1] * counts[2]
    sx, sy, sz = (ORDER * c for c in counts)
    lanes = vectors.shape[-1]
    f32 = jnp.float32
    shapes = (
        (sx, sy + 1, sz + 1, lanes), (sx + 1, sy, sz + 1, lanes), (sx + 1, sz, sy + 1, lanes),
    )
    longest = max(sx, sy, sz)
    faces = tuple((2,) + s[:2] + (lanes,) for s in shapes)
    scratch = [
        (ELEM_DOFS * ne, lanes), (ELEM_DOFS * ne, lanes), (QPTS * ne, lanes), (QPTS * ne, lanes),
        (3, ne, ELEM_DOFS), (ELEM_DOFS * ne, lanes), (3 * QPTS * ne, lanes), (3 * QPTS * ne, lanes),
        *shapes,
        (2, sx, sy, lanes), (2, longest, lanes),
        (2, sy, sz, lanes), (2, sx, sz, lanes), (2, sx, sy, lanes), (3, longest, lanes),
        *faces[:2], (12, longest, lanes),
        (2, sx, sz + 1, lanes), (2, sy, sz + 1, lanes), (2, sz, sy + 1, lanes),
        *faces, (12, longest, lanes),
        (24 * ne, lanes), (24 * ne, lanes), (24 * ne, lanes), (ne, lanes), (ne, lanes),
        (sx, sz + 1, lanes), (sx + 1, sz, lanes), (sx, sz + 1, lanes), (sx + 1, sz, lanes),
        (4, longest, lanes), (4, longest, lanes), (24 * ne, lanes),
    ]
    vmem = pl.BlockSpec(memory_space=pltpu.VMEM)
    padded = [s[0] * s[1] * (s[2] + -s[2] % 8) * lanes * 4 for s in shapes]
    room = sum(padded) + max(padded)
    anywhere = pl.BlockSpec(memory_space=pltpu.HBM)
    arguments = (vectors, orient_flip, reluctivity, conductivity)
    outs = [jax.ShapeDtypeStruct(s, f32) for s in shapes]
    held = pl.pallas_call(
        functools.partial(kernel, mesh_sizes),
        out_shape=[pltpu.VMEM(s, f32) for s in shapes],
        in_specs=[anywhere] * 4,
        out_specs=[vmem] * 3,
        scratch_shapes=[pltpu.VMEM(a.shape, a.dtype) for a in arguments]
        + [pltpu.VMEM(s, f32) for s in scratch]
        + [pltpu.SemaphoreType.DMA((1,)), pltpu.SemaphoreType.DMA((9,))]
        + [pltpu.SemaphoreType.DMA((4,)), pltpu.SemaphoreType.REGULAR],
        compiler_params=pltpu.CompilerParams(
            collective_id=0, has_side_effects=True, vmem_limit_bytes=VMEM_ALL - room
        ),
        name="curl_mass",
    )(*arguments)
    held = pl.pallas_call(
        write_out,
        out_shape=outs,
        in_specs=[pl.BlockSpec(memory_space=pl.ANY)] * 3,
        out_specs=[anywhere] * 3,
        scratch_shapes=[pltpu.SemaphoreType.DMA((3,))],
        compiler_params=pltpu.CompilerParams(vmem_limit_bytes=2**20),
        name="write_out",
    )(*held)
    return held[0], held[1], jnp.swapaxes(held[2], 1, 2)


def solution(mesh):
    return jax.shard_map(
        functools.partial(on_device, tuple(mesh.shape[a] for a in AXES)),
        mesh=mesh,
        in_specs=(
            P(None, "gx", "gy", "gz", None),
            P("gx", "gy", "gz"),
            P("gx", "gy", "gz"),
            P("gx", "gy", "gz"),
        ),
        out_specs=(P("gx", "gy", "gz", None), P("gx", "gy", "gz", None), P("gx", "gy", "gz", None)),
        check_vma=False,
    )
```

```python
import functools
import jax
import jax.numpy as jnp
import numpy as np
from jax import lax
from jax.experimental import pallas as pl
from jax.experimental.pallas import tpu as pltpu
from jax.sharding import PartitionSpec as P

ORDER = 3
QUAD = 4
ELEM_DOFS = 144
QPTS = 64
AXES = ("gx", "gy", "gz")
MESH = pl.DeviceIdType.MESH
VMEM_ALL = 67043328


def lagrange(points_at, evaluate_at):
    amount = len(points_at)
    values = np.ones((len(evaluate_at), amount))
    slopes = np.zeros((len(evaluate_at), amount))
    for which in range(amount):
        for column in range(amount):
            if column != which:
                factor = (evaluate_at - points_at[column]) / (points_at[which] - points_at[column])
                slopes[:, which] = slopes[:, which] * factor + values[:, which] / (
                    points_at[which] - points_at[column]
                )
                values[:, which] = values[:, which] * factor
    return (values, slopes)


def basis_tables():
    lobatto = np.array([0.0, (1 - 5 ** (-0.5)) / 2, (1 + 5 ** (-0.5)) / 2, 1.0])
    gauss_open = np.array([(1 - 0.6**0.5) / 2, 0.5, (1 + 0.6**0.5) / 2])
    inner_pt = (3.0 / 7 - 2.0 / 7 * (6.0 / 5) ** 0.5) ** 0.5
    outer_pt = (3.0 / 7 + 2.0 / 7 * (6.0 / 5) ** 0.5) ** 0.5
    inner_wt = (18 + 30**0.5) / 36
    outer_wt = (18 - 30**0.5) / 36
    quad_points = (1 + np.array([-outer_pt, -inner_pt, inner_pt, outer_pt])) / 2
    quad_weight = np.array([outer_wt, inner_wt, inner_wt, outer_wt]) / 2
    closed, _ = lagrange(lobatto, quad_points)
    opened, _ = lagrange(gauss_open, quad_points)
    _, colloc = lagrange(quad_points, quad_points)
    return closed, opened, colloc, quad_weight


CLOSED, OPENED, COLLOC, WEIGHT = basis_tables()


def add_all(terms):
    total = terms[0]
    for term in terms[1:]:
        total = total + term
    return total


def apply(mat, xs, sigma=1):
    rows, cols = mat.shape
    half = cols // 2
    plus = [xs[p] + xs[cols - 1 - p] for p in range(half)]
    minus = [xs[p] - xs[cols - 1 - p] for p in range(half)]
    ys = [None] * rows
    for q in range((rows + 1) // 2):
        even_c = [(mat[q, p] + mat[q, cols - 1 - p]) / 2 for p in range(half)]
        odd_c = [(mat[q, p] - mat[q, cols - 1 - p]) / 2 for p in range(half)]
        even = [np.float32(c) * s for c, s in zip(even_c, plus)]
        if cols % 2:
            even.append(np.float32(mat[q, half]) * xs[half])
        even = add_all(even)
        if 2 * q == rows - 1:
            ys[q] = even
            continue
        odd = add_all([np.float32(c) * d for c, d in zip(odd_c, minus)])
        ys[q] = even + odd
        ys[rows - 1 - q] = even - odd if sigma > 0 else odd - even
    return ys


def swap(blocks, size):
    count = blocks[0].shape[0] // size
    return [
        jnp.concatenate([b[q * size : (q + 1) * size] for b in blocks], 0) for q in range(count)
    ]


def dims_of(comp):
    return [ORDER if axis == comp else ORDER + 1 for axis in range(3)]


def kernel(
    mesh_sizes, vec_hbm, flip_hbm, reluct_hbm, conduct_hbm, out_x, out_y, out_z,
    vec, flip, reluct, conduct, elem, sign, mass, curlw, flat, tmp, uq, cq,
    res_x, res_y, res_z, pack1, corner1, hx, hy, hz, hc, pack2_x, pack2_y, corner2,
    near_x, near_y, near_z, last_x, last_y, last_z, rc,
    face, face_own, face_out, coef, coef_in, top_x, top_z, low_x, low_z,
    edge_out, edge_in, low_out, sent, came, s0, ready,
):
    f32 = jnp.float32
    cx, cy = flip.shape[0], flip.shape[1]
    cz = flip.shape[2] // ELEM_DOFS
    counts = (cx, cy, cz)
    ne = cx * cy * cz
    size = tuple(ORDER * c for c in counts)
    lanes = vec.shape[-1]
    me = [lax.axis_index(a) for a in AXES]

    def device(shift):
        return tuple(
            lax.rem(me[a] + (shift[a] + mesh_sizes[a]), mesh_sizes[a]) for a in range(3)
        )

    def signal(sem, shift):
        pl.semaphore_signal(sem, inc=1, device_id=device(shift), device_id_type=MESH)

    fetches = [
        pltpu.make_async_copy(src, dst, s0.at[t])
        for t, (src, dst) in enumerate(
            ((vec_hbm, vec), (flip_hbm, flip), (reluct_hbm, reluct), (conduct_hbm, conduct))
        )
    ]
    for fetch in fetches:
        fetch.start()
    barrier = pltpu.get_barrier_semaphore()
    lowest, highest = me[1] == 0, me[1] == mesh_sizes[1] - 1
    above = ((0, 1, 0), (1, 1, 0), (-1, 1, 0), (0, 1, 1), (0, 1, -1))
    greeted = ((1, 0, 0), (0, 0, 1), (1, 0, 1)) + tuple((s[0], -1, s[2]) for s in above)
    for shift in greeted:
        signal(barrier, shift)

    @pl.when(jnp.logical_not(highest))
    def _():
        for shift in above:
            signal(barrier, shift)

    fetches[0].wait()
    for comp in (0, 1):
        for x in range(size[0]):
            for y in range(size[1]):
                pack1[comp, x, y : y + 1, :] = vec[comp, x, y, 0:1, :]
    for x in range(size[0]):
        corner1[0, x : x + 1, :] = vec[0, x, 0, 0:1, :]
    for y in range(size[1]):
        corner1[1, y : y + 1, :] = vec[1, 0, y, 0:1, :]
    pl.semaphore_wait(barrier, len(greeted) + jnp.where(lowest, 0, len(above)))

    def remote(src, dst, shift, out, into):
        return pltpu.make_async_remote_copy(
            src_ref=src, dst_ref=dst, send_sem=sent.at[out], recv_sem=came.at[into],
            device_id=device(shift), device_id_type=MESH,
        )

    def send(src, dst, shift, out, into):
        remote(src, dst, shift, out, into).start()

    def arrived(rows, into):
        remote(elem.at[0:rows], elem.at[0:rows], (0, 1, 0), 0, into).wait_recv()

    send(vec.at[2, 0], hx.at[1], (-1, 0, 0), 0, 0)
    send(pack1.at[0], hz.at[0], (0, 0, -1), 0, 1)
    send(corner1.at[1], hc.at[0], (-1, 0, -1), 0, 2)
    send(vec.at[1, 0], hx.at[0], (-1, 0, 0), 0, 2)
    send(pack1.at[1], hz.at[1], (0, 0, -1), 0, 2)

    @pl.when(highest)
    def _():
        for shift in above:
            signal(ready, shift)

    def send_down():
        send(corner1.at[0], hc.at[1], (0, -1, -1), 0, 3)
        send(vec.at[2, 0, 0], hc.at[2], (-1, -1, 0), 0, 3)
        send(vec.at[0, :, 0], hy.at[0], (0, -1, 0), 0, 3)
        send(vec.at[2, :, 0], hy.at[1], (0, -1, 0), 0, 3)

    pl.when(jnp.logical_not(lowest))(send_down)

    for fetch in fetches[1:]:
        fetch.wait()
    for i in range(cx):
        for j in range(cy):
            for k in range(cz):
                e = (i * cy + j) * cz + k
                flat[0, e : e + 1, 0:ELEM_DOFS] = 1.0 - 2.0 * flip[
                    i, j : j + 1, k * ELEM_DOFS : (k + 1) * ELEM_DOFS
                ].astype(f32)
                flat[1, e : e + 1, 0:QPTS] = reluct[i, j : j + 1, k * QPTS : (k + 1) * QPTS]
                flat[2, e : e + 1, 0:QPTS] = conduct[i, j : j + 1, k * QPTS : (k + 1) * QPTS]
    for d in range(ELEM_DOFS):
        sign[d * ne : (d + 1) * ne, :] = jnp.broadcast_to(flat[0, :, d : d + 1], (ne, lanes))
    for q in range(QPTS):
        w = np.float32(WEIGHT[q // 16] * WEIGHT[q // 4 % 4] * WEIGHT[q % 4])
        rows = slice(q * ne, (q + 1) * ne)
        curlw[rows, :] = jnp.broadcast_to(flat[1, :, q : q + 1] * w, (ne, lanes))
        mass[rows, :] = jnp.broadcast_to(flat[2, :, q : q + 1] * w, (ne, lanes))

    line_c, line_s = CLOSED[:, ORDER], COLLOC @ CLOSED[:, ORDER]

    def plane_dofs(b):
        found = [(a * 4 + b) * 4 + c for a in range(3) for c in range(4)]
        return found + [96 + (a * 4 + b) * 3 + c for a in range(4) for c in range(3)]

    face_dofs = plane_dofs(ORDER)

    def quad_rows(ref, base, qx, qy):
        first = base + (qx * 16 + qy * 4) * ne
        return ref[first : first + 4 * ne, :]

    def pieces_of(block):
        return [block[t * ne : (t + 1) * ne] for t in range(block.shape[0] // ne)]

    summed = []
    for qx in range(QUAD):
        summed += pieces_of(add_all(
            [np.float32(line_c[qy] ** 2) * quad_rows(mass, 0, qx, qy) for qy in range(QUAD)]
            + [np.float32(line_s[qy] ** 2) * quad_rows(curlw, 0, qx, qy) for qy in range(QUAD)]
        ))
    for qx in range(QUAD):
        summed += pieces_of(add_all(
            [np.float32(line_c[qy] ** 2) * quad_rows(curlw, 0, qx, qy) for qy in range(QUAD)]
        ))
    summed += [sign[d * ne : (d + 1) * ne, :] for d in face_dofs]
    lane = lax.broadcasted_iota(jnp.int32, (ne, lanes), 1)
    packed = jnp.zeros((ne, lanes), f32)
    for t, value in enumerate(summed):
        packed = jnp.where(lane == t, value, packed)
    coef[...] = packed
    send(coef, coef_in, (0, 1, 0), 0, 4)

    def homes(comp, axis, low, high):
        found = []
        for el in range(counts[axis]):
            first = max(low, ORDER * el)
            last = min(high, ORDER * el + dims_of(comp)[axis])
            if first < last:
                found.append((el, first - ORDER * el, first - low, last - first))
        return found

    def places(comp, axis, at, low, high):
        dims = dims_of(comp)
        steps = (dims[1] * dims[2], dims[2], 1)
        span = [(p, p + 1) for p in at]
        span[axis] = (low, high)
        for fx in homes(comp, 0, *span[0]):
            for fy in homes(comp, 1, *span[1]):
                for fz in homes(comp, 2, *span[2]):
                    found = (fx, fy, fz)
                    e = (fx[0] * cy + fy[0]) * cz + fz[0]
                    d = comp * 48 + sum(found[t][1] * steps[t] for t in range(3))
                    yield found[axis][2], found[axis][3], d * ne + e, steps[axis] * ne

    def put(comp, axis, at, low, high, load):
        for offset, length, row, stride in places(comp, axis, at, low, high):
            elem[pl.ds(row, length, stride=stride), :] = load(offset, offset + length)

    def face_places(comp, x, low, high, layer=cy - 1):
        for fx in homes(comp, 0, x, x + 1):
            for fz in homes(comp, 2, low, high):
                e = (fx[0] * cy + layer) * cz + fz[0]
                d = comp // 2 * 12 + fx[1] * dims_of(comp)[2] + fz[1]
                yield fz[2], fz[3], d * ne + e

    def put_face(ref, comp, x, low, high, load):
        for offset, length, row in face_places(comp, x, low, high):
            ref[pl.ds(row, length, stride=ne), :] = load(offset, offset + length)

    blank = jnp.zeros((ne, lanes), f32)
    for t, d in enumerate(face_dofs):
        elem[d * ne : (d + 1) * ne, :] = blank
        face[t * ne : (t + 1) * ne, :] = blank
        face_own[t * ne : (t + 1) * ne, :] = blank
    for comp in range(3):
        for x in range(size[0]):
            for y in range(size[1]):
                put(comp, 2, (x, y, 0), 0, size[2], lambda a, b: vec[comp, x, y, a:b, :])
    for comp in (0, 2):
        for x in range(size[0]):
            put_face(face_own, comp, x, 0, size[2], lambda a, b: vec[comp, x, 0, a:b, :])
    results = (res_x, res_y, res_z)
    for res in (top_x, top_z, low_x, low_z) + results:
        res[...] = jnp.zeros_like(res)


    def take_halo(comp):
        if comp == 1:
            arrived(hc.shape[1] + size[1] * size[2] + size[0] * size[1], 2)
            for y in range(size[1]):
                put(1, 2, (size[0], y, 0), 0, size[2], lambda a, b: hx[0, y, a:b, :])
            for x in range(size[0]):
                put(1, 1, (x, 0, size[2]), 0, size[1], lambda a, b: hz[1, x, a:b, :])
            put(1, 1, (size[0], 0, size[2]), 0, size[1], lambda a, b: hc[0, a:b, :])
        elif comp == 0:
            arrived(size[0] * size[1], 1)
            for x in range(size[0]):
                put(0, 1, (x, 0, size[2]), 0, size[1], lambda a, b: hz[0, x, a:b, :])
                put_face(face_own, 0, x, size[2], size[2] + 1, lambda a, b: hz[0, x, 0:1, :])
        else:
            arrived(size[1] * size[2], 0)
            for y in range(size[1]):
                put(2, 2, (size[0], y, 0), 0, size[2], lambda a, b: hx[1, y, a:b, :])
            put_face(face_own, 2, size[0], 0, size[2], lambda a, b: hx[1, 0, a:b, :])

    def rows_of(axis, at, line, dims):
        others = [t for t in range(3) if t != axis]
        points = []
        for last in range(dims[others[1]]):
            index = [0, 0, 0]
            index[axis], index[others[0]], index[others[1]] = at, line, last
            points.append(((index[0] * dims[1] + index[1]) * dims[2] + index[2]) * ne)
        return points

    def load_line(ref, base, axis, at, line, dims):
        starts = [base + r for r in rows_of(axis, at, line, dims)]
        if len(starts) > 1 and starts[1] - starts[0] == ne:
            return ref[starts[0] : starts[-1] + ne, :]
        return jnp.concatenate([ref[s : s + ne, :] for s in starts], 0)

    def load_plane(ref, base, axis, at, dims):
        others = [t for t in range(3) if t != axis]
        return [load_line(ref, base, axis, at, p, dims) for p in range(dims[others[0]])]

    def store_plane(ref, base, axis, at, dims, blocks):
        for p, block in enumerate(blocks):
            starts = [base + r for r in rows_of(axis, at, p, dims)]
            if starts[1] - starts[0] == ne:
                ref[starts[0] : starts[-1] + ne, :] = block
            else:
                for t, s in enumerate(starts):
                    ref[s : s + ne, :] = block[t * ne : (t + 1) * ne]

    full = [QUAD] * 3

    def mid_dims(comp):
        return [ORDER if axis == comp else QUAD for axis in range(3)]

    def evaluate(comp):
        take_halo(comp)
        dims = dims_of(comp)
        base = comp * 48 * ne
        for a in range(ORDER):
            plane = load_plane(elem, base, comp, a, dims)
            signs = load_plane(sign, base, comp, a, dims)
            plane = [p * s for p, s in zip(plane, signs)]
            plane = apply(CLOSED, plane)
            plane = apply(CLOSED, swap(plane, ne))
            store_plane(tmp, base, comp, a, mid_dims(comp), swap(plane, ne))
        others = [t for t in range(3) if t != comp]
        for line in range(QUAD):
            xs = [load_line(tmp, base, comp, a, line, mid_dims(comp)) for a in range(ORDER)]
            for q, y in enumerate(apply(OPENED, xs)):
                starts = [comp * 64 * ne + r for r in rows_of(comp, q, line, full)]
                if starts[1] - starts[0] == ne:
                    uq[starts[0] : starts[-1] + ne, :] = y
                else:
                    for t, s in enumerate(starts):
                        uq[s : s + ne, :] = y[t * ne : (t + 1) * ne]

    part = 64 * ne

    def half_turn(c, axis, at):
        other = 3 - c - axis
        u = load_plane(uq, other * part, c, at, full)
        if axis < other:
            return apply(COLLOC, u, -1)
        return swap(apply(COLLOC, swap(u, ne), -1), ne)

    def turn_of(c, axis, kept):
        plus = (axis - c) % 3 == 1
        for at in range(QUAD):
            one = half_turn(c, axis, at)
            if kept:
                two = load_plane(cq, c * part, c, at, full)
            else:
                two = half_turn(c, 3 - c - axis, at)
            both = [a - b if plus else b - a for a, b in zip(one, two)]
            scale = load_plane(curlw, 0, c, at, full)
            store_plane(cq, c * part, c, at, full, [k * w for k, w in zip(both, scale)])

    evaluate(2)
    evaluate(0)
    turn_of(1, 2, False)
    @pl.when(lowest)
    def _():
        pl.semaphore_wait(ready, len(above))
        send_down()

    for c in (0, 2):
        for at in range(QUAD):
            store_plane(cq, c * part, c, at, full, half_turn(c, 1, at))

    evaluate(1)
    turn_of(0, 2, True)
    turn_of(2, 0, True)

    closed_t, opened_t, colloc_t = CLOSED.T, OPENED.T, COLLOC.T
    packs = (pack2_x, pack2_y)
    near = (near_x, near_y, near_z)
    last = (last_x, last_y, last_z)
    orders = ((0, 1, 2), (0, 1, 2), (0, 2, 1))

    def face_values(ref, signs):
        at = [ref[t * ne : (t + 1) * ne, :] * signs[t] for t in range(24)]
        xs = [jnp.concatenate([at[a * 4 + c] for a in range(3)], 0) for c in range(4)]
        u_x = apply(OPENED, swap(apply(CLOSED, xs), ne))
        xs = [jnp.concatenate([at[12 + a * 3 + c] for c in range(3)], 0) for a in range(4)]
        u_z = swap(apply(OPENED, swap(apply(CLOSED, xs), ne)), ne)
        along_z = swap(apply(COLLOC, swap(u_x, ne), -1), ne)
        along_x = apply(COLLOC, u_z, -1)
        return u_x, u_z, [f - g for f, g in zip(along_z, along_x)]

    def face_gradient(v_x, v_z, b, signs, into=None):
        into = face_out if into is None else into
        by_z = swap(apply(colloc_t, swap(b, ne), -1), ne)
        by_x = apply(colloc_t, b, -1)
        v_x = [v + f for v, f in zip(v_x, by_z)]
        v_z = [v - f for v, f in zip(v_z, by_x)]
        for c, block in enumerate(apply(closed_t, swap(apply(opened_t, v_x), ne))):
            for a, y in enumerate(pieces_of(block)):
                t = a * 4 + c
                into[t * ne : (t + 1) * ne, :] = y * signs[t]
        for c, block in enumerate(apply(opened_t, swap(apply(closed_t, v_z), ne))):
            for a, y in enumerate(pieces_of(block)):
                t = 12 + a * 3 + c
                into[t * ne : (t + 1) * ne, :] = y * signs[t]

    def plane_fields(values, slopes):
        v_x, v_z, b = [], [], []
        for qx in range(QUAD):
            t_x, t_z, t_b = [], [], []
            for qy in range(QUAD):
                m = quad_rows(mass, 0, qx, qy) * np.float32(values[qy])
                slope = np.float32(slopes[qy])
                t_x += [m * quad_rows(uq, 0, qx, qy), -slope * quad_rows(cq, 2 * part, qx, qy)]
                t_z += [m * quad_rows(uq, 2 * part, qx, qy), slope * quad_rows(cq, 0, qx, qy)]
                t_b += [np.float32(values[qy]) * quad_rows(cq, part, qx, qy)]
            v_x.append(add_all(t_x))
            v_z.append(add_all(t_z))
            b.append(add_all(t_b))
        return v_x, v_z, b

    def signs_of(dofs):
        return [sign[d * ne : (d + 1) * ne, :] for d in dofs]

    def pack_corner(comp, slot, load):
        for t in range(size[comp]):
            corner2[4 * comp + slot, t : t + 1, :] = load(t)

    def send_corner(comp, shift, slot):
        where = 4 * comp + slot
        send(corner2.at[where], rc.at[where], shift, 0, 8)

    def make_plane(side, plane_x, plane_z):
        b, layer = side * ORDER, side * (cy - 1)
        fields = plane_fields(CLOSED[:, b], COLLOC @ CLOSED[:, b])
        face_gradient(*fields, signs_of(plane_dofs(b)))
        for comp, plane in ((0, plane_x), (2, plane_z)):
            for x in range(plane.shape[0]):
                for offset, length, row in face_places(comp, x, 0, plane.shape[1], layer):
                    plane[x, offset : offset + length, :] += face_out[
                        pl.ds(row, length, stride=ne), :
                    ]
        for s in (0, 1):
            z, x = s * size[2], s * size[0]
            pack_corner(0, 2 * side + s, lambda t: plane_x[t, z : z + 1, :])
            pack_corner(2, 2 * s + side, lambda t: plane_z[x, t : t + 1, :])

    def send_plane(side, plane_x, plane_z):
        way = 2 * side - 1
        for s in (0, 1):
            send_corner(0, (0, way, 2 * s - 1), 2 * side + s)
            send_corner(2, (2 * s - 1, way, 0), 2 * s + side)
        send(plane_x, near_x.at[side], (0, way, 0), 0, 5)
        send(plane_z, last_z.at[side], (0, way, 0), 0, 7)

    make_plane(1, top_x, top_z)

    send_plane(1, top_x, top_z)

    if cy > 1:
        make_plane(0, low_x, low_z)
        send_plane(0, low_x, low_z)

    def low_lines():
        arrived(ne, 4)
        theirs = [jnp.broadcast_to(coef_in[:, t : t + 1], (ne, lanes)) for t in range(56)]
        u_x, u_z, turn = face_values(face_own, theirs[32:])
        m2 = [jnp.concatenate(theirs[4 * qx : 4 * qx + 4], 0) for qx in range(QUAD)]
        k2 = [jnp.concatenate(theirs[16 + 4 * qx : 20 + 4 * qx], 0) for qx in range(QUAD)]
        face_gradient(
            [m * u for m, u in zip(m2, u_x)], [m * u for m, u in zip(m2, u_z)],
            [k * u for k, u in zip(k2, turn)], theirs[32:], low_out,
        )
        for s in (0, 1):
            for x in range(size[0]):
                for _, _, row in face_places(0, x, s * size[2], s * size[2] + 1):
                    edge_out[s, x : x + 1, :] = low_out[row : row + 1, :]
            for offset, length, row in face_places(2, s * size[0], 0, size[2]):
                edge_out[2 + s, offset : offset + length, :] = low_out[
                    pl.ds(row, length, stride=ne), :
                ]
            send(edge_out.at[s], edge_in.at[s], (0, 0, 2 * s - 1), 0, 8)
            send(edge_out.at[2 + s], edge_in.at[2 + s], (2 * s - 1, 0, 0), 0, 8)

    pl.when(jnp.logical_not(lowest))(low_lines)
    arrived(2 * size[0] * size[2] + 2 * hc.shape[1], 3)
    for x in range(size[0]):
        put_face(face, 0, x, 0, size[2], lambda a, b: hy[0, x, a:b, :])
        put_face(face, 0, x, size[2], size[2] + 1, lambda a, b: hc[1, x : x + 1, :])
        put_face(face, 2, x, 0, size[2], lambda a, b: hy[1, x, a:b, :])
    put_face(face, 2, size[0], 0, size[2], lambda a, b: hc[2, a:b, :])
    own_signs = signs_of(face_dofs)
    u_x, u_z, turn = face_values(face, own_signs)

    def add_rows(ref, which, qx, qy, more):
        first = which * part + (qx * 16 + qy * 4) * ne
        ref[first : first + 4 * ne, :] += more

    for qx in range(QUAD):
        for qy in range(QUAD):
            sloped = quad_rows(curlw, 0, qx, qy) * np.float32(line_s[qy])
            add_rows(cq, 0, qx, qy, sloped * u_z[qx])
            add_rows(cq, 2, qx, qy, -sloped * u_x[qx])

    if cy == 1:
        make_plane(0, low_x, low_z)
        send_plane(0, low_x, low_z)

    for comp in (1, 2, 0):
        if comp == 2:
            for qx in range(QUAD):
                for qy in range(QUAD):
                    value = np.float32(line_c[qy])
                    add_rows(uq, 0, qx, qy, value * u_x[qx])
                    add_rows(uq, 2, qx, qy, value * u_z[qx])
                    add_rows(cq, 1, qx, qy, (quad_rows(curlw, 0, qx, qy) * value) * turn[qx])
        dims = dims_of(comp)
        base = comp * 48 * ne
        p, r = [t for t in range(3) if t != comp]
        for at in range(QUAD):
            u = load_plane(uq, comp * part, comp, at, full)
            m = load_plane(mass, 0, comp, at, full)
            total = [a * b for a, b in zip(u, m)]
            by_p = apply(colloc_t, load_plane(cq, r * part, comp, at, full), -1)
            by_r = apply(colloc_t, swap(load_plane(cq, p * part, comp, at, full), ne), -1)
            by_r = swap(by_r, ne)
            if comp == 1:
                total = [t + a - b for t, a, b in zip(total, by_p, by_r)]
            else:
                total = [t - a + b for t, a, b in zip(total, by_p, by_r)]
            total = apply(closed_t, total)
            total = apply(closed_t, swap(total, ne))
            kept = [QUAD if axis == comp else ORDER + 1 for axis in range(3)]
            store_plane(tmp, 0, comp, at, kept, swap(total, ne))
        for line in range(ORDER + 1):
            xs = [load_line(tmp, 0, comp, q, line, kept) for q in range(QUAD)]
            for a, y in enumerate(apply(opened_t, xs)):
                y = y * load_line(sign, base, comp, a, line, dims)
                for t, s in enumerate(rows_of(comp, a, line, dims)):
                    elem[base + s : base + s + ne, :] = y[t * ne : (t + 1) * ne]
        res = results[comp]
        order = orders[comp]
        for first in range(res.shape[0]):
            for middle in range(res.shape[1]):
                at = [0, 0, 0]
                at[order[0]], at[order[1]] = first, middle
                pieces = places(comp, order[2], at, 0, res.shape[2])
                for offset, length, row, stride in pieces:
                    res[first, middle, offset : offset + length, :] += elem[
                        pl.ds(row, length, stride=stride), :
                    ]
        if comp == 1:
            for s_x in (0, 1):
                for s_z in (0, 1):
                    x, z = s_x * size[0], s_z * size[2]
                    pack_corner(1, 2 * s_x + s_z, lambda t: res[x, t, z : z + 1, :])
                    send_corner(1, (2 * s_x - 1, 0, 2 * s_z - 1), 2 * s_x + s_z)
        if comp > 0:
            for side in (0, 1):
                send(
                    res.at[side * size[0]], near[comp].at[side], (2 * side - 1, 0, 0),
                    0, 5 + comp,
                )
        if comp < 2:
            for side in (0, 1):
                row = side * size[2]
                for f in range(res.shape[0]):
                    for m in range(res.shape[1]):
                        packs[comp][side, f, m : m + 1, :] = res[f, m, row : row + 1, :]
                send(
                    packs[comp].at[side], last[comp].at[side], (0, 0, 2 * side - 1),
                    0, 5 + comp,
                )
    pl.when(lowest)(low_lines)

    outs = (out_x, out_y, out_z)
    for comp in range(3):
        outs[comp][...] = results[comp][...]
    for x in range(size[0]):
        for offset, length, row in face_places(0, x, 0, size[2] + 1):
            out_x[x, 0, offset : offset + length, :] += low_out[pl.ds(row, length, stride=ne), :]
    for x in range(size[0] + 1):
        for offset, length, row in face_places(2, x, 0, size[2]):
            for t in range(length):
                out_z[x, offset + t, 0:1, :] += low_out[row + t * ne : row + t * ne + 1, :]
    def rim_of(comp):
        return orders[comp][1] if comp == 0 else orders[comp][0]

    for comp in (1, 0, 2):
        out, order, rim = outs[comp], orders[comp], rim_of(comp)
        arrived(2 * size[comp] * (size[rim] + size[order[2]] + 2), 5 + comp)
        for side in (0, 1):
            edge = (1 - side) * size[rim]
            row = (1 - side) * size[order[2]]
            if comp == 0:
                for f in range(out.shape[0]):
                    out[f, edge] += near[comp][side, f]
            else:
                out[edge] += near[comp][side]
            for f in range(out.shape[0]):
                for m in range(out.shape[1]):
                    out[f, m, row : row + 1, :] += last[comp][side, f, m : m + 1, :]
    arrived((12 + 4) * rc.shape[1], 8)
    for comp in range(3):
        out, order, rim = outs[comp], orders[comp], rim_of(comp)
        for slot in range(4):
            edge = (1 - slot // 2) * size[rim]
            row = (1 - slot % 2) * size[order[2]]
            for t in range(size[comp]):
                f, m = (t, edge) if comp == 0 else (edge, t)
                out[f, m, row : row + 1, :] += rc[4 * comp + slot, t : t + 1, :]
    for s in (0, 1):
        z, x = (1 - s) * size[2], (1 - s) * size[0]
        for t in range(size[0]):
            out_x[t, 0, z : z + 1, :] += edge_in[s, t : t + 1, :]
        for t in range(size[2]):
            out_z[x, t, 0:1, :] += edge_in[2 + s, t : t + 1, :]
    rows = ne + (3 + 12 + 4) * rc.shape[1]
    for comp in range(3):
        p, r = [size[t] for t in range(3) if t != comp]
        rows += size[comp] * (p + r) + 2 * size[comp] * (p + r + 2)
    remote(elem.at[0:rows], elem.at[0:rows], (0, 1, 0), 0, 0).wait_send()


def write_out(from_x, from_y, from_z, to_x, to_y, to_z, sems):
    pairs = ((from_x, to_x), (from_y, to_y), (from_z, to_z))
    copies = [pltpu.make_async_copy(src, dst, sems.at[t]) for t, (src, dst) in enumerate(pairs)]
    for copy in copies:
        copy.start()
    for copy in copies:
        copy.wait()


def on_device(mesh_sizes, vectors, orient_flip, reluctivity, conductivity):
    counts = (
        orient_flip.shape[0], orient_flip.shape[1], orient_flip.shape[2] // ELEM_DOFS,
    )
    ne = counts[0] * counts[1] * counts[2]
    sx, sy, sz = (ORDER * c for c in counts)
    lanes = vectors.shape[-1]
    f32 = jnp.float32
    shapes = (
        (sx, sy + 1, sz + 1, lanes), (sx + 1, sy, sz + 1, lanes), (sx + 1, sz, sy + 1, lanes),
    )
    longest = max(sx, sy, sz)
    faces = tuple((2,) + s[:2] + (lanes,) for s in shapes)
    scratch = [
        (ELEM_DOFS * ne, lanes), (ELEM_DOFS * ne, lanes), (QPTS * ne, lanes), (QPTS * ne, lanes),
        (3, ne, ELEM_DOFS), (ELEM_DOFS * ne, lanes), (3 * QPTS * ne, lanes), (3 * QPTS * ne, lanes),
        *shapes,
        (2, sx, sy, lanes), (2, longest, lanes),
        (2, sy, sz, lanes), (2, sx, sz, lanes), (2, sx, sy, lanes), (3, longest, lanes),
        *faces[:2], (12, longest, lanes),
        (2, sx, sz + 1, lanes), (2, sy, sz + 1, lanes), (2, sz, sy + 1, lanes),
        *faces, (12, longest, lanes),
        (24 * ne, lanes), (24 * ne, lanes), (24 * ne, lanes), (ne, lanes), (ne, lanes),
        (sx, sz + 1, lanes), (sx + 1, sz, lanes), (sx, sz + 1, lanes), (sx + 1, sz, lanes),
        (4, longest, lanes), (4, longest, lanes), (24 * ne, lanes),
    ]
    vmem = pl.BlockSpec(memory_space=pltpu.VMEM)
    padded = [s[0] * s[1] * (s[2] + -s[2] % 8) * lanes * 4 for s in shapes]
    room = sum(padded) + max(padded)
    anywhere = pl.BlockSpec(memory_space=pltpu.HBM)
    arguments = (vectors, orient_flip, reluctivity, conductivity)
    outs = [jax.ShapeDtypeStruct(s, f32) for s in shapes]
    held = pl.pallas_call(
        functools.partial(kernel, mesh_sizes),
        out_shape=[pltpu.VMEM(s, f32) for s in shapes],
        in_specs=[anywhere] * 4,
        out_specs=[vmem] * 3,
        scratch_shapes=[pltpu.VMEM(a.shape, a.dtype) for a in arguments]
        + [pltpu.VMEM(s, f32) for s in scratch]
        + [pltpu.SemaphoreType.DMA((1,)), pltpu.SemaphoreType.DMA((9,))]
        + [pltpu.SemaphoreType.DMA((4,)), pltpu.SemaphoreType.REGULAR],
        compiler_params=pltpu.CompilerParams(
            collective_id=0, has_side_effects=True, vmem_limit_bytes=VMEM_ALL - room
        ),
        name="curl_mass",
    )(*arguments)
    held = pl.pallas_call(
        write_out,
        out_shape=outs,
        in_specs=[pl.BlockSpec(memory_space=pl.ANY)] * 3,
        out_specs=[anywhere] * 3,
        scratch_shapes=[pltpu.SemaphoreType.DMA((3,))],
        compiler_params=pltpu.CompilerParams(vmem_limit_bytes=2**20),
        name="write_out",
    )(*held)
    return held[0], held[1], jnp.swapaxes(held[2], 1, 2)


def solution(mesh):
    return jax.shard_map(
        functools.partial(on_device, tuple(mesh.shape[a] for a in AXES)),
        mesh=mesh,
        in_specs=(
            P(None, "gx", "gy", "gz", None),
            P("gx", "gy", "gz"),
            P("gx", "gy", "gz"),
            P("gx", "gy", "gz"),
        ),
        out_specs=(P("gx", "gy", "gz", None), P("gx", "gy", "gz", None), P("gx", "gy", "gz", None)),
        check_vma=False,
    )
```
